32 devices in a mesh: dp: 4 (over x, core), expert: 8 (over z, y).
Axes of the slice: x: 2, y: 2, z: 4, core: 2. Of those that a mesh axis runs over, the one named last changes fastest.
Arguments:
- tokens: bfloat16 [32, 1024, 768], P('dp', 'expert'), may hold values from -6 to 6
- cotangent: bfloat16 [32, 1024, 768], P('dp', 'expert'), may hold values from -6 to 6
- w_project: bfloat16 [768, 2304], replicated, may hold values from -0.21875 to 0.21875
- w_output: bfloat16 [768, 768], replicated, may hold values from -0.875 to 0.875
- norm_gain: float32 [2, 768], replicated, may hold values from 0.5 to 1.5
- norm_bias: float32 [2, 768], replicated, may hold values from -3 to 3
- router: float32 [768, 8], replicated, may hold values from -0.21875 to 0.21875
- expert_weights: bfloat16 [8, 2, 768, 3072], P('expert'), may hold values from -0.21875 to 0.21875
- routes: int32 [32, 1024, 2], P('dp', 'expert'), may hold values from 0 to 7, all different within a row; in each aligned block of 128 rows (0 to 127, 128 to 255, ..., all dimensions but the last counted through in order) at most 40 rows name the same one
- keep_mask: int32 [32, 1024, 2], P('dp', 'expert'), may hold values 0 or 1
- frozen: int32 [8], replicated, may hold values from 0 to 1, as said below
- owner_list: int32 [8], replicated, may hold values from 0 to 7, each once
- attend_master: float32 [8, 768, 384], P('expert'), may hold values from -0.21875 to 0.21875
- attend_first: float32 [8, 768, 384], P('expert'), may hold values from -32 to 32
- attend_second: float32 [8, 768, 384], P('expert'), may hold values from 78.6432 to 1245.184
- attend_left: float32 [8, 768, 768], P('expert'), may hold values from -1 to 1
- attend_right: float32 [8, 384, 384], P('expert'), may hold values from -1 to 1
- expert_master: float32 [8, 2, 768, 3072], P('expert', None, None, 'dp'), may hold values from -0.21875 to 0.21875
- expert_first: float32 [8, 2, 768, 3072], P('expert', None, None, 'dp'), may hold values from -20 to 20
- expert_second: float32 [8, 2, 768, 3072], P('expert', None, None, 'dp'), may hold values from 26.2144 to 425.984
- expert_average: float32 [8, 2, 768, 3072], P('expert', None, None, 'dp'), may hold values from -0.21875 to 0.21875
- expert_basis: float32 [8, 768, 768], P('expert'), may hold values from -1 to 1
- router_first: float32 [768, 8], replicated, may hold values from -640 to 640
- router_second: float32 [768, 8], replicated, may hold values from 21299.2 to 344064
- norm_first: float32 [4, 768], replicated, may hold values from -128 to 128
- norm_second: float32 [4, 768], replicated, may hold values from 851.968 to 13762.56
Outputs:
- output: bfloat16 [32, 1024, 768], P('dp', 'expert')
- input_grad: bfloat16 [32, 1024, 768], P('dp', 'expert')
- norm_grad: float32 [4, 768], replicated
- norm_new: float32 [4, 768], replicated
- norm_first_new: float32 [4, 768], replicated
- norm_second_new: float32 [4, 768], replicated
- router_grad: float32 [768, 8], replicated
- router_new: float32 [768, 8], replicated
- router_first_new: float32 [768, 8], replicated
- router_second_new: float32 [768, 8], replicated
- attend_grad: float32 [8, 768, 384], P('expert')
- attend_master_new: float32 [8, 768, 384], P('expert')
- attend_first_new: float32 [8, 768, 384], P('expert')
- attend_second_new: float32 [8, 768, 384], P('expert')
- expert_grad: float32 [8, 2, 768, 3072], P('expert', None, None, 'dp')
- expert_master_new: float32 [8, 2, 768, 3072], P('expert', None, None, 'dp')
- expert_first_new: float32 [8, 2, 768, 3072], P('expert', None, None, 'dp')
- expert_second_new: float32 [8, 2, 768, 3072], P('expert', None, None, 'dp')
- expert_average_new: float32 [8, 2, 768, 3072], P('expert', None, None, 'dp')
The draws below stay inside these ranges and needn't reach their ends.
Inputs may be any that keep to these rules, and one draw needn't show every extreme that they name: `routes`: each token names two different experts. In each aligned block of 128 tokens (one sequence's tokens on one index of expert) no expert is named by more than 40 choices, and some block reaches 40. `frozen`: exactly half of the experts are flagged 1. `owner_list`: A permutation.
All inputs are finite; a program needn't handle non-finite values. No bound on the sum of `keep_mask` on one device may be relied on, other than what follows from the above.
Results may differ from the reference program's by a relative error of at most 0.025.
Values may be sent and summed in bfloat16 or wider, within the bound.
A program may use at most 448 MiB of HBM per device.

```python
import math
import jax
import jax.numpy as jnp
import numpy as np
from jax import lax

D = 768
HEADS = 12
HEAD_DIM = 64
F = 3072
TOP = 2
LENGTH = 1024
SEQS = 32
EXPERTS = 8
L_DEV = 128
CAPB = 40
CB = 384
N_EXPERT = 8


def orthogonal_table(key, matrix_order):
    shuffled = jax.random.permutation(key, matrix_order).astype(jnp.float32)
    flips = (2 * jax.random.randint(jax.random.fold_in(key, 11), (matrix_order,), 0, 2) - 1).astype(jnp.float32)
    column = jnp.arange(matrix_order, dtype=jnp.float32)[None, :]
    frequency = shuffled[:, None]
    cosine_wave = jnp.cos(math.pi * (column + 0.5) * frequency / matrix_order)
    weight = jnp.where(frequency == 0.0, math.sqrt(1.0 / matrix_order), math.sqrt(2.0 / matrix_order))
    return (flips[:, None] * weight * cosine_wave).astype(jnp.float32)


def draw_attend_left(key, part):
    return jax.vmap(lambda one_key: orthogonal_table(one_key, D))(jax.random.split(jax.random.fold_in(key, 21), N_EXPERT))


def draw_attend_right(key, part):
    return jax.vmap(lambda one_key: orthogonal_table(one_key, CB))(jax.random.split(jax.random.fold_in(key, 22), N_EXPERT))


def draw_expert_basis(key, part):
    return jax.vmap(lambda one_key: orthogonal_table(one_key, D))(jax.random.split(jax.random.fold_in(key, 23), EXPERTS))


def draw_frozen(key, part):
    shuffled = jax.random.permutation(jax.random.fold_in(key, 24), EXPERTS)
    return (shuffled < EXPERTS // 2).astype(jnp.int32)


def with_ends(values, key, smallest, high):
    index_at = [jax.random.randint(jax.random.fold_in(key, axis), (), 0, length) for axis, length in enumerate(values.shape)]
    main_axis = values.shape.index(max(values.shape))
    beside = index_at[:main_axis] + [(index_at[main_axis] + 1) % values.shape[main_axis]] + index_at[main_axis + 1:]
    return values.at[tuple(index_at)].set(smallest).at[tuple(beside)].set(high)


def block_scale(own_key, shape, shards, least, top_value):
    loudness, own = 1.0, jax.random.fold_in(own_key, 6)
    for position, blocks in shards:
        steps = jnp.exp(jax.random.uniform(jax.random.fold_in(own, position), (blocks,), jnp.float32, least / len(shards), top_value / len(shards)))
        loudness = loudness * jnp.repeat(steps, shape[position] // blocks).reshape([-1 if axis == position else 1 for axis in range(len(shape))])
    return loudness


def deal_out(own_key, own, number, rows, count, top, bound, lean):
    ranking = jax.random.permutation(own_key, count)
    heavy_load, common = load_shares(count, rows * top, bound, lean, True), load_shares(count, rows * top, bound, lean, False)
    places = jnp.arange(count)

    def named(lengths, turn):
        used = int((lengths > 0).sum())
        fixed = max(1, used // 4)
        shifted = fixed + (places - fixed + turn * (used - fixed)) % max(1, count - fixed)
        return jnp.zeros((count,), jnp.int32).at[ranking[jnp.where(places < fixed, places, shifted)]].set(jnp.asarray(lengths, jnp.int32))

    lengths = jnp.where(number % 4 == 0, named(heavy_load, number // 4), named(common, number - number // 4 - 1))
    mixed = jax.random.permutation(jax.random.fold_in(own, 3), count)
    giver, taker = mixed[0:count // 2 * 2:2], mixed[1:count // 2 * 2:2]
    margin = jnp.minimum(lengths[giver] - 1, bound - lengths[taker]) // 2
    margin = jnp.where((giver == ranking[0]) | (taker == ranking[0]) | (lengths[taker] == 0), 0, jnp.maximum(margin, 0))
    shifted = jax.random.randint(jax.random.fold_in(own, 4), (count // 2,), 0, 1 << 20) % (margin + 1)
    lengths = lengths.at[giver].add(-shifted).at[taker].add(shifted)
    items = jnp.searchsorted(jnp.cumsum(lengths), jnp.arange(rows * top), side="right").astype(jnp.int32)
    listing = items.reshape(top, rows).T
    listing = listing[jax.random.permutation(jax.random.fold_in(own, 1), rows)]
    turn = jax.random.randint(jax.random.fold_in(own, 2), (rows, 1), 0, top)
    return jnp.take_along_axis(listing, (jnp.arange(top)[None, :] + turn) % top, axis=1)


def load_shares(count, total, most, slope, full):
    weights = [(1 << 20) // math.isqrt(standing ** slope) + 1 for standing in range(1, count + 1)]
    largest = most if full else min(most, max(-(-total // count), total * weights[0] // sum(weights)))
    least = 1 if total - largest >= count - 1 else 0
    given, spare = [largest] + [least] * (count - 1), total - largest - least * (count - 1)
    while spare > 0:
        candidates = [i for i in range(1, count) if given[i] < largest] or [i for i in range(1, count) if given[i] < most]
        whole, remaining = sum([weights[i] for i in candidates]), spare
        for i in candidates:
            addition = min(most - given[i], max(1, remaining * weights[i] // whole), spare)
            given[i] = given[i] + addition
            spare = spare - addition
    return np.array(given)


def normal_values(key, shape, spread, bound, shards=(), kind=jnp.bfloat16):
    gain = block_scale(key, shape, shards, -0.22, 0.18) if shards else 1.0
    values = jax.random.normal(key, shape, jnp.float32) * spread * gain
    return jnp.minimum(jnp.maximum(values, -bound), bound).astype(kind)


def setup_inputs(seed: int = 0) -> dict:
    keys = jax.random.split(jax.random.key(seed), 27)
    tokens = normal_values(keys[0], (SEQS, LENGTH, D), 1.0, 6.0, ((0, 4), (1, 8)))
    cotangent = normal_values(keys[1], (SEQS, LENGTH, D), 1.0, 6.0, ((0, 4), (1, 8)))
    w_project = normal_values(keys[2], (D, 3 * D), D ** -0.5, 0.21875)
    w_output = normal_values(keys[3], (D, D), (D * 64 // LENGTH) ** -0.5, 0.875)
    norm_gain = jnp.clip(1.0 + 0.1 * jax.random.normal(keys[4], (2, D), jnp.float32), 0.5, 1.5)
    norm_bias = normal_values(keys[5], (2, D), 0.5, 3.0, (), jnp.float32)
    router = normal_values(keys[6], (D, EXPERTS), D ** -0.5, 0.21875, (), jnp.float32)
    expert_weights = normal_values(keys[7], (EXPERTS, 2, D, F), D ** -0.5, 0.21875, ((0, 8),))
    routes_keys = jax.random.split(jax.random.fold_in(keys[8], 1), SEQS * LENGTH // L_DEV)
    routes_turns = jax.random.permutation(jax.random.fold_in(keys[8], 3), SEQS * LENGTH // L_DEV)
    routes = jax.vmap(lambda own, number: deal_out(jax.random.fold_in(keys[8], 2), own, number, L_DEV, EXPERTS, TOP, CAPB, 2))(routes_keys, routes_turns).reshape((SEQS, LENGTH, TOP))
    keep_mask = with_ends((jax.random.randint(keys[9], (SEQS, LENGTH, TOP), 0, 8) < 7).astype(jnp.int32), jax.random.fold_in(keys[9], 1), 0, 1)
    frozen = draw_frozen(jax.random.fold_in(keys[26], 71), 0)
    owner_list = jax.random.permutation(keys[11], N_EXPERT).astype(jnp.int32)
    attend_master = normal_values(keys[12], (N_EXPERT, D, CB), D ** -0.5, 0.21875, ((0, 8),), jnp.float32)
    attend_first = normal_values(keys[13], (N_EXPERT, D, CB), (0.033 * (SEQS * LENGTH) ** 0.5), 32.0, ((0, 8),), jnp.float32)
    attend_second = jnp.clip(jnp.exp(math.log(1245.184) - 2.7621173 * jax.random.uniform(keys[14], (N_EXPERT, D, CB), jnp.float32) ** block_scale(keys[14], (N_EXPERT, D, CB), ((0, 8),), -0.2, 0.2)), 78.6432, 1245.184)
    attend_left = draw_attend_left(jax.random.fold_in(keys[26], 71), 0)
    attend_right = draw_attend_right(jax.random.fold_in(keys[26], 71), 0)
    expert_master = normal_values(keys[17], (EXPERTS, 2, D, F), D ** -0.5, 0.21875, ((0, 8), (3, 4)), jnp.float32)
    expert_first = normal_values(keys[18], (EXPERTS, 2, D, F), (0.039 * (SEQS * LENGTH * TOP // EXPERTS) ** 0.5), 20.0, ((0, 8), (3, 4)), jnp.float32)
    expert_second = jnp.clip(jnp.exp(math.log(425.984) - 2.78809295 * jax.random.uniform(keys[19], (EXPERTS, 2, D, F), jnp.float32) ** block_scale(keys[19], (EXPERTS, 2, D, F), ((0, 8), (3, 4)), -0.2, 0.2)), 26.2144, 425.984)
    expert_average = normal_values(keys[20], (EXPERTS, 2, D, F), D ** -0.5, 0.21875, ((0, 8), (3, 4)), jnp.float32)
    expert_basis = draw_expert_basis(jax.random.fold_in(keys[26], 71), 0)
    router_first = normal_values(keys[22], (D, EXPERTS), (1.1 * (SEQS * LENGTH * TOP // EXPERTS) ** 0.5), 640.0, (), jnp.float32)
    router_second = jnp.clip(jnp.exp(jax.random.uniform(keys[23], (D, EXPERTS), jnp.float32, math.log(21299.2), math.log(344064.0))), 21299.2, 344064.0)
    norm_first = normal_values(keys[24], (4, D), (0.11 * (SEQS * LENGTH) ** 0.5), 128.0, (), jnp.float32)
    norm_second = jnp.clip(jnp.exp(jax.random.uniform(keys[25], (4, D), jnp.float32, math.log(851.968), math.log(13762.56))), 851.968, 13762.56)
    return {"tokens": tokens, "cotangent": cotangent, "w_project": w_project, "w_output": w_output, "norm_gain": norm_gain, "norm_bias": norm_bias, "router": router, "expert_weights": expert_weights, "routes": routes, "keep_mask": keep_mask, "frozen": frozen, "owner_list": owner_list, "attend_master": attend_master, "attend_first": attend_first, "attend_second": attend_second, "attend_left": attend_left, "attend_right": attend_right, "expert_master": expert_master, "expert_first": expert_first, "expert_second": expert_second, "expert_average": expert_average, "expert_basis": expert_basis, "router_first": router_first, "router_second": router_second, "norm_first": norm_first, "norm_second": norm_second}


norm_epsilon = 1e-05
beta_one = 0.9
beta_two = 0.95
adam_epsilon = 1e-08
adam_step = 10.0
matrix_rate = 0.1
small_rate = 0.5
average_keep = 0.9
precise = lax.Precision.HIGHEST

@jax.custom_vjp
def low(v):
    return lax.optimization_barrier(v.astype(jnp.bfloat16)).astype(jnp.float32)

@jax.custom_vjp
def low_back(v):
    return v

def low_keep(v):
    return (low(v), None)

def low_pass(kept, grad):
    return (grad,)

def back_keep(v):
    return (v, None)

def back_low(kept, grad):
    return (low(grad),)
low.defvjp(low_keep, low_pass)
low_back.defvjp(back_keep, back_low)

def layer_norm(values, gain_row, bias_row):
    center = values - lax.optimization_barrier(jnp.mean(values, axis=-1, keepdims=True))
    scaled = center * lax.rsqrt(lax.optimization_barrier(jnp.mean(center * center, axis=-1, keepdims=True)) + norm_epsilon)
    return scaled * gain_row + bias_row

def adam_move(gradient, first_moment, second_moment):
    first_new = beta_one * first_moment + (1.0 - beta_one) * gradient
    second_new = beta_two * second_moment + (1.0 - beta_two) * gradient * gradient
    direction = first_new / (1.0 - beta_one ** adam_step) / (jnp.sqrt(second_new / (1.0 - beta_two ** adam_step)) + adam_epsilon)
    return (first_new, second_new, direction)

def attention(queries, keys_all, values_all):
    group_size = queries.shape[0]
    block_rows = min(LENGTH, 512)
    blocks = LENGTH // block_rows
    query_blocks = jnp.moveaxis(queries.reshape(group_size, blocks, block_rows, HEADS, HEAD_DIM), 1, 0)
    starts = jnp.arange(blocks, dtype=jnp.int32) * block_rows
    key_pos = jnp.arange(LENGTH, dtype=jnp.int32)

    def one_block(inputs):
        query_block, start_row = inputs
        scores = jnp.einsum('gqhd,gkhd->ghqk', query_block, keys_all, precision=precise) * HEAD_DIM ** (-0.5)
        scores = low_back(scores)
        query_pos = start_row + jnp.arange(block_rows, dtype=jnp.int32)
        allowed = key_pos[None, :] <= query_pos[:, None]
        scores = jnp.where(allowed, scores, -1e+30)
        weights = low(jax.nn.softmax(scores, axis=-1))
        return jnp.einsum('ghqk,gkhd->gqhd', weights, values_all, precision=precise)
    outputs = lax.map(jax.checkpoint(one_block), (query_blocks, starts))
    return jnp.moveaxis(outputs, 0, 1).reshape(group_size, LENGTH, HEADS * HEAD_DIM)

def block_forward(tokens_wide, project_wide, output_wide, gain_wide, bias_wide, router_wide, expert_wide, route_group, keep_group):
    group_size = tokens_wide.shape[0]
    row_total = group_size * LENGTH
    token_rows = tokens_wide.reshape(row_total, D)
    low_one = low(layer_norm(token_rows, gain_wide[0], bias_wide[0]))
    projected = low(low_back(jnp.dot(low_one, project_wide, precision=precise)))
    queries = projected[:, :D].reshape(group_size, LENGTH, HEADS, HEAD_DIM)
    keys_all = projected[:, D:2 * D].reshape(group_size, LENGTH, HEADS, HEAD_DIM)
    values_all = projected[:, 2 * D:].reshape(group_size, LENGTH, HEADS, HEAD_DIM)
    attended = low(low_back(attention(queries, keys_all, values_all).reshape(row_total, D)))
    middle = token_rows + low_back(jnp.dot(attended, output_wide, precision=precise))
    low_two = low(layer_norm(middle, gain_wide[1], bias_wide[1]))
    logits = jnp.dot(low_two, router_wide, precision=precise)
    choice_ids = route_group.reshape(group_size, N_EXPERT, L_DEV * TOP)
    onehot = (choice_ids[..., None] == jnp.arange(EXPERTS, dtype=jnp.int32)).astype(jnp.float32)
    slot_index = lax.optimization_barrier(jnp.sum(onehot * (jnp.cumsum(onehot, axis=2) - 1.0), axis=-1)).astype(jnp.int32)
    slot_hit = (slot_index[..., None] == jnp.arange(CAPB, dtype=jnp.int32)).astype(jnp.float32)
    kept = keep_group.reshape(group_size, N_EXPERT, L_DEV * TOP).astype(jnp.float32)
    select = kept[..., None, None] * onehot[..., :, None] * slot_hit[..., None, :]
    pair_rows = jnp.repeat(low_two.reshape(group_size, N_EXPERT, L_DEV, D), TOP, axis=2)
    sending = jnp.einsum('gjpec,gjpd->egjcd', select, pair_rows, precision=precise).reshape(EXPERTS, group_size * N_EXPERT * CAPB, D)
    sending = low_back(sending)
    before = low_back(jnp.einsum('erd,edf->erf', sending, expert_wide[:, 0], precision=precise))
    activated = low(jax.nn.gelu(before))
    returned = low(low_back(jnp.einsum('erf,edf->erd', activated, expert_wide[:, 1], precision=precise)))
    returned = returned.reshape(EXPERTS, group_size, N_EXPERT, CAPB, D)
    per_choice = jnp.einsum('gjpec,egjcd->gjpd', select, returned, precision=precise).reshape(group_size, N_EXPERT, L_DEV, TOP, D)
    chosen = lax.optimization_barrier(jnp.sum(onehot.reshape(group_size, N_EXPERT, L_DEV, TOP, EXPERTS) * logits.reshape(group_size, N_EXPERT, L_DEV, 1, EXPERTS), axis=-1))
    gates = jax.nn.softmax(chosen, axis=-1)
    mixture = lax.optimization_barrier(jnp.sum(gates[..., None] * per_choice, axis=3))
    return (middle + mixture.reshape(row_total, D)).reshape(group_size, LENGTH, D)

def reference(tokens, cotangent, w_project, w_output, norm_gain, norm_bias, router, expert_weights, routes, keep_mask, frozen, owner_list, attend_master, attend_first, attend_second, attend_left, attend_right, expert_master, expert_first, expert_second, expert_average, expert_basis, router_first, router_second, norm_first, norm_second):
    group_size = math.gcd(SEQS, 4)
    group_count = SEQS // group_size
    weights_wide = (w_project.astype(jnp.float32), w_output.astype(jnp.float32), norm_gain, norm_bias, router, expert_weights.astype(jnp.float32))

    def one_group(totals, inputs):
        token_group, cot_group, route_group, keep_group = inputs

        def forward(tokens_wide, project_wide, output_wide, gain_wide, bias_wide, router_wide, expert_wide):
            return block_forward(tokens_wide, project_wide, output_wide, gain_wide, bias_wide, router_wide, expert_wide, route_group, keep_group)
        result, pull_back = jax.vjp(forward, token_group.astype(jnp.float32), weights_wide[0], weights_wide[1], weights_wide[2], weights_wide[3], weights_wide[4], weights_wide[5])
        gradients = pull_back(cot_group.astype(jnp.float32))
        totals = tuple((running + part_grad for running, part_grad in zip(totals, gradients[1:])))
        return (totals, (result.astype(jnp.bfloat16), gradients[0].astype(jnp.bfloat16)))
    zeros_init = tuple((jnp.zeros(weight_item.shape, jnp.float32) for weight_item in weights_wide))
    stacked = (tokens.reshape(group_count, group_size, LENGTH, D), cotangent.reshape(group_count, group_size, LENGTH, D), routes.reshape(group_count, group_size, LENGTH, TOP), keep_mask.reshape(group_count, group_size, LENGTH, TOP))
    sums, (outputs, input_grads) = lax.scan(one_group, zeros_init, stacked)
    output = outputs.reshape(SEQS, LENGTH, D)
    input_grad = input_grads.reshape(SEQS, LENGTH, D)
    grad_project, grad_output, grad_gain, grad_bias, router_grad, expert_raw = sums
    norm_grad = jnp.concatenate([grad_gain, grad_bias], axis=0)
    norm_params = jnp.concatenate([norm_gain, norm_bias], axis=0)
    norm_first_new, norm_second_new, norm_step = adam_move(norm_grad, norm_first, norm_second)
    norm_new = norm_params - small_rate * norm_step
    router_first_new, router_second_new, router_step = adam_move(router_grad, router_first, router_second)
    router_new = router - matrix_rate * router_step
    grad_attend = jnp.concatenate([grad_project, grad_output], axis=1)
    blocks_all = jnp.transpose(grad_attend.reshape(D, N_EXPERT, CB), (1, 0, 2))
    slot_range = jnp.arange(N_EXPERT, dtype=jnp.int32)
    match = (owner_list[None, :] == slot_range[:, None]).astype(jnp.float32)
    attend_grad = jnp.einsum('sm,mdc->sdc', match, blocks_all, precision=precise)
    rotated = jnp.einsum('sdj,sdc->sjc', attend_left, attend_grad, precision=precise)
    rotated = jnp.einsum('sjc,sce->sje', rotated, attend_right, precision=precise)
    attend_first_new, attend_second_new, direction = adam_move(rotated, attend_first, attend_second)
    stepped = jnp.einsum('sdj,sje->sde', attend_left, direction, precision=precise)
    stepped = jnp.einsum('sde,sce->sdc', stepped, attend_right, precision=precise)
    attend_master_new = attend_master - matrix_rate * stepped
    frozen_wide = frozen.astype(jnp.float32)[:, None, None, None]
    expert_grad = expert_raw * (1.0 - frozen_wide)
    expert_rotated = jnp.einsum('edj,endf->enjf', expert_basis, expert_grad, precision=precise)
    first_new, second_new, expert_direction = adam_move(expert_rotated, expert_first, expert_second)
    expert_step = jnp.einsum('edj,enjf->endf', expert_basis, expert_direction, precision=precise)
    is_frozen = frozen_wide > 0.5
    expert_master_new = jnp.where(is_frozen, expert_master, expert_master - matrix_rate * expert_step)
    expert_first_new = jnp.where(is_frozen, expert_first, first_new)
    expert_second_new = jnp.where(is_frozen, expert_second, second_new)
    expert_average_new = average_keep * expert_average + (1.0 - average_keep) * expert_master_new
    return (output, input_grad, norm_grad, norm_new, norm_first_new, norm_second_new, router_grad, router_new, router_first_new, router_second_new, attend_grad, attend_master_new, attend_first_new, attend_second_new, expert_grad, expert_master_new, expert_first_new, expert_second_new, expert_average_new)
```

```python
import functools

import jax
import jax.numpy as jnp
from jax import lax
from jax.experimental import pallas as pl
from jax.experimental.pallas import tpu as pltpu
from jax.sharding import PartitionSpec as P

HEADS = 12
HEAD_DIM = 64
TOP = 2
TILE = 256


norm_epsilon = 1e-05
beta_one = 0.9
beta_two = 0.95
adam_epsilon = 1e-08
adam_step = 10.0
matrix_rate = 0.1
small_rate = 0.5
average_keep = 0.9
precise = lax.Precision.HIGHEST
wide = jnp.float32
low = jnp.bfloat16


def norm_parts(values):
    center = values - jnp.mean(values, axis=-1, keepdims=True)
    spread = lax.rsqrt(jnp.mean(center * center, axis=-1, keepdims=True) + norm_epsilon)
    return center * spread, spread


def norm_back(grad, normal, spread, gain_row):
    g = grad * gain_row
    moved = spread * (
        g
        - jnp.mean(g, axis=-1, keepdims=True)
        - normal * jnp.mean(g * normal, axis=-1, keepdims=True)
    )
    return moved, jnp.sum(grad * normal, axis=0), jnp.sum(grad, axis=0)


def adam_move(gradient, first_moment, second_moment):
    first_new = beta_one * first_moment + (1.0 - beta_one) * gradient
    second_new = beta_two * second_moment + (1.0 - beta_two) * gradient * gradient
    direction = (
        first_new
        / (1.0 - beta_one**adam_step)
        / (jnp.sqrt(second_new / (1.0 - beta_two**adam_step)) + adam_epsilon)
    )
    return (first_new, second_new, direction)


def dot_low(a, b, dims):
    return lax.dot_general(a.astype(low), b.astype(low), (dims, ((), ())), preferred_element_type=wide)


ROW_COL = ((1,), (0,))
ROW_ROW = ((1,), (1,))
COL_COL = ((0,), (0,))


def key_pieces(step, tile, key_len, whole):
    if whole:
        return ((0, step * tile, False), (step * tile, (step + 1) * tile, True))
    return ((0, key_len, True),)


def allowed_at(first_query, first_key, tile, key_count):
    rows = lax.broadcasted_iota(jnp.int32, (tile, key_count), 0) + first_query
    columns = lax.broadcasted_iota(jnp.int32, (tile, key_count), 1) + first_key
    return columns <= rows


def attend_kernel(whole, start_ref, q_ref, k_ref, v_ref, out_ref, log_ref):
    rows, lanes = q_ref.shape
    key_len = k_ref.shape[0]
    lane = lax.broadcasted_iota(jnp.int32, (1, lanes), 1)
    for step in range(rows // TILE):
        at = slice(step * TILE, (step + 1) * TILE)
        total, logs = None, []
        for head in range(2):
            mine = (lane // HEAD_DIM) == head
            query = jnp.where(mine, q_ref[at, :] * HEAD_DIM ** (-0.5), 0).astype(low)
            parts = []
            for first, last, masked in key_pieces(step, TILE, key_len, whole):
                if last > first:
                    scores = dot_low(query, k_ref[first:last, :], ROW_ROW)
                    if masked:
                        origin = step * TILE + (0 if whole else start_ref[0])
                        scores = jnp.where(
                            allowed_at(origin, first, TILE, last - first), scores, -1e30
                        )
                    parts.append((first, last, scores))
            top = functools.reduce(
                jnp.maximum, [jnp.max(s, axis=-1, keepdims=True) for _, _, s in parts]
            )
            summed, acc = None, None
            for first, last, scores in parts:
                weights = jnp.exp(scores - top)
                here = jnp.sum(weights, axis=-1, keepdims=True)
                values = jnp.where(mine, v_ref[first:last, :], 0).astype(low)
                add = dot_low(weights, values, ROW_COL)
                summed = here if summed is None else summed + here
                acc = add if acc is None else acc + add
            acc = acc / summed
            total = acc if total is None else total + acc
            logs.append(top + jnp.log(summed))
        out_ref[at, :] = total.astype(out_ref.dtype)
        log_ref[at, :] = jnp.where(lane < HEAD_DIM, logs[0], logs[1])


def attend_back_kernel(
    whole, start_ref, q_ref, k_ref, v_ref, g_ref, a_ref, log_ref, dq_ref, dk_ref, dv_ref, dk_sum, dv_sum
):
    rows, lanes = q_ref.shape
    key_len = k_ref.shape[0]
    lane = lax.broadcasted_iota(jnp.int32, (1, lanes), 1)
    dk_sum[...] = jnp.zeros_like(dk_sum)
    dv_sum[...] = jnp.zeros_like(dv_sum)
    for step in range(rows // TILE):
        at = slice(step * TILE, (step + 1) * TILE)
        grad_all = g_ref[at, :]
        product = grad_all.astype(wide) * a_ref[at, :].astype(wide)
        dq = None
        for head in range(2):
            mine = (lane // HEAD_DIM) == head
            query = jnp.where(mine, q_ref[at, :] * HEAD_DIM ** (-0.5), 0).astype(low)
            grad = jnp.where(mine, grad_all, 0).astype(low)
            delta = jnp.sum(jnp.where(mine, product, 0.0), axis=-1, keepdims=True)
            log_total = log_ref[at, head * HEAD_DIM : head * HEAD_DIM + 1]
            for first, last, masked in key_pieces(step, TILE, key_len, whole):
                if last > first:
                    keys, values = k_ref[first:last, :], v_ref[first:last, :]
                    weights = jnp.exp(dot_low(query, keys, ROW_ROW) - log_total)
                    if masked:
                        origin = step * TILE + (0 if whole else start_ref[0])
                        weights = jnp.where(
                            allowed_at(origin, first, TILE, last - first), weights, 0.0
                        )
                    moved = (weights * (dot_low(grad, values, ROW_ROW) - delta)).astype(low)
                    dv_sum[first:last, :] += dot_low(weights, grad, COL_COL)
                    dk_sum[first:last, :] += dot_low(moved, query, COL_COL)
                    add = dot_low(moved, jnp.where(mine, keys, 0), ROW_COL)
                    dq = add if dq is None else dq + add
        dq_ref[at, :] = (dq * HEAD_DIM ** (-0.5)).astype(low)
    dk_ref[...] = dk_sum[...].astype(low)
    dv_ref[...] = dv_sum[...].astype(low)


def head_block(rows, first):
    return pl.BlockSpec((rows, 2 * HEAD_DIM), lambda pair: (0, first + pair))


def attend(start, queries, keys, values, firsts, whole):
    rows, key_len, pairs = queries.shape[0], keys.shape[0], HEADS // 2
    width = HEADS * HEAD_DIM
    cost = 4 * rows * key_len * width // (2 if whole else 1)
    return pl.pallas_call(
        functools.partial(attend_kernel, whole),
        grid=(pairs,),
        out_shape=(
            jax.ShapeDtypeStruct((rows, width), low),
            jax.ShapeDtypeStruct((rows, width), wide),
        ),
        in_specs=[
            pl.BlockSpec(memory_space=pltpu.SMEM),
            head_block(rows, firsts[0]),
            head_block(key_len, firsts[1]),
            head_block(key_len, firsts[2]),
        ],
        out_specs=(head_block(rows, 0), head_block(rows, 0)),
        cost_estimate=pl.CostEstimate(
            flops=cost, bytes_accessed=12 * rows * width, transcendentals=rows * key_len * HEADS
        ),
        name="attend",
    )(start, queries, keys, values)


def attend_back(start, queries, keys, values, firsts, grads, attended, logs, whole):
    rows, key_len, pairs = queries.shape[0], keys.shape[0], HEADS // 2
    width = HEADS * HEAD_DIM
    cost = 10 * rows * key_len * width // (2 if whole else 1)
    return pl.pallas_call(
        functools.partial(attend_back_kernel, whole),
        grid=(pairs,),
        out_shape=(
            jax.ShapeDtypeStruct((rows, width), low),
            jax.ShapeDtypeStruct((key_len, width), low),
            jax.ShapeDtypeStruct((key_len, width), low),
        ),
        in_specs=[
            pl.BlockSpec(memory_space=pltpu.SMEM),
            head_block(rows, firsts[0]),
            head_block(key_len, firsts[1]),
            head_block(key_len, firsts[2]),
            head_block(rows, 0),
            head_block(rows, 0),
            head_block(rows, 0),
        ],
        out_specs=(head_block(rows, 0), head_block(key_len, 0), head_block(key_len, 0)),
        scratch_shapes=[
            pltpu.VMEM((key_len, 2 * HEAD_DIM), wide),
            pltpu.VMEM((key_len, 2 * HEAD_DIM), wide),
        ],
        cost_estimate=pl.CostEstimate(
            flops=cost, bytes_accessed=20 * rows * width, transcendentals=rows * key_len * HEADS
        ),
        name="attend_back",
    )(start, queries, keys, values, grads, attended, logs)


def on_device(
    tokens,
    cotangent,
    w_project,
    w_output,
    norm_gain,
    norm_bias,
    router,
    expert_weights,
    routes,
    keep_mask,
    frozen,
    owner_list,
    attend_master,
    attend_first,
    attend_second,
    attend_left,
    attend_right,
    expert_master,
    expert_first,
    expert_second,
    expert_average,
    expert_basis,
    router_first,
    router_second,
    norm_first,
    norm_second,
):
    seq_dev, row_len, model_width = tokens.shape
    expert_count = lax.axis_size("expert")
    dp_count = lax.axis_size("dp")
    my_index = lax.axis_index("expert")
    row_count = seq_dev * row_len
    capacity = max(2, 5 * row_len * TOP // (4 * expert_count))
    expert_total = router.shape[1]
    slots = expert_total * capacity
    parts = expert_count // seq_dev
    whole = parts == 1
    groups, across = None, None
    if not whole:
        groups = [[p * seq_dev + s for s in range(seq_dev)] for p in range(parts)]
        across = [[p * seq_dev + s for p in range(parts)] for s in range(seq_dev)]

    def swap(value):
        return lax.all_to_all(
            value, "expert", split_axis=0, concat_axis=0, tiled=True, axis_index_groups=groups
        )

    def exchange(value):
        return lax.all_to_all(value, "expert", split_axis=0, concat_axis=0, tiled=True)

    token_rows = swap(tokens).reshape(row_count, model_width).astype(wide)

    choice_ids = routes.reshape(seq_dev, row_len * TOP)
    onehot = choice_ids[..., None] == jnp.arange(expert_total, dtype=jnp.int32)
    before_me = jnp.tri(row_len * TOP, k=-1, dtype=low)
    earlier = jnp.einsum("pq,sqe->spe", before_me, onehot.astype(low), preferred_element_type=wide)
    slot_index = jnp.sum(jnp.where(onehot, earlier, 0.0), axis=-1).astype(jnp.int32)
    place = choice_ids * capacity + slot_index
    home_code = jnp.where(keep_mask.reshape(choice_ids.shape) > 0, place, -1 - choice_ids)
    home_code = home_code.reshape(seq_dev, row_len, TOP)
    code = swap(home_code)

    def hits_of(codes):
        return [
            codes[:, :, k, None] == jnp.arange(slots, dtype=jnp.int32) for k in range(TOP)
        ]

    home_hits = hits_of(home_code)
    home_select = functools.reduce(jnp.logical_or, home_hits).astype(low)
    home_select = home_select.reshape(seq_dev, row_len, expert_total, capacity)
    cot_slots = jnp.einsum(
        "stec,std->escd", home_select, cotangent, preferred_element_type=wide
    ).astype(low)
    cot_rows = exchange(cot_slots)
    cot_rows = jnp.swapaxes(
        cot_rows.reshape(parts, seq_dev, seq_dev, capacity, model_width), 1, 2
    ).reshape(-1, model_width)
    grad_final = swap(cotangent).reshape(row_count, model_width).astype(wide)

    normal_one, spread_one = norm_parts(token_rows)
    low_one = (normal_one * norm_gain[0] + norm_bias[0]).astype(low)
    projected = jnp.dot(low_one, w_project, preferred_element_type=wide).astype(low)
    start = ((my_index // seq_dev) * row_count).astype(jnp.int32).reshape(1)
    pairs = HEADS // 2
    if whole:
        key_value, firsts = projected, (0, pairs, 2 * pairs)
    else:
        key_value = lax.all_gather(
            projected[:, model_width:], "expert", axis=0, tiled=True, axis_index_groups=across
        )
        firsts = (0, 0, pairs)
    attended_low, logs = attend(start, projected, key_value, key_value, firsts, whole)
    middle = token_rows + jnp.dot(attended_low, w_output, preferred_element_type=wide)
    normal_two, spread_two = norm_parts(middle)
    low_two = (normal_two * norm_gain[1] + norm_bias[1]).astype(low)

    hits = hits_of(code)
    select = functools.reduce(jnp.logical_or, hits).astype(low)
    select = select.reshape(seq_dev, row_len, expert_total, capacity)
    sending = jnp.einsum(
        "jtec,jtd->ejcd",
        select,
        low_two.reshape(seq_dev, row_len, model_width),
        preferred_element_type=wide,
    ).astype(low)
    received = exchange(sending).reshape(-1, model_width)

    low_two_wide = low_two.astype(wide)
    logits = jnp.dot(low_two_wide, router, precision=precise).reshape(
        seq_dev, row_len, 1, expert_total
    )
    route = jnp.where(code >= 0, code // capacity, -1 - code)
    onehot_four = (route[..., None] == jnp.arange(expert_total, dtype=jnp.int32)).astype(wide)
    gates = jax.nn.softmax(jnp.sum(onehot_four * logits, axis=-1), axis=-1)
    gate_slots = sum(
        jnp.sum(jnp.where(hits[k], gates[:, :, k, None], 0.0), axis=1) for k in range(TOP)
    )
    gate_slots = jnp.swapaxes(gate_slots.reshape(seq_dev, expert_total, capacity), 0, 1)
    gate_rows = exchange(gate_slots).reshape(-1, 1)

    w_first = expert_weights[0, 0]
    w_second = expert_weights[0, 1]
    before = jnp.dot(received, w_first, preferred_element_type=wide)
    activated, gelu_back = jax.vjp(jax.nn.gelu, before)
    pulled = jnp.dot(cot_rows, w_second, preferred_element_type=wide)
    gate_grad = jnp.sum(activated * pulled, axis=-1)
    grad_before = gelu_back(gate_rows * pulled)[0].astype(low)
    activated_low = activated.astype(low)
    grad_inputs = jnp.einsum("rf,df->rd", grad_before, w_first, preferred_element_type=wide).astype(
        low
    )
    slot_shape = (expert_count, seq_dev, capacity)
    grad_home = exchange(grad_inputs.reshape(slot_shape + (model_width,)))
    gate_grad_home = exchange(gate_grad.reshape(slot_shape))
    result = (
        jnp.einsum("rf,df->rd", activated_low, w_second, preferred_element_type=wide) * gate_rows
    ).astype(low)
    coming_back = exchange(result.reshape(slot_shape + (model_width,)))
    grad_flat = (gate_rows * cot_rows.astype(wide)).astype(low)
    grad_first_w = jnp.einsum("rd,rf->df", received, grad_before, preferred_element_type=wide)
    grad_second_w = jnp.einsum("rd,rf->df", grad_flat, activated_low, preferred_element_type=wide)
    flag_value = jnp.sum(
        frozen * (jnp.arange(frozen.shape[0], dtype=jnp.int32) == my_index).astype(jnp.int32)
    )
    trainable = (1 - flag_value).astype(wide)
    expert_stack = jnp.stack([grad_first_w, grad_second_w]) * trainable
    expert_grad = lax.psum_scatter(
        expert_stack.astype(low), "dp", scatter_dimension=2, tiled=True
    ).astype(wide)

    gate_grad_flat = jnp.swapaxes(gate_grad_home, 0, 1).reshape(seq_dev, 1, slots)
    grad_gate = jnp.stack(
        [jnp.sum(jnp.where(hits[k], gate_grad_flat, 0.0), axis=-1) for k in range(TOP)], axis=-1
    )
    grad_chosen = gates * (grad_gate - jnp.sum(gates * grad_gate, axis=-1, keepdims=True))
    grad_logits = jnp.sum(onehot_four * grad_chosen[..., None], axis=2).reshape(
        row_count, expert_total
    )
    router_local = jnp.dot(low_two_wide.T, grad_logits, precision=precise)
    grad_low_two = jnp.dot(grad_logits, router.T, precision=precise) + jnp.einsum(
        "jtec,ejcd->jtd", select, grad_home, preferred_element_type=wide
    ).reshape(row_count, model_width)
    moved_two, gain_two, bias_two = norm_back(grad_low_two, normal_two, spread_two, norm_gain[1])
    grad_middle = grad_final + moved_two
    grad_branch = grad_middle.astype(low)
    grad_w_output = jnp.einsum("rd,re->de", attended_low, grad_branch, preferred_element_type=wide)
    grad_attended = jnp.einsum("re,de->rd", grad_branch, w_output, preferred_element_type=wide).astype(
        low
    )

    mixture = jnp.einsum("jtec,ejcd->jtd", select, coming_back, preferred_element_type=wide)
    output = swap(
        (middle + mixture.reshape(row_count, model_width))
        .astype(low)
        .reshape(seq_dev, row_len, model_width)
    )

    grad_query, grad_keys, grad_values = attend_back(
        start, projected, key_value, key_value, firsts, grad_attended, attended_low, logs, whole
    )
    if not whole:
        grad_keys, grad_values = (
            lax.psum_scatter(
                g, "expert", scatter_dimension=0, tiled=True, axis_index_groups=across
            )
            for g in (grad_keys, grad_values)
        )
    grad_projected = jnp.concatenate([grad_query, grad_keys, grad_values], axis=1)
    grad_low_one = jnp.einsum("re,de->rd", grad_projected, w_project, preferred_element_type=wide)
    moved_one, gain_one, bias_one = norm_back(grad_low_one, normal_one, spread_one, norm_gain[0])
    input_grad = swap(
        (grad_middle + moved_one).astype(low).reshape(seq_dev, row_len, model_width)
    )

    grad_w_project = jnp.einsum("rd,re->de", low_one, grad_projected, preferred_element_type=wide)
    grad_norms = jnp.stack([gain_one, gain_two, bias_one, bias_two])
    block_width = attend_master.shape[2]
    grad_full = jnp.concatenate([grad_w_project, grad_w_output], axis=1).astype(low)
    slot_range = jnp.arange(expert_count, dtype=jnp.int32)
    which_block = jnp.sum(
        slot_range[None, :] * (owner_list[None, :] == slot_range[:, None]).astype(jnp.int32), axis=1
    )
    small = jnp.concatenate([router_local.reshape(-1), grad_norms.reshape(-1)])
    small_rows = small.shape[0] // block_width
    padded_rows = -(-small_rows // (16 * dp_count)) * 16 * dp_count
    small = jnp.pad(
        small.astype(low).reshape(small_rows, block_width), ((0, padded_rows - small_rows), (0, 0))
    )
    to_owner = jnp.stack(
        [
            jnp.concatenate(
                [
                    lax.dynamic_slice_in_dim(
                        grad_full, which_block[s] * block_width, block_width, 1
                    ),
                    small,
                ]
            )
            for s in range(expert_count)
        ]
    )
    my_rows = lax.psum_scatter(to_owner, "dp", scatter_dimension=1, tiled=True)
    my_rows = jnp.sum(exchange(my_rows).astype(wide), axis=0)
    summed = lax.all_gather(my_rows, "dp", axis=0, tiled=True)
    block_grad = summed[:model_width]
    small_sum = summed[model_width : model_width + small_rows].reshape(-1)
    router_grad = small_sum[: router.size].reshape(router.shape)
    norm_grad = small_sum[router.size :].reshape(grad_norms.shape)

    left_basis = attend_left[0].astype(low)
    right_basis = attend_right[0].astype(low)
    rotated = dot_low(dot_low(left_basis, block_grad, COL_COL), right_basis, ROW_COL)
    attend_first_new, attend_second_new, direction = adam_move(
        rotated, attend_first[0], attend_second[0]
    )
    stepped = dot_low(dot_low(left_basis, direction, ROW_COL), right_basis, ROW_ROW)
    attend_master_new = attend_master[0] - matrix_rate * stepped

    basis = expert_basis[0].astype(low)
    is_frozen = flag_value > 0
    news = []
    for i in range(2):
        rotated_one = dot_low(basis, expert_grad[i], COL_COL)
        first_new, second_new, move = adam_move(rotated_one, expert_first[0, i], expert_second[0, i])
        master_new = expert_master[0, i] - matrix_rate * dot_low(basis, move, ROW_COL)
        master_new = jnp.where(is_frozen, expert_master[0, i], master_new)
        news.append(
            (
                master_new,
                jnp.where(is_frozen, expert_first[0, i], first_new),
                jnp.where(is_frozen, expert_second[0, i], second_new),
                average_keep * expert_average[0, i] + (1.0 - average_keep) * master_new,
            )
        )
    expert_master_new, expert_first_new, expert_second_new, expert_average_new = (
        jnp.stack(pair) for pair in zip(*news)
    )

    router_first_new, router_second_new, router_step = adam_move(
        router_grad, router_first, router_second
    )
    router_new = router - matrix_rate * router_step
    norm_params = jnp.concatenate([norm_gain, norm_bias], axis=0)
    norm_first_new, norm_second_new, norm_step = adam_move(norm_grad, norm_first, norm_second)
    norm_new = norm_params - small_rate * norm_step
    return (
        output,
        input_grad,
        norm_grad,
        norm_new,
        norm_first_new,
        norm_second_new,
        router_grad,
        router_new,
        router_first_new,
        router_second_new,
        block_grad[None],
        attend_master_new[None],
        attend_first_new[None],
        attend_second_new[None],
        expert_grad[None],
        expert_master_new[None],
        expert_first_new[None],
        expert_second_new[None],
        expert_average_new[None],
    )


def solution(mesh):
    return jax.shard_map(
        on_device,
        mesh=mesh,
        in_specs=(
            P("dp", "expert", None),
            P("dp", "expert", None),
            P(),
            P(),
            P(),
            P(),
            P(),
            P("expert", None, None, None),
            P("dp", "expert", None),
            P("dp", "expert", None),
            P(),
            P(),
            P("expert", None, None),
            P("expert", None, None),
            P("expert", None, None),
            P("expert", None, None),
            P("expert", None, None),
            P("expert", None, None, "dp"),
            P("expert", None, None, "dp"),
            P("expert", None, None, "dp"),
            P("expert", None, None, "dp"),
            P("expert", None, None),
            P(),
            P(),
            P(),
            P(),
        ),
        out_specs=(
            P("dp", "expert", None),
            P("dp", "expert", None),
            P(),
            P(),
            P(),
            P(),
            P(),
            P(),
            P(),
            P(),
            P("expert", None, None),
            P("expert", None, None),
            P("expert", None, None),
            P("expert", None, None),
            P("expert", None, None, "dp"),
            P("expert", None, None, "dp"),
            P("expert", None, None, "dp"),
            P("expert", None, None, "dp"),
            P("expert", None, None, "dp"),
        ),
        check_vma=False,
    )
```

```python
import functools

import jax
import jax.numpy as jnp
from jax import lax
from jax.experimental import pallas as pl
from jax.experimental.pallas import tpu as pltpu
from jax.sharding import PartitionSpec as P

HEADS = 12
HEAD_DIM = 64
TOP = 2
TILE = 256
CHUNK = 512
ROOT = 0.7978845608028654
CUBIC = 0.044715


norm_epsilon = 1e-05
beta_one = 0.9
beta_two = 0.95
adam_epsilon = 1e-08
adam_step = 10.0
matrix_rate = 0.1
small_rate = 0.5
average_keep = 0.9
precise = lax.Precision.HIGHEST
wide = jnp.float32
low = jnp.bfloat16


def norm_parts(values):
    center = values - jnp.mean(values, axis=-1, keepdims=True)
    spread = lax.rsqrt(jnp.mean(center * center, axis=-1, keepdims=True) + norm_epsilon)
    return center * spread, spread


def norm_back(grad, normal, spread, gain_row):
    g = grad * gain_row
    moved = spread * (
        g
        - jnp.mean(g, axis=-1, keepdims=True)
        - normal * jnp.mean(g * normal, axis=-1, keepdims=True)
    )
    return moved, jnp.sum(grad * normal, axis=0), jnp.sum(grad, axis=0)


def adam_move(gradient, first_moment, second_moment):
    first_new = beta_one * first_moment + (1.0 - beta_one) * gradient
    second_new = beta_two * second_moment + (1.0 - beta_two) * gradient * gradient
    direction = (
        first_new
        / (1.0 - beta_one**adam_step)
        / (jnp.sqrt(second_new / (1.0 - beta_two**adam_step)) + adam_epsilon)
    )
    return (first_new, second_new, direction)


def dot_low(a, b, dims):
    return lax.dot_general(a.astype(low), b.astype(low), (dims, ((), ())), preferred_element_type=wide)


ROW_COL = ((1,), (0,))
ROW_ROW = ((1,), (1,))
COL_COL = ((0,), (0,))


def key_pieces(step, tile, key_len, whole):
    if whole:
        return ((0, step * tile, False), (step * tile, (step + 1) * tile, True))
    return ((0, key_len, True),)


def allowed_at(first_query, first_key, tile, key_count):
    rows = lax.broadcasted_iota(jnp.int32, (tile, key_count), 0) + first_query
    columns = lax.broadcasted_iota(jnp.int32, (tile, key_count), 1) + first_key
    return columns <= rows


def attend_kernel(whole, start_ref, q_ref, k_ref, v_ref, out_ref, log_ref):
    rows, lanes = q_ref.shape
    key_len = k_ref.shape[0]
    lane = lax.broadcasted_iota(jnp.int32, (1, lanes), 1)
    for step in range(rows // TILE):
        at = slice(step * TILE, (step + 1) * TILE)
        total, logs = None, []
        for head in range(2):
            mine = (lane // HEAD_DIM) == head
            query = jnp.where(mine, q_ref[at, :] * HEAD_DIM ** (-0.5), 0).astype(low)
            parts = []
            for first, last, masked in key_pieces(step, TILE, key_len, whole):
                if last > first:
                    scores = dot_low(query, k_ref[first:last, :], ROW_ROW)
                    if masked:
                        origin = step * TILE + (0 if whole else start_ref[0])
                        scores = jnp.where(
                            allowed_at(origin, first, TILE, last - first), scores, -1e30
                        )
                    parts.append((first, last, scores))
            top = functools.reduce(
                jnp.maximum, [jnp.max(s, axis=-1, keepdims=True) for _, _, s in parts]
            )
            summed, acc = None, None
            for first, last, scores in parts:
                weights = jnp.exp(scores - top)
                here = jnp.sum(weights, axis=-1, keepdims=True)
                values = jnp.where(mine, v_ref[first:last, :], 0).astype(low)
                add = dot_low(weights, values, ROW_COL)
                summed = here if summed is None else summed + here
                acc = add if acc is None else acc + add
            acc = acc / summed
            total = acc if total is None else total + acc
            logs.append(top + jnp.log(summed))
        out_ref[at, :] = total.astype(out_ref.dtype)
        log_ref[at, :] = jnp.where(lane < HEAD_DIM, logs[0], logs[1])


def attend_back_kernel(
    whole, start_ref, q_ref, k_ref, v_ref, g_ref, a_ref, log_ref, dq_ref, dk_ref, dv_ref, dk_sum, dv_sum
):
    rows, lanes = q_ref.shape
    key_len = k_ref.shape[0]
    lane = lax.broadcasted_iota(jnp.int32, (1, lanes), 1)
    dk_sum[...] = jnp.zeros_like(dk_sum)
    dv_sum[...] = jnp.zeros_like(dv_sum)
    for step in range(rows // TILE):
        at = slice(step * TILE, (step + 1) * TILE)
        grad_all = g_ref[at, :]
        product = grad_all.astype(wide) * a_ref[at, :].astype(wide)
        dq = None
        for head in range(2):
            mine = (lane // HEAD_DIM) == head
            query = jnp.where(mine, q_ref[at, :] * HEAD_DIM ** (-0.5), 0).astype(low)
            grad = jnp.where(mine, grad_all, 0).astype(low)
            delta = jnp.sum(jnp.where(mine, product, 0.0), axis=-1, keepdims=True)
            log_total = log_ref[at, head * HEAD_DIM : head * HEAD_DIM + 1]
            for first, last, masked in key_pieces(step, TILE, key_len, whole):
                if last > first:
                    keys, values = k_ref[first:last, :], v_ref[first:last, :]
                    weights = jnp.exp(dot_low(query, keys, ROW_ROW) - log_total)
                    if masked:
                        origin = step * TILE + (0 if whole else start_ref[0])
                        weights = jnp.where(
                            allowed_at(origin, first, TILE, last - first), weights, 0.0
                        )
                    moved = (weights * (dot_low(grad, values, ROW_ROW) - delta)).astype(low)
                    dv_sum[first:last, :] += dot_low(weights, grad, COL_COL)
                    dk_sum[first:last, :] += dot_low(moved, query, COL_COL)
                    add = dot_low(moved, jnp.where(mine, keys, 0), ROW_COL)
                    dq = add if dq is None else dq + add
        dq_ref[at, :] = (dq * HEAD_DIM ** (-0.5)).astype(low)
    dk_ref[...] = dk_sum[...].astype(low)
    dv_ref[...] = dv_sum[...].astype(low)


def head_block(rows, first):
    return pl.BlockSpec((rows, 2 * HEAD_DIM), lambda pair: (0, first + pair))


def attend(start, queries, keys, values, firsts, whole):
    rows, key_len, pairs = queries.shape[0], keys.shape[0], HEADS // 2
    width = HEADS * HEAD_DIM
    cost = 4 * rows * key_len * width // (2 if whole else 1)
    return pl.pallas_call(
        functools.partial(attend_kernel, whole),
        grid=(pairs,),
        out_shape=(
            jax.ShapeDtypeStruct((rows, width), low),
            jax.ShapeDtypeStruct((rows, width), wide),
        ),
        in_specs=[
            pl.BlockSpec(memory_space=pltpu.SMEM),
            head_block(rows, firsts[0]),
            head_block(key_len, firsts[1]),
            head_block(key_len, firsts[2]),
        ],
        out_specs=(head_block(rows, 0), head_block(rows, 0)),
        cost_estimate=pl.CostEstimate(
            flops=cost, bytes_accessed=12 * rows * width, transcendentals=rows * key_len * HEADS
        ),
        name="attend",
    )(start, queries, keys, values)


def attend_back(start, queries, keys, values, firsts, grads, attended, logs, whole):
    rows, key_len, pairs = queries.shape[0], keys.shape[0], HEADS // 2
    width = HEADS * HEAD_DIM
    cost = 10 * rows * key_len * width // (2 if whole else 1)
    return pl.pallas_call(
        functools.partial(attend_back_kernel, whole),
        grid=(pairs,),
        out_shape=(
            jax.ShapeDtypeStruct((rows, width), low),
            jax.ShapeDtypeStruct((key_len, width), low),
            jax.ShapeDtypeStruct((key_len, width), low),
        ),
        in_specs=[
            pl.BlockSpec(memory_space=pltpu.SMEM),
            head_block(rows, firsts[0]),
            head_block(key_len, firsts[1]),
            head_block(key_len, firsts[2]),
            head_block(rows, 0),
            head_block(rows, 0),
            head_block(rows, 0),
        ],
        out_specs=(head_block(rows, 0), head_block(key_len, 0), head_block(key_len, 0)),
        scratch_shapes=[
            pltpu.VMEM((key_len, 2 * HEAD_DIM), wide),
            pltpu.VMEM((key_len, 2 * HEAD_DIM), wide),
        ],
        cost_estimate=pl.CostEstimate(
            flops=cost, bytes_accessed=20 * rows * width, transcendentals=rows * key_len * HEADS
        ),
        name="attend_back",
    )(start, queries, keys, values, grads, attended, logs)


def expert_kernel(x_ref, u_ref, gate_ref, w_ref, act_ref, grad_ref, input_ref, gate_grad_ref):
    x, gate = x_ref[...], gate_ref[...]
    inputs, gate_grad = None, None
    hidden = w_ref.shape[1]
    for first in range(0, hidden, CHUNK):
        at = slice(first, first + CHUNK)
        w = w_ref[:, at]
        v = dot_low(x, w, ROW_COL)
        u = u_ref[:, at].astype(wide)
        square = v * v
        t = jnp.tanh(ROOT * v * (1.0 + CUBIC * square))
        half = 0.5 * (1.0 + t)
        act = v * half
        slope = half + 0.5 * ROOT * v * (1.0 - t * t) * (1.0 + 3.0 * CUBIC * square)
        grad = (gate * u * slope).astype(low)
        act_ref[:, at] = act.astype(low)
        grad_ref[:, at] = grad
        here = jnp.sum(act * u, axis=-1, keepdims=True)
        add = dot_low(grad, w, ROW_ROW)
        gate_grad = here if gate_grad is None else gate_grad + here
        inputs = add if inputs is None else inputs + add
    input_ref[...] = inputs.astype(low)
    gate_grad_ref[...] = gate_grad


def expert_stage(x, u, gate, w):
    rows, width = x.shape
    hidden = w.shape[1]

    def row_block(columns):
        return pl.BlockSpec((TILE, columns), lambda i: (i, 0))

    return pl.pallas_call(
        expert_kernel,
        grid=(rows // TILE,),
        out_shape=(
            jax.ShapeDtypeStruct((rows, hidden), low),
            jax.ShapeDtypeStruct((rows, hidden), low),
            jax.ShapeDtypeStruct((rows, width), low),
            jax.ShapeDtypeStruct((rows, 1), wide),
        ),
        in_specs=[
            row_block(width),
            row_block(hidden),
            row_block(1),
            pl.BlockSpec((width, hidden), lambda i: (0, 0)),
        ],
        out_specs=(row_block(hidden), row_block(hidden), row_block(width), row_block(1)),
        cost_estimate=pl.CostEstimate(
            flops=4 * rows * width * hidden,
            bytes_accessed=6 * rows * hidden,
            transcendentals=rows * hidden,
        ),
        name="expert_stage",
    )(x, u, gate, w)


def refresh_kernel(
    flag_ref,
    basis_ref,
    turned_ref,
    grad_ref,
    master_ref,
    first_ref,
    second_ref,
    average_ref,
    grad_out,
    master_out,
    first_out,
    second_out,
    average_out,
):
    is_frozen = flag_ref[0] > 0
    grad = grad_ref[0]
    grad_out[0, 0] = grad.astype(wide)
    first_new, second_new, move = adam_move(
        dot_low(turned_ref[...], grad, ROW_COL), first_ref[0, 0], second_ref[0, 0]
    )
    master_new = master_ref[0, 0] - matrix_rate * dot_low(basis_ref[...], move, ROW_COL)
    master_new = jnp.where(is_frozen, master_ref[0, 0], master_new)
    master_out[0, 0] = master_new
    first_out[0, 0] = jnp.where(is_frozen, first_ref[0, 0], first_new)
    second_out[0, 0] = jnp.where(is_frozen, second_ref[0, 0], second_new)
    average_out[0, 0] = average_keep * average_ref[0, 0] + (1.0 - average_keep) * master_new


def refresh(flag, basis, grad, master, first, second, average):
    _, mats, width, columns = master.shape
    step = 256 if columns % 256 == 0 else 128
    block = pl.BlockSpec((1, 1, width, step), lambda i, j: (0, i, 0, j))
    square = pl.BlockSpec((width, width), lambda i, j: (0, 0))
    return pl.pallas_call(
        refresh_kernel,
        grid=(mats, columns // step),
        out_shape=(jax.ShapeDtypeStruct(master.shape, wide),) * 5,
        in_specs=[
            pl.BlockSpec(memory_space=pltpu.SMEM),
            square,
            square,
            pl.BlockSpec((1, width, step), lambda i, j: (i, 0, j)),
        ]
        + [block] * 4,
        out_specs=(block,) * 5,
        cost_estimate=pl.CostEstimate(
            flops=4 * mats * width * width * columns,
            bytes_accessed=38 * mats * width * columns,
            transcendentals=0,
        ),
        name="refresh",
    )(flag, basis, basis.T, grad, master, first, second, average)


def deal_kernel(which_ref, block_ref, small_ref, out_ref):
    width = block_ref.shape[1]
    out_ref[0, :, :width] = block_ref[...]
    out_ref[0, :, width:] = small_ref[...]


def deal(which, rows, block_width, count):
    height, total = rows.shape
    extra = total - block_width * count
    if block_width % 128:
        return jnp.stack(
            [
                jnp.concatenate(
                    [
                        lax.dynamic_slice_in_dim(rows, which[s] * block_width, block_width, 1),
                        rows[:, total - extra :],
                    ],
                    axis=1,
                )
                for s in range(count)
            ]
        )
    return pl.pallas_call(
        deal_kernel,
        grid_spec=pltpu.PrefetchScalarGridSpec(
            num_scalar_prefetch=1,
            grid=(count,),
            in_specs=[
                pl.BlockSpec((height, block_width), lambda s, which: (0, which[s])),
                pl.BlockSpec((height, extra), lambda s, which: (0, total // extra - 1)),
            ],
            out_specs=pl.BlockSpec((1, height, block_width + extra), lambda s, which: (s, 0, 0)),
        ),
        out_shape=jax.ShapeDtypeStruct((count, height, block_width + extra), rows.dtype),
        name="deal",
    )(which, rows, rows)


def after(value, *others):
    return lax.optimization_barrier((value, *others))[0]


def on_device(
    tokens,
    cotangent,
    w_project,
    w_output,
    norm_gain,
    norm_bias,
    router,
    expert_weights,
    routes,
    keep_mask,
    frozen,
    owner_list,
    attend_master,
    attend_first,
    attend_second,
    attend_left,
    attend_right,
    expert_master,
    expert_first,
    expert_second,
    expert_average,
    expert_basis,
    router_first,
    router_second,
    norm_first,
    norm_second,
):
    seq_dev, row_len, model_width = tokens.shape
    expert_count = lax.axis_size("expert")
    dp_count = lax.axis_size("dp")
    my_index = lax.axis_index("expert")
    row_count = seq_dev * row_len
    capacity = max(2, 5 * row_len * TOP // (4 * expert_count))
    expert_total = router.shape[1]
    slots = expert_total * capacity
    parts = expert_count // seq_dev
    whole = parts == 1
    groups, across = None, None
    if not whole:
        groups = [[p * seq_dev + s for s in range(seq_dev)] for p in range(parts)]
        across = [[p * seq_dev + s for p in range(parts)] for s in range(seq_dev)]

    def swap(value):
        return lax.all_to_all(
            value, "expert", split_axis=0, concat_axis=0, tiled=True, axis_index_groups=groups
        )

    def sum_dp(value):
        lines = dp_count // 2
        mine = lax.axis_index("dp")
        line, core = mine // 2, mine % 2
        cut = value.reshape(lines, 2, value.shape[0] // dp_count, value.shape[1])
        given = lax.dynamic_index_in_dim(cut, 1 - core, 1, keepdims=False)
        kept = lax.dynamic_index_in_dim(cut, core, 1, keepdims=False)
        got = lax.ppermute(given, "dp", [(d, d ^ 1) for d in range(dp_count)])
        half = (kept.astype(wide) + got.astype(wide)).astype(low)
        total = lax.dynamic_index_in_dim(half, line, 0, keepdims=False).astype(wide)
        for shift in range(1, lines):
            given = lax.dynamic_index_in_dim(half, (line + shift) % lines, 0, keepdims=False)
            moves = [(d, (d + 2 * shift) % dp_count) for d in range(dp_count)]
            total = total + lax.ppermute(given, "dp", moves).astype(wide)
        return total.astype(low)

    def exchange(value):
        return lax.all_to_all(value, "expert", split_axis=0, concat_axis=0, tiled=True)

    token_seq = swap(tokens)
    token_rows = token_seq.reshape(row_count, model_width).astype(wide)

    choice_ids = routes.reshape(seq_dev, row_len * TOP)
    onehot = choice_ids[..., None] == jnp.arange(expert_total, dtype=jnp.int32)
    before_me = jnp.tri(row_len * TOP, k=-1, dtype=low)
    earlier = jnp.einsum("pq,sqe->spe", before_me, onehot.astype(low), preferred_element_type=wide)
    slot_index = jnp.sum(jnp.where(onehot, earlier, 0.0), axis=-1).astype(jnp.int32)
    place = choice_ids * capacity + slot_index
    home_code = jnp.where(keep_mask.reshape(choice_ids.shape) > 0, place, -1 - choice_ids)
    home_code = jnp.swapaxes(home_code.reshape(seq_dev, row_len, TOP), 1, 2)
    all_codes = lax.all_gather(home_code, "expert", axis=0)
    code = lax.dynamic_slice(
        all_codes,
        ((my_index // seq_dev) * seq_dev, my_index % seq_dev, 0, 0),
        (seq_dev, 1, TOP, row_len),
    )[:, 0]

    def hits_of(codes):
        return [
            codes[:, k, :, None] == jnp.arange(slots, dtype=jnp.int32) for k in range(TOP)
        ]

    home_hits = hits_of(home_code)
    home_select = functools.reduce(jnp.logical_or, home_hits).astype(low)
    home_select = home_select.reshape(seq_dev, row_len, expert_total, capacity)
    cot_slots = jnp.einsum(
        "stec,std->escd", home_select, cotangent, preferred_element_type=wide
    ).astype(low)
    cot_back = exchange(after(cot_slots, token_seq))
    cot_rows = jnp.swapaxes(
        cot_back.reshape(parts, seq_dev, seq_dev, capacity, model_width), 1, 2
    ).reshape(-1, model_width)

    normal_one, spread_one = norm_parts(token_rows)
    low_one = (normal_one * norm_gain[0] + norm_bias[0]).astype(low)
    projected = jnp.dot(low_one, w_project, preferred_element_type=wide).astype(low)
    start = ((my_index // seq_dev) * row_count).astype(jnp.int32).reshape(1)
    pairs = HEADS // 2
    if whole:
        key_value, firsts = projected, (0, pairs, 2 * pairs)
    else:
        key_value = lax.all_gather(
            projected[:, model_width:], "expert", axis=0, tiled=True, axis_index_groups=across
        )
        firsts = (0, 0, pairs)
    attended_low, logs = attend(start, projected, key_value, key_value, firsts, whole)
    middle = token_rows + jnp.dot(attended_low, w_output, preferred_element_type=wide)
    normal_two, spread_two = norm_parts(middle)
    low_two = (normal_two * norm_gain[1] + norm_bias[1]).astype(low)

    hits = hits_of(code)
    select = functools.reduce(jnp.logical_or, hits).astype(low)
    select = select.reshape(seq_dev, row_len, expert_total, capacity)
    sending = jnp.einsum(
        "jtec,jtd->ejcd",
        select,
        low_two.reshape(seq_dev, row_len, model_width),
        preferred_element_type=wide,
    ).astype(low)
    received = exchange(after(sending, cot_back))
    cot_seq = swap(after(cotangent, received))
    grad_final = cot_seq.reshape(row_count, model_width).astype(wide)
    received = received.reshape(-1, model_width)

    low_two_wide = low_two.astype(wide)
    logits = jnp.dot(low_two_wide, router, precision=precise).reshape(
        seq_dev, 1, row_len, expert_total
    )
    route = jnp.where(code >= 0, code // capacity, -1 - code)
    onehot_four = (route[..., None] == jnp.arange(expert_total, dtype=jnp.int32)).astype(wide)
    gates = jax.nn.softmax(jnp.sum(onehot_four * logits, axis=-1), axis=1)
    gate_slots = sum(
        jnp.sum(jnp.where(hits[k], gates[:, k, :, None], 0.0), axis=1) for k in range(TOP)
    )
    gate_slots = jnp.swapaxes(gate_slots.reshape(seq_dev, expert_total, capacity), 0, 1)
    gate_slots = gate_slots.reshape(expert_total, seq_dev * capacity)
    gate_rows = lax.all_gather(gate_slots, "expert", axis=0)
    gate_rows = lax.dynamic_index_in_dim(gate_rows, my_index, 1, keepdims=False).reshape(-1, 1)

    w_first = expert_weights[0, 0]
    w_second = expert_weights[0, 1]
    pulled = jnp.dot(cot_rows, w_second, preferred_element_type=wide).astype(low)
    activated_low, grad_before, grad_inputs, gate_grad = expert_stage(
        received, pulled, gate_rows, w_first
    )
    slot_shape = (expert_count, seq_dev, capacity)
    grad_home = exchange(after(grad_inputs.reshape(slot_shape + (model_width,)), cot_seq))
    gate_grad_home = lax.all_gather(
        gate_grad.reshape(expert_count, seq_dev * capacity), "expert", axis=0
    )
    gate_grad_home = lax.dynamic_index_in_dim(gate_grad_home, my_index, 1, keepdims=False)
    result = (
        jnp.einsum("rf,df->rd", activated_low, w_second, preferred_element_type=wide) * gate_rows
    ).astype(low)
    coming_back = exchange(after(result.reshape(slot_shape + (model_width,)), grad_home))
    grad_flat = (gate_rows * cot_rows.astype(wide)).astype(low)
    grad_first_w = jnp.einsum("rd,rf->df", received, grad_before, preferred_element_type=wide)
    grad_second_w = jnp.einsum("rd,rf->df", grad_flat, activated_low, preferred_element_type=wide)
    flag_value = jnp.sum(
        frozen * (jnp.arange(frozen.shape[0], dtype=jnp.int32) == my_index).astype(jnp.int32)
    )
    trainable = (1 - flag_value).astype(wide)
    expert_stack = jnp.stack(
        [(grad_first_w * trainable).astype(low), (grad_second_w * trainable).astype(low)]
    )
    expert_sum = lax.psum_scatter(expert_stack, "dp", scatter_dimension=2, tiled=True)

    gate_grad_flat = jnp.swapaxes(
        gate_grad_home.reshape(expert_count, seq_dev, capacity), 0, 1
    ).reshape(seq_dev, 1, slots)
    grad_gate = jnp.stack(
        [jnp.sum(jnp.where(hits[k], gate_grad_flat, 0.0), axis=-1) for k in range(TOP)], axis=1
    )
    grad_chosen = gates * (grad_gate - jnp.sum(gates * grad_gate, axis=1, keepdims=True))
    grad_logits = jnp.sum(onehot_four * grad_chosen[..., None], axis=1).reshape(
        row_count, expert_total
    )
    router_local = jnp.dot(low_two_wide.T, grad_logits, precision=precise)
    grad_low_two = jnp.dot(grad_logits, router.T, precision=precise) + jnp.einsum(
        "jtec,ejcd->jtd", select, grad_home, preferred_element_type=wide
    ).reshape(row_count, model_width)
    moved_two, gain_two, bias_two = norm_back(grad_low_two, normal_two, spread_two, norm_gain[1])
    grad_middle = grad_final + moved_two
    grad_branch = grad_middle.astype(low)
    grad_w_output = jnp.einsum("rd,re->de", attended_low, grad_branch, preferred_element_type=wide)
    grad_attended = jnp.einsum("re,de->rd", grad_branch, w_output, preferred_element_type=wide).astype(
        low
    )

    mixture = jnp.einsum("jtec,ejcd->jtd", select, coming_back, preferred_element_type=wide)
    output = swap(
        (middle + mixture.reshape(row_count, model_width))
        .astype(low)
        .reshape(seq_dev, row_len, model_width)
    )

    grad_query, grad_keys, grad_values = attend_back(
        start, projected, key_value, key_value, firsts, grad_attended, attended_low, logs, whole
    )
    if not whole:
        grad_keys, grad_values = (
            lax.psum_scatter(
                g, "expert", scatter_dimension=0, tiled=True, axis_index_groups=across
            )
            for g in (grad_keys, grad_values)
        )
    grad_projected = jnp.concatenate([grad_query, grad_keys, grad_values], axis=1)
    grad_low_one = jnp.einsum("re,de->rd", grad_projected, w_project, preferred_element_type=wide)
    moved_one, gain_one, bias_one = norm_back(grad_low_one, normal_one, spread_one, norm_gain[0])
    input_grad = swap(
        (grad_middle + moved_one).astype(low).reshape(seq_dev, row_len, model_width)
    )

    grad_w_project = jnp.einsum("rd,re->de", low_one, grad_projected, preferred_element_type=wide)
    grad_norms = jnp.stack([gain_one, gain_two, bias_one, bias_two])
    block_width = attend_master.shape[2]
    slot_range = jnp.arange(expert_count, dtype=jnp.int32)
    which_block = jnp.sum(
        slot_range[None, :] * (owner_list[None, :] == slot_range[:, None]).astype(jnp.int32), axis=1
    )
    small_width = expert_total + 4
    small = jnp.concatenate([router_local, grad_norms.T], axis=1).astype(low)
    small = jnp.pad(small, ((0, 0), (0, 128 - small_width)))
    grad_full = jnp.concatenate(
        [grad_w_project.astype(low), grad_w_output.astype(low), small], axis=1
    )
    my_rows = sum_dp(grad_full)
    my_rows = exchange(deal(which_block, my_rows, block_width, expert_count))
    my_rows = jnp.sum(my_rows.astype(wide), axis=0)
    summed = lax.all_gather(my_rows, "dp", axis=0, tiled=True)
    block_grad = summed[:, :block_width]
    small_sum = summed[:, block_width : block_width + small_width]
    router_grad = small_sum[:, :expert_total]
    norm_grad = small_sum[:, expert_total:].T

    left_basis = attend_left[0].astype(low)
    right_basis = attend_right[0].astype(low)
    rotated = dot_low(dot_low(left_basis, block_grad, COL_COL), right_basis, ROW_COL)
    attend_first_new, attend_second_new, direction = adam_move(
        rotated, attend_first[0], attend_second[0]
    )
    stepped = dot_low(dot_low(left_basis, direction, ROW_COL), right_basis, ROW_ROW)
    attend_master_new = attend_master[0] - matrix_rate * stepped

    expert_grad, expert_master_new, expert_first_new, expert_second_new, expert_average_new = refresh(
        flag_value.astype(jnp.int32).reshape(1),
        expert_basis[0].astype(low),
        expert_sum,
        expert_master,
        expert_first,
        expert_second,
        expert_average,
    )

    router_first_new, router_second_new, router_step = adam_move(
        router_grad, router_first, router_second
    )
    router_new = router - matrix_rate * router_step
    norm_params = jnp.concatenate([norm_gain, norm_bias], axis=0)
    norm_first_new, norm_second_new, norm_step = adam_move(norm_grad, norm_first, norm_second)
    norm_new = norm_params - small_rate * norm_step
    return (
        output,
        input_grad,
        norm_grad,
        norm_new,
        norm_first_new,
        norm_second_new,
        router_grad,
        router_new,
        router_first_new,
        router_second_new,
        block_grad[None],
        attend_master_new[None],
        attend_first_new[None],
        attend_second_new[None],
        expert_grad,
        expert_master_new,
        expert_first_new,
        expert_second_new,
        expert_average_new,
    )


def solution(mesh):
    return jax.shard_map(
        on_device,
        mesh=mesh,
        in_specs=(
            P("dp", "expert", None),
            P("dp", "expert", None),
            P(),
            P(),
            P(),
            P(),
            P(),
            P("expert", None, None, None),
            P("dp", "expert", None),
            P("dp", "expert", None),
            P(),
            P(),
            P("expert", None, None),
            P("expert", None, None),
            P("expert", None, None),
            P("expert", None, None),
            P("expert", None, None),
            P("expert", None, None, "dp"),
            P("expert", None, None, "dp"),
            P("expert", None, None, "dp"),
            P("expert", None, None, "dp"),
            P("expert", None, None),
            P(),
            P(),
            P(),
            P(),
        ),
        out_specs=(
            P("dp", "expert", None),
            P("dp", "expert", None),
            P(),
            P(),
            P(),
            P(),
            P(),
            P(),
            P(),
            P(),
            P("expert", None, None),
            P("expert", None, None),
            P("expert", None, None),
            P("expert", None, None),
            P("expert", None, None, "dp"),
            P("expert", None, None, "dp"),
            P("expert", None, None, "dp"),
            P("expert", None, None, "dp"),
            P("expert", None, None, "dp"),
        ),
        check_vma=False,
    )
```

```python
import functools

import jax
import jax.numpy as jnp
from jax import lax
from jax.experimental import pallas as pl
from jax.experimental.pallas import tpu as pltpu
from jax.sharding import PartitionSpec as P

HEADS = 12
HEAD_DIM = 64
TOP = 2
TILE = 256
CHUNK = 512
ROOT = 0.7978845608028654
CUBIC = 0.044715


norm_epsilon = 1e-05
beta_one = 0.9
beta_two = 0.95
adam_epsilon = 1e-08
adam_step = 10.0
matrix_rate = 0.1
small_rate = 0.5
average_keep = 0.9
precise = lax.Precision.HIGHEST
wide = jnp.float32
low = jnp.bfloat16


def norm_parts(values):
    center = values - jnp.mean(values, axis=-1, keepdims=True)
    spread = lax.rsqrt(jnp.mean(center * center, axis=-1, keepdims=True) + norm_epsilon)
    return center * spread, spread


def norm_back(grad, normal, spread, gain_row):
    g = grad * gain_row
    moved = spread * (
        g
        - jnp.mean(g, axis=-1, keepdims=True)
        - normal * jnp.mean(g * normal, axis=-1, keepdims=True)
    )
    return moved, jnp.sum(grad * normal, axis=0), jnp.sum(grad, axis=0)


def adam_move(gradient, first_moment, second_moment):
    first_new = beta_one * first_moment + (1.0 - beta_one) * gradient
    second_new = beta_two * second_moment + (1.0 - beta_two) * gradient * gradient
    direction = (
        first_new
        / (1.0 - beta_one**adam_step)
        / (jnp.sqrt(second_new / (1.0 - beta_two**adam_step)) + adam_epsilon)
    )
    return (first_new, second_new, direction)


def dot_low(a, b, dims):
    return lax.dot_general(a.astype(low), b.astype(low), (dims, ((), ())), preferred_element_type=wide)


ROW_COL = ((1,), (0,))
ROW_ROW = ((1,), (1,))
COL_COL = ((0,), (0,))


def key_pieces(step, tile, key_len, whole):
    if whole:
        return ((0, step * tile, False), (step * tile, (step + 1) * tile, True))
    return ((0, key_len, True),)


def allowed_at(first_query, first_key, tile, key_count):
    rows = lax.broadcasted_iota(jnp.int32, (tile, key_count), 0) + first_query
    columns = lax.broadcasted_iota(jnp.int32, (tile, key_count), 1) + first_key
    return columns <= rows


def attend_kernel(whole, start_ref, q_ref, k_ref, v_ref, out_ref, log_ref):
    rows, lanes = q_ref.shape
    key_len = k_ref.shape[0]
    lane = lax.broadcasted_iota(jnp.int32, (1, lanes), 1)
    for step in range(rows // TILE):
        at = slice(step * TILE, (step + 1) * TILE)
        total, logs = None, []
        for head in range(2):
            mine = (lane // HEAD_DIM) == head
            query = jnp.where(mine, q_ref[at, :] * HEAD_DIM ** (-0.5), 0).astype(low)
            parts = []
            for first, last, masked in key_pieces(step, TILE, key_len, whole):
                if last > first:
                    scores = dot_low(query, k_ref[first:last, :], ROW_ROW)
                    if masked:
                        origin = step * TILE + (0 if whole else start_ref[0])
                        scores = jnp.where(
                            allowed_at(origin, first, TILE, last - first), scores, -1e30
                        )
                    parts.append((first, last, scores))
            top = functools.reduce(
                jnp.maximum, [jnp.max(s, axis=-1, keepdims=True) for _, _, s in parts]
            )
            summed, acc = None, None
            for first, last, scores in parts:
                weights = jnp.exp(scores - top)
                here = jnp.sum(weights, axis=-1, keepdims=True)
                values = jnp.where(mine, v_ref[first:last, :], 0).astype(low)
                add = dot_low(weights, values, ROW_COL)
                summed = here if summed is None else summed + here
                acc = add if acc is None else acc + add
            acc = acc / summed
            total = acc if total is None else total + acc
            logs.append(top + jnp.log(summed))
        out_ref[at, :] = total.astype(out_ref.dtype)
        log_ref[at, :] = jnp.where(lane < HEAD_DIM, logs[0], logs[1])


def attend_back_kernel(
    whole, start_ref, q_ref, k_ref, v_ref, g_ref, a_ref, log_ref, dq_ref, dk_ref, dv_ref, dk_sum, dv_sum
):
    rows, lanes = q_ref.shape
    key_len = k_ref.shape[0]
    lane = lax.broadcasted_iota(jnp.int32, (1, lanes), 1)
    dk_sum[...] = jnp.zeros_like(dk_sum)
    dv_sum[...] = jnp.zeros_like(dv_sum)
    for step in range(rows // TILE):
        at = slice(step * TILE, (step + 1) * TILE)
        grad_all = g_ref[at, :]
        product = grad_all.astype(wide) * a_ref[at, :].astype(wide)
        dq = None
        for head in range(2):
            mine = (lane // HEAD_DIM) == head
            query = jnp.where(mine, q_ref[at, :] * HEAD_DIM ** (-0.5), 0).astype(low)
            grad = jnp.where(mine, grad_all, 0).astype(low)
            delta = jnp.sum(jnp.where(mine, product, 0.0), axis=-1, keepdims=True)
            log_total = log_ref[at, head * HEAD_DIM : head * HEAD_DIM + 1]
            for first, last, masked in key_pieces(step, TILE, key_len, whole):
                if last > first:
                    keys, values = k_ref[first:last, :], v_ref[first:last, :]
                    weights = jnp.exp(dot_low(query, keys, ROW_ROW) - log_total)
                    if masked:
                        origin = step * TILE + (0 if whole else start_ref[0])
                        weights = jnp.where(
                            allowed_at(origin, first, TILE, last - first), weights, 0.0
                        )
                    moved = (weights * (dot_low(grad, values, ROW_ROW) - delta)).astype(low)
                    dv_sum[first:last, :] += dot_low(weights, grad, COL_COL)
                    dk_sum[first:last, :] += dot_low(moved, query, COL_COL)
                    add = dot_low(moved, jnp.where(mine, keys, 0), ROW_COL)
                    dq = add if dq is None else dq + add
        dq_ref[at, :] = (dq * HEAD_DIM ** (-0.5)).astype(low)
    dk_ref[...] = dk_sum[...].astype(low)
    dv_ref[...] = dv_sum[...].astype(low)


def head_block(rows, first):
    return pl.BlockSpec((rows, 2 * HEAD_DIM), lambda pair: (0, first + pair))


def attend(start, queries, keys, values, firsts, whole):
    rows, key_len, pairs = queries.shape[0], keys.shape[0], HEADS // 2
    width = HEADS * HEAD_DIM
    cost = 4 * rows * key_len * width // (2 if whole else 1)
    return pl.pallas_call(
        functools.partial(attend_kernel, whole),
        grid=(pairs,),
        out_shape=(
            jax.ShapeDtypeStruct((rows, width), low),
            jax.ShapeDtypeStruct((rows, width), wide),
        ),
        in_specs=[
            pl.BlockSpec(memory_space=pltpu.SMEM),
            head_block(rows, firsts[0]),
            head_block(key_len, firsts[1]),
            head_block(key_len, firsts[2]),
        ],
        out_specs=(head_block(rows, 0), head_block(rows, 0)),
        cost_estimate=pl.CostEstimate(
            flops=cost, bytes_accessed=12 * rows * width, transcendentals=rows * key_len * HEADS
        ),
        name="attend",
    )(start, queries, keys, values)


def attend_back(start, queries, keys, values, firsts, grads, attended, logs, whole):
    rows, key_len, pairs = queries.shape[0], keys.shape[0], HEADS // 2
    width = HEADS * HEAD_DIM
    cost = 10 * rows * key_len * width // (2 if whole else 1)
    return pl.pallas_call(
        functools.partial(attend_back_kernel, whole),
        grid=(pairs,),
        out_shape=(
            jax.ShapeDtypeStruct((rows, width), low),
            jax.ShapeDtypeStruct((key_len, width), low),
            jax.ShapeDtypeStruct((key_len, width), low),
        ),
        in_specs=[
            pl.BlockSpec(memory_space=pltpu.SMEM),
            head_block(rows, firsts[0]),
            head_block(key_len, firsts[1]),
            head_block(key_len, firsts[2]),
            head_block(rows, 0),
            head_block(rows, 0),
            head_block(rows, 0),
        ],
        out_specs=(head_block(rows, 0), head_block(key_len, 0), head_block(key_len, 0)),
        scratch_shapes=[
            pltpu.VMEM((key_len, 2 * HEAD_DIM), wide),
            pltpu.VMEM((key_len, 2 * HEAD_DIM), wide),
        ],
        cost_estimate=pl.CostEstimate(
            flops=cost, bytes_accessed=20 * rows * width, transcendentals=rows * key_len * HEADS
        ),
        name="attend_back",
    )(start, queries, keys, values, grads, attended, logs)


def expert_kernel(x_ref, u_ref, gate_ref, w_ref, act_ref, grad_ref, input_ref, gate_grad_ref):
    x, gate = x_ref[...], gate_ref[...]
    inputs, gate_grad = None, None
    hidden = w_ref.shape[3]
    for first in range(0, hidden, CHUNK):
        at = slice(first, first + CHUNK)
        w = w_ref[0, 0, :, at]
        v = dot_low(x, w, ROW_COL)
        u = u_ref[:, at].astype(wide)
        square = v * v
        t = jnp.tanh(ROOT * v * (1.0 + CUBIC * square))
        half = 0.5 * (1.0 + t)
        act = v * half
        slope = half + 0.5 * ROOT * v * (1.0 - t * t) * (1.0 + 3.0 * CUBIC * square)
        grad = (gate * u * slope).astype(low)
        act_ref[:, at] = act.astype(low)
        grad_ref[:, at] = grad
        here = jnp.sum(act * u, axis=-1, keepdims=True)
        add = dot_low(grad, w, ROW_ROW)
        gate_grad = here if gate_grad is None else gate_grad + here
        inputs = add if inputs is None else inputs + add
    input_ref[...] = inputs.astype(low)
    gate_grad_ref[...] = gate_grad


def expert_stage(x, u, gate, w):
    rows, width = x.shape
    hidden = w.shape[3]

    def row_block(columns):
        return pl.BlockSpec((TILE, columns), lambda i: (i, 0))

    return pl.pallas_call(
        expert_kernel,
        grid=(rows // TILE,),
        out_shape=(
            jax.ShapeDtypeStruct((rows, hidden), low),
            jax.ShapeDtypeStruct((rows, hidden), low),
            jax.ShapeDtypeStruct((rows, width), low),
            jax.ShapeDtypeStruct((rows, 1), wide),
        ),
        in_specs=[
            row_block(width),
            row_block(hidden),
            row_block(1),
            pl.BlockSpec((1, 1, width, hidden), lambda i: (0, 0, 0, 0)),
        ],
        out_specs=(row_block(hidden), row_block(hidden), row_block(width), row_block(1)),
        cost_estimate=pl.CostEstimate(
            flops=4 * rows * width * hidden,
            bytes_accessed=6 * rows * hidden,
            transcendentals=rows * hidden,
        ),
        name="expert_stage",
    )(x, u, gate, w)


def refresh_kernel(
    flag_ref,
    basis_ref,
    turned_ref,
    grad_ref,
    master_ref,
    first_ref,
    second_ref,
    average_ref,
    grad_out,
    master_out,
    first_out,
    second_out,
    average_out,
):
    is_frozen = flag_ref[0] > 0
    grad = grad_ref[0]
    grad_out[0, 0] = grad.astype(wide)
    first_new, second_new, move = adam_move(
        dot_low(turned_ref[...], grad, ROW_COL), first_ref[0, 0], second_ref[0, 0]
    )
    master_new = master_ref[0, 0] - matrix_rate * dot_low(basis_ref[...], move, ROW_COL)
    master_new = jnp.where(is_frozen, master_ref[0, 0], master_new)
    master_out[0, 0] = master_new
    first_out[0, 0] = jnp.where(is_frozen, first_ref[0, 0], first_new)
    second_out[0, 0] = jnp.where(is_frozen, second_ref[0, 0], second_new)
    average_out[0, 0] = average_keep * average_ref[0, 0] + (1.0 - average_keep) * master_new


def refresh(flag, basis, grad, master, first, second, average):
    _, mats, width, columns = master.shape
    step = 256 if columns % 256 == 0 else 128
    block = pl.BlockSpec((1, 1, width, step), lambda i, j: (0, i, 0, j))
    square = pl.BlockSpec((width, width), lambda i, j: (0, 0))
    return pl.pallas_call(
        refresh_kernel,
        grid=(mats, columns // step),
        out_shape=(jax.ShapeDtypeStruct(master.shape, wide),) * 5,
        in_specs=[
            pl.BlockSpec(memory_space=pltpu.SMEM),
            square,
            square,
            pl.BlockSpec((1, width, step), lambda i, j: (i, 0, j)),
        ]
        + [block] * 4,
        out_specs=(block,) * 5,
        cost_estimate=pl.CostEstimate(
            flops=4 * mats * width * width * columns,
            bytes_accessed=38 * mats * width * columns,
            transcendentals=0,
        ),
        name="refresh",
    )(flag, basis, basis.T, grad, master, first, second, average)


def deal_kernel(which_ref, block_ref, small_ref, out_ref):
    width = block_ref.shape[1]
    out_ref[0, :, :width] = block_ref[...]
    out_ref[0, :, width:] = small_ref[...]


def deal(which, rows, block_width, count):
    height, total = rows.shape
    extra = total - block_width * count
    if block_width % 128:
        return jnp.stack(
            [
                jnp.concatenate(
                    [
                        lax.dynamic_slice_in_dim(rows, which[s] * block_width, block_width, 1),
                        rows[:, total - extra :],
                    ],
                    axis=1,
                )
                for s in range(count)
            ]
        )
    return pl.pallas_call(
        deal_kernel,
        grid_spec=pltpu.PrefetchScalarGridSpec(
            num_scalar_prefetch=1,
            grid=(count,),
            in_specs=[
                pl.BlockSpec((height, block_width), lambda s, which: (0, which[s])),
                pl.BlockSpec((height, extra), lambda s, which: (0, total // extra - 1)),
            ],
            out_specs=pl.BlockSpec((1, height, block_width + extra), lambda s, which: (s, 0, 0)),
        ),
        out_shape=jax.ShapeDtypeStruct((count, height, block_width + extra), rows.dtype),
        name="deal",
    )(which, rows, rows)


def send_kernel(count, capacity, code_ref, row_ref, out_ref):
    place = lax.broadcasted_iota(jnp.int32, (count * capacity, row_ref.shape[0]), 0)
    hit = jnp.logical_or(place == code_ref[0, 0:1, :], place == code_ref[0, 1:2, :])
    rows = dot_low(hit.astype(wide), row_ref[...], ROW_COL)
    for e in range(count):
        out_ref[e, 0] = rows[e * capacity : (e + 1) * capacity].astype(low)


def send_rows(code, rows, count, capacity):
    blocks, _, row_len = code.shape
    width = rows.shape[1]
    return pl.pallas_call(
        functools.partial(send_kernel, count, capacity),
        grid=(blocks,),
        out_shape=jax.ShapeDtypeStruct((count, blocks, capacity, width), low),
        in_specs=[
            pl.BlockSpec((1, TOP, row_len), lambda j: (j, 0, 0)),
            pl.BlockSpec((row_len, width), lambda j: (j, 0)),
        ],
        out_specs=pl.BlockSpec((count, 1, capacity, width), lambda j: (0, j, 0, 0)),
        cost_estimate=pl.CostEstimate(
            flops=2 * blocks * count * capacity * row_len * width,
            bytes_accessed=2 * blocks * (count * capacity + row_len) * width,
            transcendentals=0,
        ),
        name="send_rows",
    )(code, rows)


def after(value, *others):
    return lax.optimization_barrier((value, *others))[0]


def on_device(
    tokens,
    cotangent,
    w_project,
    w_output,
    norm_gain,
    norm_bias,
    router,
    expert_weights,
    routes,
    keep_mask,
    frozen,
    owner_list,
    attend_master,
    attend_first,
    attend_second,
    attend_left,
    attend_right,
    expert_master,
    expert_first,
    expert_second,
    expert_average,
    expert_basis,
    router_first,
    router_second,
    norm_first,
    norm_second,
):
    seq_dev, row_len, model_width = tokens.shape
    expert_count = lax.axis_size("expert")
    dp_count = lax.axis_size("dp")
    my_index = lax.axis_index("expert")
    row_count = seq_dev * row_len
    capacity = max(2, 5 * row_len * TOP // (4 * expert_count))
    expert_total = router.shape[1]
    slots = expert_total * capacity
    parts = expert_count // seq_dev
    whole = parts == 1
    groups, across = None, None
    if not whole:
        groups = [[p * seq_dev + s for s in range(seq_dev)] for p in range(parts)]
        across = [[p * seq_dev + s for p in range(parts)] for s in range(seq_dev)]

    def swap(value):
        return lax.all_to_all(
            value, "expert", split_axis=0, concat_axis=0, tiled=True, axis_index_groups=groups
        )

    def ring(value):
        size = value.shape[0]
        me = my_index % size
        rows = [lax.dynamic_index_in_dim(value, me, 0, keepdims=False)]
        for shift in range(1, size):
            given = lax.dynamic_index_in_dim(value, (me + shift) % size, 0, keepdims=False)
            moves = [
                (d, d - d % size + (d % size + shift) % size) for d in range(expert_count)
            ]
            rows.append(lax.ppermute(given, "expert", moves))
        rows = jnp.stack(rows[::-1])
        return lax.dynamic_slice_in_dim(jnp.concatenate([rows, rows]), size - 1 - me, size, 0)

    def sum_dp(value):
        lines = dp_count // 2
        mine = lax.axis_index("dp")
        line, core = mine // 2, mine % 2
        cut = value.reshape(lines, 2, value.shape[0] // dp_count, value.shape[1])
        given = lax.dynamic_index_in_dim(cut, 1 - core, 1, keepdims=False)
        kept = lax.dynamic_index_in_dim(cut, core, 1, keepdims=False)
        got = lax.ppermute(given, "dp", [(d, d ^ 1) for d in range(dp_count)])
        half = (kept.astype(wide) + got.astype(wide)).astype(low)
        total = lax.dynamic_index_in_dim(half, line, 0, keepdims=False).astype(wide)
        for shift in range(1, lines):
            given = lax.dynamic_index_in_dim(half, (line + shift) % lines, 0, keepdims=False)
            moves = [(d, (d + 2 * shift) % dp_count) for d in range(dp_count)]
            total = total + lax.ppermute(given, "dp", moves).astype(wide)
        return total.astype(low)

    def exchange(value):
        return lax.all_to_all(value, "expert", split_axis=0, concat_axis=0, tiled=True)

    token_seq = swap(tokens)
    token_rows = token_seq.reshape(row_count, model_width).astype(wide)

    choice_ids = routes.reshape(seq_dev, row_len * TOP)
    onehot = choice_ids[..., None] == jnp.arange(expert_total, dtype=jnp.int32)
    before_me = jnp.tri(row_len * TOP, k=-1, dtype=low)
    earlier = jnp.einsum("pq,sqe->spe", before_me, onehot.astype(low), preferred_element_type=wide)
    slot_index = jnp.sum(jnp.where(onehot, earlier, 0.0), axis=-1).astype(jnp.int32)
    place = choice_ids * capacity + slot_index
    home_code = jnp.where(keep_mask.reshape(choice_ids.shape) > 0, place, -1 - choice_ids)
    home_code = jnp.swapaxes(home_code.reshape(seq_dev, row_len, TOP), 1, 2)
    code = ring(home_code)

    def hits_of(codes):
        return [
            codes[:, k, :, None] == jnp.arange(slots, dtype=jnp.int32) for k in range(TOP)
        ]

    cot_slots = send_rows(
        home_code, cotangent.reshape(row_count, model_width), expert_total, capacity
    )
    cot_back = exchange(after(cot_slots, token_seq))
    normal_one, spread_one = norm_parts(token_rows)
    low_one = (normal_one * norm_gain[0] + norm_bias[0]).astype(low)
    projected = jnp.dot(low_one, w_project, preferred_element_type=wide).astype(low)
    start = ((my_index // seq_dev) * row_count).astype(jnp.int32).reshape(1)
    pairs = HEADS // 2
    if whole:
        key_value, firsts = projected, (0, pairs, 2 * pairs)
    else:
        key_value = lax.all_gather(
            projected[:, model_width:], "expert", axis=0, tiled=True, axis_index_groups=across
        )
        firsts = (0, 0, pairs)
    attended_low, logs = attend(start, projected, key_value, key_value, firsts, whole)
    middle = token_rows + jnp.dot(attended_low, w_output, preferred_element_type=wide)
    normal_two, spread_two = norm_parts(middle)
    low_two = (normal_two * norm_gain[1] + norm_bias[1]).astype(low)

    hits = hits_of(code)
    select = functools.reduce(jnp.logical_or, hits).astype(low)
    select = select.reshape(seq_dev, row_len, expert_total, capacity)
    sending = send_rows(code, low_two, expert_total, capacity)
    received = exchange(after(sending, cot_back))
    cot_rows = jnp.swapaxes(
        cot_back.reshape(parts, seq_dev, seq_dev, capacity, model_width), 1, 2
    ).reshape(-1, model_width)
    w_second = expert_weights[0, 1]
    pulled = jnp.dot(cot_rows, w_second, preferred_element_type=wide).astype(low)
    received = received.reshape(-1, model_width)

    low_two_wide = low_two.astype(wide)
    logits = jnp.dot(low_two_wide, router, precision=precise).reshape(
        seq_dev, 1, row_len, expert_total
    )
    route = jnp.where(code >= 0, code // capacity, -1 - code)
    onehot_four = (route[..., None] == jnp.arange(expert_total, dtype=jnp.int32)).astype(wide)
    gates = jax.nn.softmax(jnp.sum(onehot_four * logits, axis=-1), axis=1)
    gate_slots = sum(
        jnp.sum(jnp.where(hits[k], gates[:, k, :, None], 0.0), axis=1) for k in range(TOP)
    )
    gate_slots = jnp.swapaxes(gate_slots.reshape(seq_dev, expert_total, capacity), 0, 1)
    gate_slots = gate_slots.reshape(expert_total, seq_dev * capacity)
    gate_rows = ring(gate_slots).reshape(-1, 1)
    cot_seq = swap(after(cotangent, received, pulled, gate_rows))
    grad_final = cot_seq.reshape(row_count, model_width).astype(wide)

    activated_low, grad_before, grad_inputs, gate_grad = expert_stage(
        received, pulled, gate_rows, expert_weights
    )
    slot_shape = (expert_count, seq_dev, capacity)
    grad_inputs = grad_inputs.reshape(slot_shape + (model_width,))
    grad_inputs, activated_low, grad_before, gate_grad, _ = lax.optimization_barrier(
        (grad_inputs, activated_low, grad_before, gate_grad, cot_seq)
    )
    grad_home = exchange(grad_inputs)
    gate_grad_home = ring(gate_grad.reshape(expert_count, seq_dev * capacity))
    result = (
        jnp.einsum("rf,df->rd", activated_low, w_second, preferred_element_type=wide) * gate_rows
    ).astype(low)
    coming_back = exchange(
        after(result.reshape(slot_shape + (model_width,)), grad_home, gate_grad_home)
    )
    grad_flat = (gate_rows * cot_rows.astype(wide)).astype(low)
    grad_first_w = jnp.einsum("rd,rf->df", received, grad_before, preferred_element_type=wide)
    grad_second_w = jnp.einsum("rd,rf->df", grad_flat, activated_low, preferred_element_type=wide)
    flag_value = jnp.sum(
        frozen * (jnp.arange(frozen.shape[0], dtype=jnp.int32) == my_index).astype(jnp.int32)
    )
    trainable = (1 - flag_value).astype(wide)
    expert_stack = jnp.stack(
        [(grad_first_w * trainable).astype(low), (grad_second_w * trainable).astype(low)]
    )
    expert_sum = lax.psum_scatter(expert_stack, "dp", scatter_dimension=2, tiled=True)

    gate_grad_flat = jnp.swapaxes(
        gate_grad_home.reshape(expert_count, seq_dev, capacity), 0, 1
    ).reshape(seq_dev, 1, slots)
    grad_gate = jnp.stack(
        [jnp.sum(jnp.where(hits[k], gate_grad_flat, 0.0), axis=-1) for k in range(TOP)], axis=1
    )
    grad_chosen = gates * (grad_gate - jnp.sum(gates * grad_gate, axis=1, keepdims=True))
    grad_logits = jnp.sum(onehot_four * grad_chosen[..., None], axis=1).reshape(
        row_count, expert_total
    )
    router_local = jnp.dot(low_two_wide.T, grad_logits, precision=precise)
    grad_low_two = jnp.dot(grad_logits, router.T, precision=precise) + jnp.einsum(
        "jtec,ejcd->jtd", select, grad_home, preferred_element_type=wide
    ).reshape(row_count, model_width)
    moved_two, gain_two, bias_two = norm_back(grad_low_two, normal_two, spread_two, norm_gain[1])
    grad_middle = grad_final + moved_two
    grad_branch = grad_middle.astype(low)
    grad_w_output = jnp.einsum("rd,re->de", attended_low, grad_branch, preferred_element_type=wide)
    grad_attended = jnp.einsum("re,de->rd", grad_branch, w_output, preferred_element_type=wide).astype(
        low
    )

    grad_query, grad_keys, grad_values = attend_back(
        start, projected, key_value, key_value, firsts, grad_attended, attended_low, logs, whole
    )
    mixture = jnp.einsum("jtec,ejcd->jtd", select, after(coming_back, grad_query), preferred_element_type=wide)
    output_seq = (
        (middle + mixture.reshape(row_count, model_width))
        .astype(low)
        .reshape(seq_dev, row_len, model_width)
    )
    if not whole:
        grad_keys, grad_values = (
            lax.psum_scatter(
                g, "expert", scatter_dimension=0, tiled=True, axis_index_groups=across
            )
            for g in (grad_keys, grad_values)
        )
    grad_projected = jnp.concatenate([grad_query, grad_keys, grad_values], axis=1)
    grad_low_one = jnp.einsum("re,de->rd", grad_projected, w_project, preferred_element_type=wide)
    moved_one, gain_one, bias_one = norm_back(grad_low_one, normal_one, spread_one, norm_gain[0])
    input_grad = (grad_middle + moved_one).astype(low).reshape(seq_dev, row_len, model_width)
    input_grad = swap(after(input_grad, coming_back))

    grad_w_project = jnp.einsum("rd,re->de", low_one, grad_projected, preferred_element_type=wide)
    grad_norms = jnp.stack([gain_one, gain_two, bias_one, bias_two])
    block_width = attend_master.shape[2]
    slot_range = jnp.arange(expert_count, dtype=jnp.int32)
    which_block = jnp.sum(
        slot_range[None, :] * (owner_list[None, :] == slot_range[:, None]).astype(jnp.int32), axis=1
    )
    small_width = expert_total + 4
    small = jnp.concatenate([router_local, grad_norms.T], axis=1).astype(low)
    small = jnp.pad(small, ((0, 0), (0, 128 - small_width)))
    grad_full = jnp.concatenate(
        [grad_w_project.astype(low), grad_w_output.astype(low), small], axis=1
    )
    my_rows = sum_dp(grad_full)
    my_rows = deal(which_block, my_rows, block_width, expert_count)
    my_rows = exchange(after(my_rows, input_grad))
    my_rows = jnp.sum(my_rows.astype(wide), axis=0)
    summed = lax.all_gather(my_rows, "dp", axis=0, tiled=True)
    block_grad = summed[:, :block_width]
    small_sum = summed[:, block_width : block_width + small_width]
    router_grad = small_sum[:, :expert_total]
    norm_grad = small_sum[:, expert_total:].T

    left_basis = attend_left[0].astype(low)
    right_basis = attend_right[0].astype(low)
    rotated = dot_low(dot_low(left_basis, block_grad, COL_COL), right_basis, ROW_COL)
    attend_first_new, attend_second_new, direction = adam_move(
        rotated, attend_first[0], attend_second[0]
    )
    stepped = dot_low(dot_low(left_basis, direction, ROW_COL), right_basis, ROW_ROW)
    attend_master_new = attend_master[0] - matrix_rate * stepped

    expert_grad, expert_master_new, expert_first_new, expert_second_new, expert_average_new = refresh(
        flag_value.astype(jnp.int32).reshape(1),
        expert_basis[0].astype(low),
        expert_sum,
        expert_master,
        expert_first,
        expert_second,
        expert_average,
    )

    output = swap(after(output_seq, expert_grad))

    output = after(output, attend_master_new)

    router_first_new, router_second_new, router_step = adam_move(
        router_grad, router_first, router_second
    )
    router_new = router - matrix_rate * router_step
    norm_params = jnp.concatenate([norm_gain, norm_bias], axis=0)
    norm_first_new, norm_second_new, norm_step = adam_move(norm_grad, norm_first, norm_second)
    norm_new = norm_params - small_rate * norm_step
    return (
        output,
        input_grad,
        norm_grad,
        norm_new,
        norm_first_new,
        norm_second_new,
        router_grad,
        router_new,
        router_first_new,
        router_second_new,
        block_grad[None],
        attend_master_new[None],
        attend_first_new[None],
        attend_second_new[None],
        expert_grad,
        expert_master_new,
        expert_first_new,
        expert_second_new,
        expert_average_new,
    )


def solution(mesh):
    return jax.shard_map(
        on_device,
        mesh=mesh,
        in_specs=(
            P("dp", "expert", None),
            P("dp", "expert", None),
            P(),
            P(),
            P(),
            P(),
            P(),
            P("expert", None, None, None),
            P("dp", "expert", None),
            P("dp", "expert", None),
            P(),
            P(),
            P("expert", None, None),
            P("expert", None, None),
            P("expert", None, None),
            P("expert", None, None),
            P("expert", None, None),
            P("expert", None, None, "dp"),
            P("expert", None, None, "dp"),
            P("expert", None, None, "dp"),
            P("expert", None, None, "dp"),
            P("expert", None, None),
            P(),
            P(),
            P(),
            P(),
        ),
        out_specs=(
            P("dp", "expert", None),
            P("dp", "expert", None),
            P(),
            P(),
            P(),
            P(),
            P(),
            P(),
            P(),
            P(),
            P("expert", None, None),
            P("expert", None, None),
            P("expert", None, None),
            P("expert", None, None),
            P("expert", None, None, "dp"),
            P("expert", None, None, "dp"),
            P("expert", None, None, "dp"),
            P("expert", None, None, "dp"),
            P("expert", None, None, "dp"),
        ),
        check_vma=False,
    )
```

```python
import functools

import jax
import jax.numpy as jnp
from jax import lax
from jax.experimental import pallas as pl
from jax.experimental.pallas import tpu as pltpu
from jax.sharding import PartitionSpec as P

HEADS = 12
HEAD_DIM = 64
TOP = 2
TILE = 256
CHUNK = 512
ROOT = 0.7978845608028654
CUBIC = 0.044715


norm_epsilon = 1e-05
beta_one = 0.9
beta_two = 0.95
adam_epsilon = 1e-08
adam_step = 10.0
matrix_rate = 0.1
small_rate = 0.5
average_keep = 0.9
precise = lax.Precision.HIGHEST
wide = jnp.float32
low = jnp.bfloat16


def norm_parts(values):
    center = values - jnp.mean(values, axis=-1, keepdims=True)
    spread = lax.rsqrt(jnp.mean(center * center, axis=-1, keepdims=True) + norm_epsilon)
    return center * spread, spread


def norm_back(grad, normal, spread, gain_row):
    g = grad * gain_row
    moved = spread * (
        g
        - jnp.mean(g, axis=-1, keepdims=True)
        - normal * jnp.mean(g * normal, axis=-1, keepdims=True)
    )
    return moved, jnp.sum(grad * normal, axis=0), jnp.sum(grad, axis=0)


def adam_move(gradient, first_moment, second_moment):
    first_new = beta_one * first_moment + (1.0 - beta_one) * gradient
    second_new = beta_two * second_moment + (1.0 - beta_two) * gradient * gradient
    direction = (
        first_new
        / (1.0 - beta_one**adam_step)
        / (jnp.sqrt(second_new / (1.0 - beta_two**adam_step)) + adam_epsilon)
    )
    return (first_new, second_new, direction)


def dot_low(a, b, dims):
    return lax.dot_general(a.astype(low), b.astype(low), (dims, ((), ())), preferred_element_type=wide)


ROW_COL = ((1,), (0,))
ROW_ROW = ((1,), (1,))
COL_COL = ((0,), (0,))


def key_pieces(step, tile, key_len, whole):
    if whole:
        return ((0, step * tile, False), (step * tile, (step + 1) * tile, True))
    return ((0, key_len, True),)


def allowed_at(first_query, first_key, tile, key_count):
    rows = lax.broadcasted_iota(jnp.int32, (tile, key_count), 0) + first_query
    columns = lax.broadcasted_iota(jnp.int32, (tile, key_count), 1) + first_key
    return columns <= rows


def attend_kernel(whole, start_ref, q_ref, k_ref, v_ref, out_ref, log_ref):
    rows, lanes = q_ref.shape
    key_len = k_ref.shape[0]
    lane = lax.broadcasted_iota(jnp.int32, (1, lanes), 1)
    for step in range(rows // TILE):
        at = slice(step * TILE, (step + 1) * TILE)
        total, logs = None, []
        for head in range(2):
            mine = (lane // HEAD_DIM) == head
            query = jnp.where(mine, q_ref[at, :] * HEAD_DIM ** (-0.5), 0).astype(low)
            parts = []
            for first, last, masked in key_pieces(step, TILE, key_len, whole):
                if last > first:
                    scores = dot_low(query, k_ref[first:last, :], ROW_ROW)
                    if masked:
                        origin = step * TILE + (0 if whole else start_ref[0])
                        scores = jnp.where(
                            allowed_at(origin, first, TILE, last - first), scores, -1e30
                        )
                    parts.append((first, last, scores))
            top = functools.reduce(
                jnp.maximum, [jnp.max(s, axis=-1, keepdims=True) for _, _, s in parts]
            )
            summed, acc = None, None
            for first, last, scores in parts:
                weights = jnp.exp(scores - top)
                here = jnp.sum(weights, axis=-1, keepdims=True)
                values = jnp.where(mine, v_ref[first:last, :], 0).astype(low)
                add = dot_low(weights, values, ROW_COL)
                summed = here if summed is None else summed + here
                acc = add if acc is None else acc + add
            acc = acc / summed
            total = acc if total is None else total + acc
            logs.append(top + jnp.log(summed))
        out_ref[at, :] = total.astype(out_ref.dtype)
        log_ref[at, :] = jnp.where(lane < HEAD_DIM, logs[0], logs[1])


def attend_back_kernel(
    whole, start_ref, q_ref, k_ref, v_ref, g_ref, a_ref, log_ref, dq_ref, dk_ref, dv_ref, dk_sum, dv_sum
):
    rows, lanes = q_ref.shape
    key_len = k_ref.shape[0]
    lane = lax.broadcasted_iota(jnp.int32, (1, lanes), 1)
    dk_sum[...] = jnp.zeros_like(dk_sum)
    dv_sum[...] = jnp.zeros_like(dv_sum)
    for step in range(rows // TILE):
        at = slice(step * TILE, (step + 1) * TILE)
        grad_all = g_ref[at, :]
        product = grad_all.astype(wide) * a_ref[at, :].astype(wide)
        dq = None
        for head in range(2):
            mine = (lane // HEAD_DIM) == head
            query = jnp.where(mine, q_ref[at, :] * HEAD_DIM ** (-0.5), 0).astype(low)
            grad = jnp.where(mine, grad_all, 0).astype(low)
            delta = jnp.sum(jnp.where(mine, product, 0.0), axis=-1, keepdims=True)
            log_total = log_ref[at, head * HEAD_DIM : head * HEAD_DIM + 1]
            for first, last, masked in key_pieces(step, TILE, key_len, whole):
                if last > first:
                    keys, values = k_ref[first:last, :], v_ref[first:last, :]
                    weights = jnp.exp(dot_low(query, keys, ROW_ROW) - log_total)
                    if masked:
                        origin = step * TILE + (0 if whole else start_ref[0])
                        weights = jnp.where(
                            allowed_at(origin, first, TILE, last - first), weights, 0.0
                        )
                    moved = (weights * (dot_low(grad, values, ROW_ROW) - delta)).astype(low)
                    dv_sum[first:last, :] += dot_low(weights, grad, COL_COL)
                    dk_sum[first:last, :] += dot_low(moved, query, COL_COL)
                    add = dot_low(moved, jnp.where(mine, keys, 0), ROW_COL)
                    dq = add if dq is None else dq + add
        dq_ref[at, :] = (dq * HEAD_DIM ** (-0.5)).astype(low)
    dk_ref[...] = dk_sum[...].astype(low)
    dv_ref[...] = dv_sum[...].astype(low)


def head_block(rows, first):
    return pl.BlockSpec((rows, 2 * HEAD_DIM), lambda pair: (0, first + pair))


def attend(start, queries, keys, values, firsts, whole):
    rows, key_len, pairs = queries.shape[0], keys.shape[0], HEADS // 2
    width = HEADS * HEAD_DIM
    cost = 4 * rows * key_len * width // (2 if whole else 1)
    return pl.pallas_call(
        functools.partial(attend_kernel, whole),
        grid=(pairs,),
        out_shape=(
            jax.ShapeDtypeStruct((rows, width), low),
            jax.ShapeDtypeStruct((rows, width), wide),
        ),
        in_specs=[
            pl.BlockSpec(memory_space=pltpu.SMEM),
            head_block(rows, firsts[0]),
            head_block(key_len, firsts[1]),
            head_block(key_len, firsts[2]),
        ],
        out_specs=(head_block(rows, 0), head_block(rows, 0)),
        cost_estimate=pl.CostEstimate(
            flops=cost, bytes_accessed=12 * rows * width, transcendentals=rows * key_len * HEADS
        ),
        name="attend",
    )(start, queries, keys, values)


def attend_back(start, queries, keys, values, firsts, grads, attended, logs, whole):
    rows, key_len, pairs = queries.shape[0], keys.shape[0], HEADS // 2
    width = HEADS * HEAD_DIM
    cost = 10 * rows * key_len * width // (2 if whole else 1)
    return pl.pallas_call(
        functools.partial(attend_back_kernel, whole),
        grid=(pairs,),
        out_shape=(
            jax.ShapeDtypeStruct((rows, width), low),
            jax.ShapeDtypeStruct((key_len, width), low),
            jax.ShapeDtypeStruct((key_len, width), low),
        ),
        in_specs=[
            pl.BlockSpec(memory_space=pltpu.SMEM),
            head_block(rows, firsts[0]),
            head_block(key_len, firsts[1]),
            head_block(key_len, firsts[2]),
            head_block(rows, 0),
            head_block(rows, 0),
            head_block(rows, 0),
        ],
        out_specs=(head_block(rows, 0), head_block(key_len, 0), head_block(key_len, 0)),
        scratch_shapes=[
            pltpu.VMEM((key_len, 2 * HEAD_DIM), wide),
            pltpu.VMEM((key_len, 2 * HEAD_DIM), wide),
        ],
        cost_estimate=pl.CostEstimate(
            flops=cost, bytes_accessed=20 * rows * width, transcendentals=rows * key_len * HEADS
        ),
        name="attend_back",
    )(start, queries, keys, values, grads, attended, logs)


def expert_kernel(x_ref, u_ref, w_ref, act_ref, grad_ref, input_ref, gate_grad_ref):
    x = x_ref[...]
    inputs, gate_grad = None, None
    hidden = w_ref.shape[3]
    for first in range(0, hidden, CHUNK):
        at = slice(first, first + CHUNK)
        w = w_ref[0, 0, :, at]
        v = dot_low(x, w, ROW_COL)
        u = u_ref[:, at].astype(wide)
        square = v * v
        t = jnp.tanh(ROOT * v * (1.0 + CUBIC * square))
        half = 0.5 * (1.0 + t)
        act = v * half
        slope = half + 0.5 * ROOT * v * (1.0 - t * t) * (1.0 + 3.0 * CUBIC * square)
        grad = (u * slope).astype(low)
        act_ref[:, at] = act.astype(low)
        grad_ref[:, at] = grad
        here = jnp.sum(act * u, axis=-1, keepdims=True)
        add = dot_low(grad, w, ROW_ROW)
        gate_grad = here if gate_grad is None else gate_grad + here
        inputs = add if inputs is None else inputs + add
    input_ref[...] = inputs.astype(low)
    gate_grad_ref[...] = gate_grad


def expert_stage(x, u, w):
    rows, width = x.shape
    hidden = w.shape[3]

    def row_block(columns):
        return pl.BlockSpec((TILE, columns), lambda i: (i, 0))

    return pl.pallas_call(
        expert_kernel,
        grid=(rows // TILE,),
        out_shape=(
            jax.ShapeDtypeStruct((rows, hidden), low),
            jax.ShapeDtypeStruct((rows, hidden), low),
            jax.ShapeDtypeStruct((rows, width), low),
            jax.ShapeDtypeStruct((rows, 1), wide),
        ),
        in_specs=[
            row_block(width),
            row_block(hidden),
            pl.BlockSpec((1, 1, width, hidden), lambda i: (0, 0, 0, 0)),
        ],
        out_specs=(row_block(hidden), row_block(hidden), row_block(width), row_block(1)),
        cost_estimate=pl.CostEstimate(
            flops=4 * rows * width * hidden,
            bytes_accessed=6 * rows * hidden,
            transcendentals=rows * hidden,
        ),
        name="expert_stage",
    )(x, u, w)


def refresh_kernel(
    flag_ref,
    basis_ref,
    turned_ref,
    grad_ref,
    master_ref,
    first_ref,
    second_ref,
    average_ref,
    grad_out,
    master_out,
    first_out,
    second_out,
    average_out,
):
    is_frozen = flag_ref[0] > 0
    grad = grad_ref[0]
    grad_out[0, 0] = grad.astype(wide)
    first_new, second_new, move = adam_move(
        dot_low(turned_ref[...], grad, ROW_COL), first_ref[0, 0], second_ref[0, 0]
    )
    master_new = master_ref[0, 0] - matrix_rate * dot_low(basis_ref[...], move, ROW_COL)
    master_new = jnp.where(is_frozen, master_ref[0, 0], master_new)
    master_out[0, 0] = master_new
    first_out[0, 0] = jnp.where(is_frozen, first_ref[0, 0], first_new)
    second_out[0, 0] = jnp.where(is_frozen, second_ref[0, 0], second_new)
    average_out[0, 0] = average_keep * average_ref[0, 0] + (1.0 - average_keep) * master_new


def refresh(flag, basis, grad, master, first, second, average):
    _, mats, width, columns = master.shape
    step = 256 if columns % 256 == 0 else 128
    block = pl.BlockSpec((1, 1, width, step), lambda i, j: (0, i, 0, j))
    square = pl.BlockSpec((width, width), lambda i, j: (0, 0))
    return pl.pallas_call(
        refresh_kernel,
        grid=(mats, columns // step),
        out_shape=(jax.ShapeDtypeStruct(master.shape, wide),) * 5,
        in_specs=[
            pl.BlockSpec(memory_space=pltpu.SMEM),
            square,
            square,
            pl.BlockSpec((1, width, step), lambda i, j: (i, 0, j)),
        ]
        + [block] * 4,
        out_specs=(block,) * 5,
        cost_estimate=pl.CostEstimate(
            flops=4 * mats * width * width * columns,
            bytes_accessed=38 * mats * width * columns,
            transcendentals=0,
        ),
        name="refresh",
    )(flag, basis, basis.T, grad, master, first, second, average)


def deal_kernel(which_ref, block_ref, small_ref, out_ref):
    width = block_ref.shape[1]
    out_ref[0, :, :width] = block_ref[...]
    out_ref[0, :, width:] = small_ref[...]


def deal(which, rows, block_width, count):
    height, total = rows.shape
    extra = total - block_width * count
    if block_width % 128:
        return jnp.stack(
            [
                jnp.concatenate(
                    [
                        lax.dynamic_slice_in_dim(rows, which[s] * block_width, block_width, 1),
                        rows[:, total - extra :],
                    ],
                    axis=1,
                )
                for s in range(count)
            ]
        )
    return pl.pallas_call(
        deal_kernel,
        grid_spec=pltpu.PrefetchScalarGridSpec(
            num_scalar_prefetch=1,
            grid=(count,),
            in_specs=[
                pl.BlockSpec((height, block_width), lambda s, which: (0, which[s])),
                pl.BlockSpec((height, extra), lambda s, which: (0, total // extra - 1)),
            ],
            out_specs=pl.BlockSpec((1, height, block_width + extra), lambda s, which: (s, 0, 0)),
        ),
        out_shape=jax.ShapeDtypeStruct((count, height, block_width + extra), rows.dtype),
        name="deal",
    )(which, rows, rows)


def trade_kernel(count, in_ref, out_ref, landed, send_sem, recv_sem):
    me = lax.axis_index("expert")
    barrier = pltpu.get_barrier_semaphore()
    for shift in range(1, count):
        peer = lax.rem(me + shift, count)
        pl.semaphore_signal(
            barrier, inc=1, device_id={"expert": peer}, device_id_type=pl.DeviceIdType.MESH
        )
    pl.semaphore_wait(barrier, count - 1)
    copies = []
    for shift in range(1, count):
        peer = lax.rem(me + shift, count)
        copy = pltpu.make_async_remote_copy(
            src_ref=in_ref.at[peer],
            dst_ref=landed.at[me],
            send_sem=send_sem.at[shift - 1],
            recv_sem=recv_sem.at[shift - 1],
            device_id={"expert": peer},
            device_id_type=pl.DeviceIdType.MESH,
        )
        copy.start()
        copies.append(copy)
    for shift, copy in zip(range(1, count), copies):
        copy.wait()
        source = lax.rem(me + count - shift, count)
        out_ref[pl.ds(source, 1)] = landed[pl.ds(source, 1)]
    out_ref[pl.ds(me, 1)] = in_ref[pl.ds(me, 1)]


def trade(value):
    count, size = value.shape
    lines = -(-size // 1024) * 8
    padded = jnp.pad(value, ((0, 0), (0, lines * 128 - size))).reshape(count, lines, 128)
    out = pl.pallas_call(
        functools.partial(trade_kernel, count),
        out_shape=jax.ShapeDtypeStruct(padded.shape, padded.dtype),
        in_specs=[pl.BlockSpec(memory_space=pltpu.VMEM)],
        out_specs=pl.BlockSpec(memory_space=pltpu.VMEM),
        scratch_shapes=[
            pltpu.VMEM(padded.shape, padded.dtype),
            pltpu.SemaphoreType.DMA((count - 1,)),
            pltpu.SemaphoreType.DMA((count - 1,)),
        ],
        compiler_params=pltpu.CompilerParams(collective_id=0, has_side_effects=True),
        name="trade",
    )(padded)
    return out.reshape(count, lines * 128)[:, :size]


def send_kernel(count, capacity, code_ref, row_ref, out_ref):
    place = lax.broadcasted_iota(jnp.int32, (count * capacity, row_ref.shape[0]), 0)
    hit = jnp.logical_or(place == code_ref[0, 0:1, :], place == code_ref[0, 1:2, :])
    rows = dot_low(hit.astype(wide), row_ref[...], ROW_COL)
    for e in range(count):
        out_ref[e, 0] = rows[e * capacity : (e + 1) * capacity].astype(low)


def send_rows(code, rows, count, capacity):
    blocks, _, row_len = code.shape
    width = rows.shape[1]
    return pl.pallas_call(
        functools.partial(send_kernel, count, capacity),
        grid=(blocks,),
        out_shape=jax.ShapeDtypeStruct((count, blocks, capacity, width), low),
        in_specs=[
            pl.BlockSpec((1, TOP, row_len), lambda j: (j, 0, 0)),
            pl.BlockSpec((row_len, width), lambda j: (j, 0)),
        ],
        out_specs=pl.BlockSpec((count, 1, capacity, width), lambda j: (0, j, 0, 0)),
        cost_estimate=pl.CostEstimate(
            flops=2 * blocks * count * capacity * row_len * width,
            bytes_accessed=2 * blocks * (count * capacity + row_len) * width,
            transcendentals=0,
        ),
        name="send_rows",
    )(code, rows)


def after(value, *others):
    return lax.optimization_barrier((value, *others))[0]


def on_device(
    tokens,
    cotangent,
    w_project,
    w_output,
    norm_gain,
    norm_bias,
    router,
    expert_weights,
    routes,
    keep_mask,
    frozen,
    owner_list,
    attend_master,
    attend_first,
    attend_second,
    attend_left,
    attend_right,
    expert_master,
    expert_first,
    expert_second,
    expert_average,
    expert_basis,
    router_first,
    router_second,
    norm_first,
    norm_second,
):
    seq_dev, row_len, model_width = tokens.shape
    expert_count = lax.axis_size("expert")
    dp_count = lax.axis_size("dp")
    my_index = lax.axis_index("expert")
    row_count = seq_dev * row_len
    capacity = max(2, 5 * row_len * TOP // (4 * expert_count))
    expert_total = router.shape[1]
    slots = expert_total * capacity
    parts = expert_count // seq_dev
    whole = parts == 1
    groups, across = None, None
    if not whole:
        groups = [[p * seq_dev + s for s in range(seq_dev)] for p in range(parts)]
        across = [[p * seq_dev + s for p in range(parts)] for s in range(seq_dev)]

    def swap(value):
        return lax.all_to_all(
            value, "expert", split_axis=0, concat_axis=0, tiled=True, axis_index_groups=groups
        )

    def ring(value):
        size = value.shape[0]
        me = my_index % size
        rows = [lax.dynamic_index_in_dim(value, me, 0, keepdims=False)]
        for shift in range(1, size):
            given = lax.dynamic_index_in_dim(value, (me + shift) % size, 0, keepdims=False)
            moves = [
                (d, d - d % size + (d % size + shift) % size) for d in range(expert_count)
            ]
            rows.append(lax.ppermute(given, "expert", moves))
        return rows

    def ring_place(rows):
        size = len(rows)
        rows = jnp.stack(rows[::-1])
        first = size - 1 - my_index % size
        return lax.dynamic_slice_in_dim(jnp.concatenate([rows, rows]), first, size, 0)

    def sum_dp(value):
        lines = dp_count // 2
        mine = lax.axis_index("dp")
        line, core = mine // 2, mine % 2
        cut = value.reshape(lines, 2, value.shape[0] // dp_count, value.shape[1])
        given = lax.dynamic_index_in_dim(cut, 1 - core, 1, keepdims=False)
        kept = lax.dynamic_index_in_dim(cut, core, 1, keepdims=False)
        got = lax.ppermute(given, "dp", [(d, d ^ 1) for d in range(dp_count)])
        half = (kept.astype(wide) + got.astype(wide)).astype(low)
        total = lax.dynamic_index_in_dim(half, line, 0, keepdims=False).astype(wide)
        for shift in range(1, lines):
            given = lax.dynamic_index_in_dim(half, (line + shift) % lines, 0, keepdims=False)
            moves = [(d, (d + 2 * shift) % dp_count) for d in range(dp_count)]
            total = total + lax.ppermute(given, "dp", moves).astype(wide)
        return total.astype(low)

    def exchange(value):
        return lax.all_to_all(value, "expert", split_axis=0, concat_axis=0, tiled=True)

    token_seq = swap(tokens)
    token_rows = token_seq.reshape(row_count, model_width).astype(wide)

    choice_ids = routes.reshape(seq_dev, row_len * TOP)
    onehot = choice_ids[..., None] == jnp.arange(expert_total, dtype=jnp.int32)
    before_me = jnp.tri(row_len * TOP, k=-1, dtype=low)
    earlier = jnp.einsum("pq,sqe->spe", before_me, onehot.astype(low), preferred_element_type=wide)
    slot_index = jnp.sum(jnp.where(onehot, earlier, 0.0), axis=-1).astype(jnp.int32)
    place = choice_ids * capacity + slot_index
    home_code = jnp.where(keep_mask.reshape(choice_ids.shape) > 0, place, -1 - choice_ids)
    home_code = jnp.swapaxes(home_code.reshape(seq_dev, row_len, TOP), 1, 2)
    code = ring_place(ring(home_code))

    def hits_of(codes):
        return [
            codes[:, k, :, None] == jnp.arange(slots, dtype=jnp.int32) for k in range(TOP)
        ]

    cot_slots = send_rows(
        home_code, cotangent.reshape(row_count, model_width), expert_total, capacity
    )
    cot_back = exchange(after(cot_slots, token_seq))
    normal_one, spread_one = norm_parts(token_rows)
    low_one = (normal_one * norm_gain[0] + norm_bias[0]).astype(low)
    projected = jnp.dot(low_one, w_project, preferred_element_type=wide).astype(low)
    start = ((my_index // seq_dev) * row_count).astype(jnp.int32).reshape(1)
    pairs = HEADS // 2
    if whole:
        key_value, firsts = projected, (0, pairs, 2 * pairs)
    else:
        key_value = lax.all_gather(
            projected[:, model_width:], "expert", axis=0, tiled=True, axis_index_groups=across
        )
        firsts = (0, 0, pairs)
    attended_low, logs = attend(start, projected, key_value, key_value, firsts, whole)
    middle = token_rows + jnp.dot(attended_low, w_output, preferred_element_type=wide)
    normal_two, spread_two = norm_parts(middle)
    low_two = (normal_two * norm_gain[1] + norm_bias[1]).astype(low)

    hits = hits_of(code)
    sending = send_rows(code, low_two, expert_total, capacity)
    received = exchange(after(sending, cot_back))
    cot_rows = jnp.swapaxes(
        cot_back.reshape(parts, seq_dev, seq_dev, capacity, model_width), 1, 2
    ).reshape(-1, model_width)
    w_second = expert_weights[0, 1]
    pulled = jnp.dot(cot_rows, w_second, preferred_element_type=wide).astype(low)
    received = received.reshape(-1, model_width)

    low_two_wide = low_two.astype(wide)
    logits = jnp.dot(low_two_wide, router, precision=precise).reshape(
        seq_dev, 1, row_len, expert_total
    )
    route = jnp.where(code >= 0, code // capacity, -1 - code)
    onehot_four = (route[..., None] == jnp.arange(expert_total, dtype=jnp.int32)).astype(wide)
    gates = jax.nn.softmax(jnp.sum(onehot_four * logits, axis=-1), axis=1)
    gate_slots = sum(
        jnp.sum(jnp.where(hits[k], gates[:, k, :, None], 0.0), axis=1) for k in range(TOP)
    )
    gate_slots = jnp.swapaxes(gate_slots.reshape(seq_dev, expert_total, capacity), 0, 1)
    gate_slots = gate_slots.reshape(expert_total, seq_dev * capacity)
    select = sum(jnp.where(hits[k], gates[:, k, :, None], 0.0) for k in range(TOP)).astype(low)
    select = select.reshape(seq_dev, row_len, expert_total, capacity)
    cot_seq = swap(after(cotangent, received, pulled, gate_slots))
    grad_final = cot_seq.reshape(row_count, model_width).astype(wide)

    activated_low, grad_before, grad_inputs, gate_grad = expert_stage(
        received, pulled, expert_weights
    )
    slot_shape = (expert_count, seq_dev, capacity)
    grad_inputs = grad_inputs.reshape(slot_shape + (model_width,))
    pair_slots = seq_dev * capacity
    traded = trade(
        jnp.concatenate([gate_slots, gate_grad.reshape(expert_count, pair_slots)], axis=1)
    )
    grad_inputs, activated_low, grad_before, traded, _ = lax.optimization_barrier(
        (grad_inputs, activated_low, grad_before, traded, cot_seq)
    )
    gate_rows = traded[:, :pair_slots].reshape(-1, 1)
    gate_grad_home = traded[:, pair_slots:]
    grad_home = exchange(grad_inputs)
    result = jnp.einsum(
        "rf,df->rd", activated_low, w_second, preferred_element_type=wide
    ).astype(low)
    coming_back = exchange(after(result.reshape(slot_shape + (model_width,)), grad_home))
    grad_flat = (gate_rows * cot_rows.astype(wide)).astype(low)
    input_flat = (gate_rows * received.astype(wide)).astype(low)
    grad_first_w = jnp.einsum("rd,rf->df", input_flat, grad_before, preferred_element_type=wide)
    grad_second_w = jnp.einsum("rd,rf->df", grad_flat, activated_low, preferred_element_type=wide)
    flag_value = jnp.sum(
        frozen * (jnp.arange(frozen.shape[0], dtype=jnp.int32) == my_index).astype(jnp.int32)
    )
    trainable = (1 - flag_value).astype(wide)
    expert_stack = jnp.stack(
        [(grad_first_w * trainable).astype(low), (grad_second_w * trainable).astype(low)]
    )
    expert_sum = lax.psum_scatter(expert_stack, "dp", scatter_dimension=2, tiled=True)

    gate_grad_flat = jnp.swapaxes(
        gate_grad_home.reshape(expert_count, seq_dev, capacity), 0, 1
    ).reshape(seq_dev, 1, slots)
    grad_gate = jnp.stack(
        [jnp.sum(jnp.where(hits[k], gate_grad_flat, 0.0), axis=-1) for k in range(TOP)], axis=1
    )
    grad_chosen = gates * (grad_gate - jnp.sum(gates * grad_gate, axis=1, keepdims=True))
    grad_logits = jnp.sum(onehot_four * grad_chosen[..., None], axis=1).reshape(
        row_count, expert_total
    )
    router_local = jnp.dot(low_two_wide.T, grad_logits, precision=precise)
    grad_low_two = jnp.dot(grad_logits, router.T, precision=precise) + jnp.einsum(
        "jtec,ejcd->jtd", select, grad_home, preferred_element_type=wide
    ).reshape(row_count, model_width)
    moved_two, gain_two, bias_two = norm_back(grad_low_two, normal_two, spread_two, norm_gain[1])
    grad_middle = grad_final + moved_two
    grad_branch = grad_middle.astype(low)
    grad_w_output = jnp.einsum("rd,re->de", attended_low, grad_branch, preferred_element_type=wide)
    grad_attended = jnp.einsum("re,de->rd", grad_branch, w_output, preferred_element_type=wide).astype(
        low
    )

    grad_query, grad_keys, grad_values = attend_back(
        start, projected, key_value, key_value, firsts, grad_attended, attended_low, logs, whole
    )
    mixture = jnp.einsum("jtec,ejcd->jtd", select, after(coming_back, grad_query), preferred_element_type=wide)
    output_seq = (
        (middle + mixture.reshape(row_count, model_width))
        .astype(low)
        .reshape(seq_dev, row_len, model_width)
    )
    if not whole:
        grad_keys, grad_values = (
            lax.psum_scatter(
                g, "expert", scatter_dimension=0, tiled=True, axis_index_groups=across
            )
            for g in (grad_keys, grad_values)
        )
    grad_projected = jnp.concatenate([grad_query, grad_keys, grad_values], axis=1)
    grad_low_one = jnp.einsum("re,de->rd", grad_projected, w_project, preferred_element_type=wide)
    moved_one, gain_one, bias_one = norm_back(grad_low_one, normal_one, spread_one, norm_gain[0])
    input_grad = (grad_middle + moved_one).astype(low).reshape(seq_dev, row_len, model_width)
    input_grad = swap(after(input_grad, coming_back))

    grad_w_project = jnp.einsum("rd,re->de", low_one, grad_projected, preferred_element_type=wide)
    grad_norms = jnp.stack([gain_one, gain_two, bias_one, bias_two])
    block_width = attend_master.shape[2]
    expert_grad, expert_master_new, expert_first_new, expert_second_new, expert_average_new = refresh(
        flag_value.astype(jnp.int32).reshape(1),
        expert_basis[0].astype(low),
        expert_sum,
        expert_master,
        expert_first,
        expert_second,
        expert_average,
    )

    slot_range = jnp.arange(expert_count, dtype=jnp.int32)
    which_block = jnp.sum(
        slot_range[None, :] * (owner_list[None, :] == slot_range[:, None]).astype(jnp.int32), axis=1
    )
    small_width = expert_total + 4
    small = jnp.concatenate([router_local, grad_norms.T], axis=1).astype(low)
    small = jnp.pad(small, ((0, 0), (0, 128 - small_width)))
    grad_full = jnp.concatenate(
        [grad_w_project.astype(low), grad_w_output.astype(low), small], axis=1
    )
    my_rows = sum_dp(grad_full)
    my_rows = deal(which_block, my_rows, block_width, expert_count)
    my_rows = after(exchange(after(my_rows, input_grad)), expert_grad)
    my_rows_done = my_rows
    my_rows = jnp.sum(my_rows.astype(wide), axis=0)
    summed = lax.all_gather(my_rows, "dp", axis=0, tiled=True)
    block_grad = summed[:, :block_width]
    small_sum = summed[:, block_width : block_width + small_width]
    router_grad = small_sum[:, :expert_total]
    norm_grad = small_sum[:, expert_total:].T

    left_basis = attend_left[0].astype(low)
    right_basis = attend_right[0].astype(low)
    rotated = dot_low(dot_low(left_basis, block_grad, COL_COL), right_basis, ROW_COL)
    attend_first_new, attend_second_new, direction = adam_move(
        rotated, attend_first[0], attend_second[0]
    )
    stepped = dot_low(dot_low(left_basis, direction, ROW_COL), right_basis, ROW_ROW)
    attend_master_new = attend_master[0] - matrix_rate * stepped

    output = swap(after(output_seq, my_rows_done))

    output = after(output, attend_master_new)

    router_first_new, router_second_new, router_step = adam_move(
        router_grad, router_first, router_second
    )
    router_new = router - matrix_rate * router_step
    norm_params = jnp.concatenate([norm_gain, norm_bias], axis=0)
    norm_first_new, norm_second_new, norm_step = adam_move(norm_grad, norm_first, norm_second)
    norm_new = norm_params - small_rate * norm_step
    return (
        output,
        input_grad,
        norm_grad,
        norm_new,
        norm_first_new,
        norm_second_new,
        router_grad,
        router_new,
        router_first_new,
        router_second_new,
        block_grad[None],
        attend_master_new[None],
        attend_first_new[None],
        attend_second_new[None],
        expert_grad,
        expert_master_new,
        expert_first_new,
        expert_second_new,
        expert_average_new,
    )


def solution(mesh):
    return jax.shard_map(
        on_device,
        mesh=mesh,
        in_specs=(
            P("dp", "expert", None),
            P("dp", "expert", None),
            P(),
            P(),
            P(),
            P(),
            P(),
            P("expert", None, None, None),
            P("dp", "expert", None),
            P("dp", "expert", None),
            P(),
            P(),
            P("expert", None, None),
            P("expert", None, None),
            P("expert", None, None),
            P("expert", None, None),
            P("expert", None, None),
            P("expert", None, None, "dp"),
            P("expert", None, None, "dp"),
            P("expert", None, None, "dp"),
            P("expert", None, None, "dp"),
            P("expert", None, None),
            P(),
            P(),
            P(),
            P(),
        ),
        out_specs=(
            P("dp", "expert", None),
            P("dp", "expert", None),
            P(),
            P(),
            P(),
            P(),
            P(),
            P(),
            P(),
            P(),
            P("expert", None, None),
            P("expert", None, None),
            P("expert", None, None),
            P("expert", None, None),
            P("expert", None, None, "dp"),
            P("expert", None, None, "dp"),
            P("expert", None, None, "dp"),
            P("expert", None, None, "dp"),
            P("expert", None, None, "dp"),
        ),
        check_vma=False,
    )
```

```python
import functools

import jax
import jax.numpy as jnp
from jax import lax
from jax.experimental import pallas as pl
from jax.experimental.pallas import tpu as pltpu
from jax.sharding import PartitionSpec as P


HEADS = 12
HEAD_DIM = 64
TOP = 2
TILE = 256
CHUNK = 512
ROOT = 0.7978845608028654
CUBIC = 0.044715


norm_epsilon = 1e-05
beta_one = 0.9
beta_two = 0.95
adam_epsilon = 1e-08
adam_step = 10.0
matrix_rate = 0.1
small_rate = 0.5
average_keep = 0.9
precise = lax.Precision.HIGHEST
wide = jnp.float32
low = jnp.bfloat16


def norm_parts(values):
    center = values - jnp.mean(values, axis=-1, keepdims=True)
    spread = lax.rsqrt(jnp.mean(center * center, axis=-1, keepdims=True) + norm_epsilon)
    return center * spread, spread


def norm_back(grad, normal, spread, gain_row):
    g = grad * gain_row
    moved = spread * (
        g
        - jnp.mean(g, axis=-1, keepdims=True)
        - normal * jnp.mean(g * normal, axis=-1, keepdims=True)
    )
    return moved, jnp.sum(grad * normal, axis=0), jnp.sum(grad, axis=0)


def adam_move(gradient, first_moment, second_moment):
    first_new = beta_one * first_moment + (1.0 - beta_one) * gradient
    second_new = beta_two * second_moment + (1.0 - beta_two) * gradient * gradient
    direction = (
        first_new
        / (1.0 - beta_one**adam_step)
        / (jnp.sqrt(second_new / (1.0 - beta_two**adam_step)) + adam_epsilon)
    )
    return (first_new, second_new, direction)


def dot_low(a, b, dims):
    return lax.dot_general(a.astype(low), b.astype(low), (dims, ((), ())), preferred_element_type=wide)


ROW_COL = ((1,), (0,))
ROW_ROW = ((1,), (1,))
COL_COL = ((0,), (0,))


def key_pieces(step, tile, key_len, whole):
    if whole:
        return ((0, step * tile, False), (step * tile, (step + 1) * tile, True))
    return ((0, key_len, True),)


def allowed_at(first_query, first_key, tile, key_count):
    rows = lax.broadcasted_iota(jnp.int32, (tile, key_count), 0) + first_query
    columns = lax.broadcasted_iota(jnp.int32, (tile, key_count), 1) + first_key
    return columns <= rows


def attend_kernel(whole, start_ref, q_ref, k_ref, v_ref, out_ref, log_ref):
    rows, lanes = q_ref.shape
    key_len = k_ref.shape[0]
    lane = lax.broadcasted_iota(jnp.int32, (1, lanes), 1)
    for step in range(rows // TILE):
        at = slice(step * TILE, (step + 1) * TILE)
        total, logs = None, []
        for head in range(2):
            mine = (lane // HEAD_DIM) == head
            query = jnp.where(mine, q_ref[at, :] * HEAD_DIM ** (-0.5), 0).astype(low)
            parts = []
            for first, last, masked in key_pieces(step, TILE, key_len, whole):
                if last > first:
                    scores = dot_low(query, k_ref[first:last, :], ROW_ROW)
                    if masked:
                        origin = step * TILE + (0 if whole else start_ref[0])
                        scores = jnp.where(
                            allowed_at(origin, first, TILE, last - first), scores, -1e30
                        )
                    parts.append((first, last, scores))
            top = functools.reduce(
                jnp.maximum, [jnp.max(s, axis=-1, keepdims=True) for _, _, s in parts]
            )
            summed, acc = None, None
            for first, last, scores in parts:
                weights = jnp.exp(scores - top)
                here = jnp.sum(weights, axis=-1, keepdims=True)
                values = jnp.where(mine, v_ref[first:last, :], 0).astype(low)
                add = dot_low(weights, values, ROW_COL)
                summed = here if summed is None else summed + here
                acc = add if acc is None else acc + add
            acc = acc / summed
            total = acc if total is None else total + acc
            logs.append(top + jnp.log(summed))
        out_ref[at, :] = total.astype(out_ref.dtype)
        log_ref[at, :] = jnp.where(lane < HEAD_DIM, logs[0], logs[1])


def attend_back_kernel(
    whole, start_ref, q_ref, k_ref, v_ref, g_ref, a_ref, log_ref, dq_ref, dk_ref, dv_ref, dk_sum, dv_sum
):
    rows, lanes = q_ref.shape
    key_len = k_ref.shape[0]
    lane = lax.broadcasted_iota(jnp.int32, (1, lanes), 1)
    dk_sum[...] = jnp.zeros_like(dk_sum)
    dv_sum[...] = jnp.zeros_like(dv_sum)
    for step in range(rows // TILE):
        at = slice(step * TILE, (step + 1) * TILE)
        grad_all = g_ref[at, :]
        product = grad_all.astype(wide) * a_ref[at, :].astype(wide)
        dq = None
        for head in range(2):
            mine = (lane // HEAD_DIM) == head
            query = jnp.where(mine, q_ref[at, :] * HEAD_DIM ** (-0.5), 0).astype(low)
            grad = jnp.where(mine, grad_all, 0).astype(low)
            delta = jnp.sum(jnp.where(mine, product, 0.0), axis=-1, keepdims=True)
            log_total = log_ref[at, head * HEAD_DIM : head * HEAD_DIM + 1]
            for first, last, masked in key_pieces(step, TILE, key_len, whole):
                if last > first:
                    keys, values = k_ref[first:last, :], v_ref[first:last, :]
                    weights = jnp.exp(dot_low(query, keys, ROW_ROW) - log_total)
                    if masked:
                        origin = step * TILE + (0 if whole else start_ref[0])
                        weights = jnp.where(
                            allowed_at(origin, first, TILE, last - first), weights, 0.0
                        )
                    moved = (weights * (dot_low(grad, values, ROW_ROW) - delta)).astype(low)
                    dv_sum[first:last, :] += dot_low(weights, grad, COL_COL)
                    dk_sum[first:last, :] += dot_low(moved, query, COL_COL)
                    add = dot_low(moved, jnp.where(mine, keys, 0), ROW_COL)
                    dq = add if dq is None else dq + add
        dq_ref[at, :] = (dq * HEAD_DIM ** (-0.5)).astype(low)
    dk_ref[...] = dk_sum[...].astype(low)
    dv_ref[...] = dv_sum[...].astype(low)


def head_block(rows, first):
    return pl.BlockSpec((rows, 2 * HEAD_DIM), lambda pair: (0, first + pair))


def attend(start, queries, keys, values, firsts, whole):
    rows, key_len, pairs = queries.shape[0], keys.shape[0], HEADS // 2
    width = HEADS * HEAD_DIM
    cost = 4 * rows * key_len * width // (2 if whole else 1)
    return pl.pallas_call(
        functools.partial(attend_kernel, whole),
        grid=(pairs,),
        out_shape=(
            jax.ShapeDtypeStruct((rows, width), low),
            jax.ShapeDtypeStruct((rows, width), wide),
        ),
        in_specs=[
            pl.BlockSpec(memory_space=pltpu.SMEM),
            head_block(rows, firsts[0]),
            head_block(key_len, firsts[1]),
            head_block(key_len, firsts[2]),
        ],
        out_specs=(head_block(rows, 0), head_block(rows, 0)),
        cost_estimate=pl.CostEstimate(
            flops=cost, bytes_accessed=12 * rows * width, transcendentals=rows * key_len * HEADS
        ),
        name="attend",
    )(start, queries, keys, values)


def attend_back(start, queries, keys, values, firsts, grads, attended, logs, whole):
    rows, key_len, pairs = queries.shape[0], keys.shape[0], HEADS // 2
    width = HEADS * HEAD_DIM
    cost = 10 * rows * key_len * width // (2 if whole else 1)
    return pl.pallas_call(
        functools.partial(attend_back_kernel, whole),
        grid=(pairs,),
        out_shape=(
            jax.ShapeDtypeStruct((rows, width), low),
            jax.ShapeDtypeStruct((key_len, width), low),
            jax.ShapeDtypeStruct((key_len, width), low),
        ),
        in_specs=[
            pl.BlockSpec(memory_space=pltpu.SMEM),
            head_block(rows, firsts[0]),
            head_block(key_len, firsts[1]),
            head_block(key_len, firsts[2]),
            head_block(rows, 0),
            head_block(rows, 0),
            head_block(rows, 0),
        ],
        out_specs=(head_block(rows, 0), head_block(key_len, 0), head_block(key_len, 0)),
        scratch_shapes=[
            pltpu.VMEM((key_len, 2 * HEAD_DIM), wide),
            pltpu.VMEM((key_len, 2 * HEAD_DIM), wide),
        ],
        cost_estimate=pl.CostEstimate(
            flops=cost, bytes_accessed=20 * rows * width, transcendentals=rows * key_len * HEADS
        ),
        name="attend_back",
    )(start, queries, keys, values, grads, attended, logs)


def expert_kernel(x_ref, u_ref, w_ref, act_ref, grad_ref, input_ref, gate_grad_ref):
    x = x_ref[...]
    inputs, gate_grad = None, None
    hidden = w_ref.shape[3]
    for first in range(0, hidden, CHUNK):
        at = slice(first, first + CHUNK)
        w = w_ref[0, 0, :, at]
        v = dot_low(x, w, ROW_COL)
        u = u_ref[:, at].astype(wide)
        square = v * v
        t = jnp.tanh(ROOT * v * (1.0 + CUBIC * square))
        half = 0.5 * (1.0 + t)
        act = v * half
        slope = half + 0.5 * ROOT * v * (1.0 - t * t) * (1.0 + 3.0 * CUBIC * square)
        grad = (u * slope).astype(low)
        act_ref[:, at] = act.astype(low)
        grad_ref[:, at] = grad
        here = jnp.sum(act * u, axis=-1, keepdims=True)
        add = dot_low(grad, w, ROW_ROW)
        gate_grad = here if gate_grad is None else gate_grad + here
        inputs = add if inputs is None else inputs + add
    input_ref[...] = inputs.astype(low)
    gate_grad_ref[...] = gate_grad


def expert_stage(x, u, w):
    rows, width = x.shape
    hidden = w.shape[3]

    def row_block(columns):
        return pl.BlockSpec((TILE, columns), lambda i: (i, 0))

    return pl.pallas_call(
        expert_kernel,
        grid=(rows // TILE,),
        out_shape=(
            jax.ShapeDtypeStruct((rows, hidden), low),
            jax.ShapeDtypeStruct((rows, hidden), low),
            jax.ShapeDtypeStruct((rows, width), low),
            jax.ShapeDtypeStruct((rows, 1), wide),
        ),
        in_specs=[
            row_block(width),
            row_block(hidden),
            pl.BlockSpec((1, 1, width, hidden), lambda i: (0, 0, 0, 0)),
        ],
        out_specs=(row_block(hidden), row_block(hidden), row_block(width), row_block(1)),
        cost_estimate=pl.CostEstimate(
            flops=4 * rows * width * hidden,
            bytes_accessed=6 * rows * hidden,
            transcendentals=rows * hidden,
        ),
        name="expert_stage",
    )(x, u, w)


def refresh_kernel(count, flag_ref, basis_ref, turned_ref, *refs):
    terms = [functools.reduce(jnp.add, [r[...].astype(wide) for r in refs[i : i + count]]) for i in (0, count)]
    master_ref, first_ref, second_ref, average_ref = refs[2 * count : 2 * count + 4]
    grad_out, master_out, first_out, second_out, average_out = refs[2 * count + 4 :]
    is_frozen = flag_ref[0] > 0
    grad = jnp.where(pl.program_id(0) == 0, terms[0], terms[1])
    grad_out[0, 0] = grad
    first_new, second_new, move = adam_move(
        dot_low(turned_ref[...], grad, ROW_COL), first_ref[0, 0], second_ref[0, 0]
    )
    master_new = master_ref[0, 0] - matrix_rate * dot_low(basis_ref[...], move, ROW_COL)
    master_new = jnp.where(is_frozen, master_ref[0, 0], master_new)
    master_out[0, 0] = master_new
    first_out[0, 0] = jnp.where(is_frozen, first_ref[0, 0], first_new)
    second_out[0, 0] = jnp.where(is_frozen, second_ref[0, 0], second_new)
    average_out[0, 0] = average_keep * average_ref[0, 0] + (1.0 - average_keep) * master_new


def refresh(flag, basis, terms, master, first, second, average):
    count = len(terms[0])
    _, mats, width, columns = master.shape
    step = 256 if columns % 256 == 0 else 128
    block = pl.BlockSpec((1, 1, width, step), lambda i, j: (0, i, 0, j))
    square = pl.BlockSpec((width, width), lambda i, j: (0, 0))
    return pl.pallas_call(
        functools.partial(refresh_kernel, count),
        grid=(mats, columns // step),
        out_shape=(jax.ShapeDtypeStruct(master.shape, wide),) * 5,
        in_specs=[
            pl.BlockSpec(memory_space=pltpu.SMEM),
            square,
            square,
        ]
        + [pl.BlockSpec((width, step), lambda i, j: (0, jnp.where(i == 0, j, columns // step - 1)))]
        * count
        + [pl.BlockSpec((width, step), lambda i, j: (0, jnp.where(i == 0, 0, j)))] * count
        + [block] * 4,
        out_specs=(block,) * 5,
        cost_estimate=pl.CostEstimate(
            flops=4 * mats * width * width * columns,
            bytes_accessed=38 * mats * width * columns,
            transcendentals=0,
        ),
        name="refresh",
    )(flag, basis, basis.T, *terms[0], *terms[1], master, first, second, average)


def deal_kernel(which_ref, block_ref, small_ref, out_ref):
    width = block_ref.shape[1]
    out_ref[0, :, :width] = block_ref[...]
    out_ref[0, :, width:] = small_ref[...]


def deal(which, rows, block_width, count):
    height, total = rows.shape
    extra = total - block_width * count
    if block_width % 128:
        return jnp.stack(
            [
                jnp.concatenate(
                    [
                        lax.dynamic_slice_in_dim(rows, which[s] * block_width, block_width, 1),
                        rows[:, total - extra :],
                    ],
                    axis=1,
                )
                for s in range(count)
            ]
        )
    return pl.pallas_call(
        deal_kernel,
        grid_spec=pltpu.PrefetchScalarGridSpec(
            num_scalar_prefetch=1,
            grid=(count,),
            in_specs=[
                pl.BlockSpec((height, block_width), lambda s, which: (0, which[s])),
                pl.BlockSpec((height, extra), lambda s, which: (0, total // extra - 1)),
            ],
            out_specs=pl.BlockSpec((1, height, block_width + extra), lambda s, which: (s, 0, 0)),
        ),
        out_shape=jax.ShapeDtypeStruct((count, height, block_width + extra), rows.dtype),
        name="deal",
    )(which, rows, rows)


def trade_kernel(count, in_ref, out_ref, landed, send_sem, recv_sem):
    me = lax.axis_index("expert")
    barrier = pltpu.get_barrier_semaphore()
    for shift in range(1, count):
        peer = lax.rem(me + shift, count)
        pl.semaphore_signal(
            barrier, inc=1, device_id={"expert": peer}, device_id_type=pl.DeviceIdType.MESH
        )
    pl.semaphore_wait(barrier, count - 1)
    copies = []
    for shift in range(1, count):
        peer = lax.rem(me + shift, count)
        copy = pltpu.make_async_remote_copy(
            src_ref=in_ref.at[peer],
            dst_ref=landed.at[me],
            send_sem=send_sem.at[shift - 1],
            recv_sem=recv_sem.at[shift - 1],
            device_id={"expert": peer},
            device_id_type=pl.DeviceIdType.MESH,
        )
        copy.start()
        copies.append(copy)
    for shift, copy in zip(range(1, count), copies):
        copy.wait()
        source = lax.rem(me + count - shift, count)
        out_ref[pl.ds(source, 1)] = landed[pl.ds(source, 1)]
    out_ref[pl.ds(me, 1)] = in_ref[pl.ds(me, 1)]


def trade(value):
    count, size = value.shape
    lines = -(-size // 1024) * 8
    padded = jnp.pad(value, ((0, 0), (0, lines * 128 - size))).reshape(count, lines, 128)
    out = pl.pallas_call(
        functools.partial(trade_kernel, count),
        out_shape=jax.ShapeDtypeStruct(padded.shape, padded.dtype),
        in_specs=[pl.BlockSpec(memory_space=pltpu.VMEM)],
        out_specs=pl.BlockSpec(memory_space=pltpu.VMEM),
        scratch_shapes=[
            pltpu.VMEM(padded.shape, padded.dtype),
            pltpu.SemaphoreType.DMA((count - 1,)),
            pltpu.SemaphoreType.DMA((count - 1,)),
        ],
        compiler_params=pltpu.CompilerParams(collective_id=0, has_side_effects=True),
        name="trade",
    )(padded)
    return out.reshape(count, lines * 128)[:, :size]


def send_kernel(count, capacity, code_ref, row_ref, out_ref):
    place = lax.broadcasted_iota(jnp.int32, (count * capacity, row_ref.shape[0]), 0)
    hit = jnp.logical_or(place == code_ref[0, 0:1, :], place == code_ref[0, 1:2, :])
    rows = dot_low(hit.astype(wide), row_ref[...], ROW_COL)
    for e in range(count):
        out_ref[e, 0] = rows[e * capacity : (e + 1) * capacity].astype(low)


def send_rows(code, rows, count, capacity):
    blocks, _, row_len = code.shape
    width = rows.shape[1]
    return pl.pallas_call(
        functools.partial(send_kernel, count, capacity),
        grid=(blocks,),
        out_shape=jax.ShapeDtypeStruct((count, blocks, capacity, width), low),
        in_specs=[
            pl.BlockSpec((1, TOP, row_len), lambda j: (j, 0, 0)),
            pl.BlockSpec((row_len, width), lambda j: (j, 0)),
        ],
        out_specs=pl.BlockSpec((count, 1, capacity, width), lambda j: (0, j, 0, 0)),
        cost_estimate=pl.CostEstimate(
            flops=2 * blocks * count * capacity * row_len * width,
            bytes_accessed=2 * blocks * (count * capacity + row_len) * width,
            transcendentals=0,
        ),
        name="send_rows",
    )(code, rows)


def after(value, *others):
    return lax.optimization_barrier((value, *others))[0]


def on_device(
    tokens,
    cotangent,
    w_project,
    w_output,
    norm_gain,
    norm_bias,
    router,
    expert_weights,
    routes,
    keep_mask,
    frozen,
    owner_list,
    attend_master,
    attend_first,
    attend_second,
    attend_left,
    attend_right,
    expert_master,
    expert_first,
    expert_second,
    expert_average,
    expert_basis,
    router_first,
    router_second,
    norm_first,
    norm_second,
):
    seq_dev, row_len, model_width = tokens.shape
    expert_count = lax.axis_size("expert")
    dp_count = lax.axis_size("dp")
    my_index = lax.axis_index("expert")
    row_count = seq_dev * row_len
    capacity = max(2, 5 * row_len * TOP // (4 * expert_count))
    expert_total = router.shape[1]
    slots = expert_total * capacity
    parts = expert_count // seq_dev
    whole = parts == 1
    groups, across = None, None
    if not whole:
        groups = [[p * seq_dev + s for s in range(seq_dev)] for p in range(parts)]
        across = [[p * seq_dev + s for p in range(parts)] for s in range(seq_dev)]

    def swap(value):
        return lax.all_to_all(
            value, "expert", split_axis=0, concat_axis=0, tiled=True, axis_index_groups=groups
        )

    def ring(value):
        size = value.shape[0]
        me = my_index % size
        rows = [lax.dynamic_index_in_dim(value, me, 0, keepdims=False)]
        for shift in range(1, size):
            given = lax.dynamic_index_in_dim(value, (me + shift) % size, 0, keepdims=False)
            moves = [
                (d, d - d % size + (d % size + shift) % size) for d in range(expert_count)
            ]
            rows.append(lax.ppermute(given, "expert", moves))
        return rows

    def ring_place(rows):
        size = len(rows)
        rows = jnp.stack(rows[::-1])
        first = size - 1 - my_index % size
        return lax.dynamic_slice_in_dim(jnp.concatenate([rows, rows]), first, size, 0)

    lines = dp_count // 2
    line = lax.axis_index("dp") // 2
    core = lax.axis_index("dp") % 2

    def dp_move(value, shift):
        return lax.ppermute(value, "dp", [(d, (d + 2 * shift) % dp_count) for d in range(dp_count)])

    def other_core(value):
        return lax.ppermute(value, "dp", [(d, d ^ 1) for d in range(dp_count)])

    def cut_dp(value, axis, side):
        size = value.shape[axis] // dp_count
        return [
            lax.dynamic_slice_in_dim(
                value, ((line + shift) % lines * 2 + side) * size, size, axis
            )
            for shift in range(lines)
        ]

    def halve(value, axis, given):
        return [
            (mine.astype(wide) + other_core(theirs).astype(wide)).astype(low)
            for mine, theirs in zip(cut_dp(value, axis, core), given)
        ]

    def spread(half):
        return [half[0]] + [dp_move(half[shift], shift) for shift in range(1, lines)]

    def gather_dp(value):
        rows = jnp.stack([value] + [dp_move(value, shift) for shift in range(1, lines)])
        others = other_core(rows)
        out = jnp.zeros((dp_count,) + value.shape, value.dtype)
        for shift in range(lines):
            first = (line + lines - shift) % lines * 2
            out = lax.dynamic_update_index_in_dim(out, rows[shift], first + core, 0)
            out = lax.dynamic_update_index_in_dim(out, others[shift], first + 1 - core, 0)
        return out.reshape((-1,) + value.shape[1:])

    def exchange(value):
        return lax.all_to_all(value, "expert", split_axis=0, concat_axis=0, tiled=True)

    token_seq = swap(tokens)
    token_rows = token_seq.reshape(row_count, model_width).astype(wide)

    choice_ids = routes.reshape(seq_dev, row_len * TOP)
    onehot = choice_ids[..., None] == jnp.arange(expert_total, dtype=jnp.int32)
    before_me = jnp.tri(row_len * TOP, k=-1, dtype=low)
    earlier = jnp.einsum("pq,sqe->spe", before_me, onehot.astype(low), preferred_element_type=wide)
    slot_index = jnp.sum(jnp.where(onehot, earlier, 0.0), axis=-1).astype(jnp.int32)
    place = choice_ids * capacity + slot_index
    home_code = jnp.where(keep_mask.reshape(choice_ids.shape) > 0, place, -1 - choice_ids)
    home_code = jnp.swapaxes(home_code.reshape(seq_dev, row_len, TOP), 1, 2)
    code = ring_place(ring(home_code))

    def hits_of(codes):
        return [
            codes[:, k, :, None] == jnp.arange(slots, dtype=jnp.int32) for k in range(TOP)
        ]

    cot_slots = send_rows(
        home_code, cotangent.reshape(row_count, model_width), expert_total, capacity
    )
    cot_back = exchange(after(cot_slots, token_seq))
    normal_one, spread_one = norm_parts(token_rows)
    low_one = (normal_one * norm_gain[0] + norm_bias[0]).astype(low)
    projected = jnp.dot(low_one, w_project, preferred_element_type=wide).astype(low)
    start = ((my_index // seq_dev) * row_count).astype(jnp.int32).reshape(1)
    pairs = HEADS // 2
    if whole:
        key_value, firsts = projected, (0, pairs, 2 * pairs)
    else:
        key_value = lax.all_gather(
            projected[:, model_width:], "expert", axis=0, tiled=True, axis_index_groups=across
        )
        firsts = (0, 0, pairs)
    attended_low, logs = attend(start, projected, key_value, key_value, firsts, whole)
    middle = token_rows + jnp.dot(attended_low, w_output, preferred_element_type=wide)
    normal_two, spread_two = norm_parts(middle)
    low_two = (normal_two * norm_gain[1] + norm_bias[1]).astype(low)

    hits = hits_of(code)
    sending = send_rows(code, low_two, expert_total, capacity)
    received = exchange(after(sending, cot_back))
    cot_rows = jnp.swapaxes(
        cot_back.reshape(parts, seq_dev, seq_dev, capacity, model_width), 1, 2
    ).reshape(-1, model_width)
    w_second = expert_weights[0, 1]
    pulled = jnp.dot(cot_rows, w_second, preferred_element_type=wide).astype(low)
    received = received.reshape(-1, model_width)

    low_two_wide = low_two.astype(wide)
    logits = jnp.dot(low_two_wide, router, precision=precise).reshape(
        seq_dev, 1, row_len, expert_total
    )
    route = jnp.where(code >= 0, code // capacity, -1 - code)
    onehot_four = (route[..., None] == jnp.arange(expert_total, dtype=jnp.int32)).astype(wide)
    gates = jax.nn.softmax(jnp.sum(onehot_four * logits, axis=-1), axis=1)
    gate_slots = sum(
        jnp.sum(jnp.where(hits[k], gates[:, k, :, None], 0.0), axis=1) for k in range(TOP)
    )
    gate_slots = jnp.swapaxes(gate_slots.reshape(seq_dev, expert_total, capacity), 0, 1)
    gate_slots = gate_slots.reshape(expert_total, seq_dev * capacity)
    select = sum(jnp.where(hits[k], gates[:, k, :, None], 0.0) for k in range(TOP)).astype(low)
    select = select.reshape(seq_dev, row_len, expert_total, capacity)
    cot_seq = swap(after(cotangent, received, pulled, gate_slots))
    grad_final = cot_seq.reshape(row_count, model_width).astype(wide)

    activated_low, grad_before, grad_inputs, gate_grad = expert_stage(
        received, pulled, expert_weights
    )
    slot_shape = (expert_count, seq_dev, capacity)
    grad_inputs = grad_inputs.reshape(slot_shape + (model_width,))
    pair_slots = seq_dev * capacity
    traded = trade(
        jnp.concatenate([gate_slots, gate_grad.reshape(expert_count, pair_slots)], axis=1)
    )
    grad_inputs, activated_low, grad_before, traded, _ = lax.optimization_barrier(
        (grad_inputs, activated_low, grad_before, traded, cot_seq)
    )
    gate_rows = traded[:, :pair_slots].reshape(-1, 1)
    gate_grad_home = traded[:, pair_slots:]
    grad_home = exchange(grad_inputs)
    result = jnp.einsum(
        "rf,df->rd", activated_low, w_second, preferred_element_type=wide
    ).astype(low)
    grad_flat = (gate_rows * cot_rows.astype(wide)).astype(low)
    input_flat = (gate_rows * received.astype(wide)).astype(low)
    grad_first_w = jnp.einsum("rd,rf->df", input_flat, grad_before, preferred_element_type=wide)
    grad_second_w = jnp.einsum("rd,rf->df", grad_flat, activated_low, preferred_element_type=wide)
    flag_value = jnp.sum(
        frozen * (jnp.arange(frozen.shape[0], dtype=jnp.int32) == my_index).astype(jnp.int32)
    )
    trainable = (1 - flag_value).astype(wide)
    expert_grads = [(grad * trainable).astype(low) for grad in (grad_first_w, grad_second_w)]
    expert_given = [cut_dp(grad, 1, 1 - core) for grad in expert_grads]
    coming_back = exchange(after(result.reshape(slot_shape + (model_width,)), grad_home, expert_given))
    expert_half = [halve(grad, 1, given) for grad, given in zip(expert_grads, expert_given)]
    expert_terms = [spread(half) for half in expert_half]

    gate_grad_flat = jnp.swapaxes(
        gate_grad_home.reshape(expert_count, seq_dev, capacity), 0, 1
    ).reshape(seq_dev, 1, slots)
    grad_gate = jnp.stack(
        [jnp.sum(jnp.where(hits[k], gate_grad_flat, 0.0), axis=-1) for k in range(TOP)], axis=1
    )
    grad_chosen = gates * (grad_gate - jnp.sum(gates * grad_gate, axis=1, keepdims=True))
    grad_logits = jnp.sum(onehot_four * grad_chosen[..., None], axis=1).reshape(
        row_count, expert_total
    )
    router_local = jnp.dot(low_two_wide.T, grad_logits, precision=precise)
    grad_low_two = jnp.dot(grad_logits, router.T, precision=precise) + jnp.einsum(
        "jtec,ejcd->jtd", select, grad_home, preferred_element_type=wide
    ).reshape(row_count, model_width)
    moved_two, gain_two, bias_two = norm_back(grad_low_two, normal_two, spread_two, norm_gain[1])
    grad_middle = grad_final + moved_two
    grad_branch = grad_middle.astype(low)
    grad_w_output = jnp.einsum("rd,re->de", attended_low, grad_branch, preferred_element_type=wide)
    grad_attended = jnp.einsum("re,de->rd", grad_branch, w_output, preferred_element_type=wide).astype(
        low
    )

    grad_attended = after(grad_attended, expert_half)
    grad_query, grad_keys, grad_values = attend_back(
        start, projected, key_value, key_value, firsts, grad_attended, attended_low, logs, whole
    )
    mixture = jnp.einsum("jtec,ejcd->jtd", select, after(coming_back, grad_query), preferred_element_type=wide)
    output_seq = (
        (middle + mixture.reshape(row_count, model_width))
        .astype(low)
        .reshape(seq_dev, row_len, model_width)
    )
    if not whole:
        grad_keys, grad_values = (
            lax.psum_scatter(
                g, "expert", scatter_dimension=0, tiled=True, axis_index_groups=across
            )
            for g in (grad_keys, grad_values)
        )
    grad_projected = jnp.concatenate([grad_query, grad_keys, grad_values], axis=1)
    grad_low_one = jnp.einsum("re,de->rd", grad_projected, w_project, preferred_element_type=wide)
    moved_one, gain_one, bias_one = norm_back(grad_low_one, normal_one, spread_one, norm_gain[0])
    input_grad = (grad_middle + moved_one).astype(low).reshape(seq_dev, row_len, model_width)
    input_grad = swap(after(input_grad, coming_back, expert_terms))

    grad_w_project = jnp.einsum("rd,re->de", low_one, grad_projected, preferred_element_type=wide)
    grad_norms = jnp.stack([gain_one, gain_two, bias_one, bias_two])
    block_width = attend_master.shape[2]
    expert_grad, expert_master_new, expert_first_new, expert_second_new, expert_average_new = refresh(
        flag_value.astype(jnp.int32).reshape(1),
        expert_basis[0].astype(low),
        expert_terms,
        expert_master,
        expert_first,
        expert_second,
        expert_average,
    )

    slot_range = jnp.arange(expert_count, dtype=jnp.int32)
    which_block = jnp.sum(
        slot_range[None, :] * (owner_list[None, :] == slot_range[:, None]).astype(jnp.int32), axis=1
    )
    small_width = expert_total + 4
    small = jnp.concatenate([router_local, grad_norms.T], axis=1).astype(low)
    small = jnp.pad(small, ((0, 0), (0, 128 - small_width)))
    grad_full = jnp.concatenate(
        [grad_w_project.astype(low), grad_w_output.astype(low), small], axis=1
    )
    half_rows = halve(grad_full, 0, cut_dp(grad_full, 0, 1 - core))
    my_rows = sum(term.astype(wide) for term in spread(half_rows)).astype(low)
    my_rows = deal(which_block, my_rows, block_width, expert_count)
    my_rows = after(exchange(after(my_rows, input_grad)), expert_grad)
    my_rows_done = my_rows
    my_rows = jnp.sum(my_rows.astype(wide), axis=0)
    summed = gather_dp(my_rows.astype(low)).astype(wide)
    block_grad = summed[:, :block_width]
    small_sum = summed[:, block_width : block_width + small_width]
    router_grad = small_sum[:, :expert_total]
    norm_grad = small_sum[:, expert_total:].T

    left_basis = attend_left[0].astype(low)
    right_basis = attend_right[0].astype(low)
    rotated = dot_low(dot_low(left_basis, block_grad, COL_COL), right_basis, ROW_COL)
    attend_first_new, attend_second_new, direction = adam_move(
        rotated, attend_first[0], attend_second[0]
    )
    stepped = dot_low(dot_low(left_basis, direction, ROW_COL), right_basis, ROW_ROW)
    attend_master_new = attend_master[0] - matrix_rate * stepped

    output = swap(after(output_seq, my_rows_done))

    output = after(output, attend_master_new)

    router_first_new, router_second_new, router_step = adam_move(
        router_grad, router_first, router_second
    )
    router_new = router - matrix_rate * router_step
    norm_params = jnp.concatenate([norm_gain, norm_bias], axis=0)
    norm_first_new, norm_second_new, norm_step = adam_move(norm_grad, norm_first, norm_second)
    norm_new = norm_params - small_rate * norm_step
    return (
        output,
        input_grad,
        norm_grad,
        norm_new,
        norm_first_new,
        norm_second_new,
        router_grad,
        router_new,
        router_first_new,
        router_second_new,
        block_grad[None],
        attend_master_new[None],
        attend_first_new[None],
        attend_second_new[None],
        expert_grad,
        expert_master_new,
        expert_first_new,
        expert_second_new,
        expert_average_new,
    )


def solution(mesh):
    return jax.shard_map(
        on_device,
        mesh=mesh,
        in_specs=(
            P("dp", "expert", None),
            P("dp", "expert", None),
            P(),
            P(),
            P(),
            P(),
            P(),
            P("expert", None, None, None),
            P("dp", "expert", None),
            P("dp", "expert", None),
            P(),
            P(),
            P("expert", None, None),
            P("expert", None, None),
            P("expert", None, None),
            P("expert", None, None),
            P("expert", None, None),
            P("expert", None, None, "dp"),
            P("expert", None, None, "dp"),
            P("expert", None, None, "dp"),
            P("expert", None, None, "dp"),
            P("expert", None, None),
            P(),
            P(),
            P(),
            P(),
        ),
        out_specs=(
            P("dp", "expert", None),
            P("dp", "expert", None),
            P(),
            P(),
            P(),
            P(),
            P(),
            P(),
            P(),
            P(),
            P("expert", None, None),
            P("expert", None, None),
            P("expert", None, None),
            P("expert", None, None),
            P("expert", None, None, "dp"),
            P("expert", None, None, "dp"),
            P("expert", None, None, "dp"),
            P("expert", None, None, "dp"),
            P("expert", None, None, "dp"),
        ),
        check_vma=False,
    )
```

```python
import functools

import jax
import jax.numpy as jnp
from jax import lax
from jax.experimental import pallas as pl
from jax.experimental.pallas import tpu as pltpu
from jax.sharding import PartitionSpec as P


HEADS = 12
HEAD_DIM = 64
TOP = 2
TILE = 256
CHUNK = 512
ROOT = 0.7978845608028654
CUBIC = 0.044715


norm_epsilon = 1e-05
beta_one = 0.9
beta_two = 0.95
adam_epsilon = 1e-08
adam_step = 10.0
matrix_rate = 0.1
small_rate = 0.5
average_keep = 0.9
precise = lax.Precision.HIGHEST
wide = jnp.float32
low = jnp.bfloat16


def norm_parts(values):
    center = values - jnp.mean(values, axis=-1, keepdims=True)
    spread = lax.rsqrt(jnp.mean(center * center, axis=-1, keepdims=True) + norm_epsilon)
    return center * spread, spread


def norm_back(grad, normal, spread, gain_row):
    g = grad * gain_row
    moved = spread * (
        g
        - jnp.mean(g, axis=-1, keepdims=True)
        - normal * jnp.mean(g * normal, axis=-1, keepdims=True)
    )
    return moved, jnp.sum(grad * normal, axis=0), jnp.sum(grad, axis=0)


def adam_move(gradient, first_moment, second_moment):
    first_new = beta_one * first_moment + (1.0 - beta_one) * gradient
    second_new = beta_two * second_moment + (1.0 - beta_two) * gradient * gradient
    direction = (
        first_new
        / (1.0 - beta_one**adam_step)
        / (jnp.sqrt(second_new / (1.0 - beta_two**adam_step)) + adam_epsilon)
    )
    return (first_new, second_new, direction)


def dot_low(a, b, dims):
    return lax.dot_general(a.astype(low), b.astype(low), (dims, ((), ())), preferred_element_type=wide)


ROW_COL = ((1,), (0,))
ROW_ROW = ((1,), (1,))
COL_COL = ((0,), (0,))


def key_pieces(step, tile, key_len, whole):
    if whole:
        return ((0, step * tile, False), (step * tile, (step + 1) * tile, True))
    return ((0, key_len, True),)


def allowed_at(first_query, first_key, tile, key_count):
    rows = lax.broadcasted_iota(jnp.int32, (tile, key_count), 0) + first_query
    columns = lax.broadcasted_iota(jnp.int32, (tile, key_count), 1) + first_key
    return columns <= rows


def attend_kernel(whole, start_ref, q_ref, k_ref, v_ref, out_ref, log_ref):
    rows, lanes = q_ref.shape
    key_len = k_ref.shape[0]
    lane = lax.broadcasted_iota(jnp.int32, (1, lanes), 1)
    for step in range(rows // TILE):
        at = slice(step * TILE, (step + 1) * TILE)
        total, logs = None, []
        for head in range(2):
            mine = (lane // HEAD_DIM) == head
            query = jnp.where(mine, q_ref[at, :] * HEAD_DIM ** (-0.5), 0).astype(low)
            parts = []
            for first, last, masked in key_pieces(step, TILE, key_len, whole):
                if last > first:
                    scores = dot_low(query, k_ref[first:last, :], ROW_ROW)
                    if masked:
                        origin = step * TILE + (0 if whole else start_ref[0])
                        scores = jnp.where(
                            allowed_at(origin, first, TILE, last - first), scores, -1e30
                        )
                    parts.append((first, last, scores))
            top = functools.reduce(
                jnp.maximum, [jnp.max(s, axis=-1, keepdims=True) for _, _, s in parts]
            )
            summed, acc = None, None
            for first, last, scores in parts:
                weights = jnp.exp(scores - top)
                here = jnp.sum(weights, axis=-1, keepdims=True)
                values = jnp.where(mine, v_ref[first:last, :], 0).astype(low)
                add = dot_low(weights, values, ROW_COL)
                summed = here if summed is None else summed + here
                acc = add if acc is None else acc + add
            acc = acc / summed
            total = acc if total is None else total + acc
            logs.append(top + jnp.log(summed))
        out_ref[at, :] = total.astype(out_ref.dtype)
        log_ref[at, :] = jnp.where(lane < HEAD_DIM, logs[0], logs[1])


def attend_back_kernel(
    whole, start_ref, q_ref, k_ref, v_ref, g_ref, a_ref, log_ref, dq_ref, dk_ref, dv_ref, dk_sum, dv_sum
):
    rows, lanes = q_ref.shape
    key_len = k_ref.shape[0]
    lane = lax.broadcasted_iota(jnp.int32, (1, lanes), 1)
    dk_sum[...] = jnp.zeros_like(dk_sum)
    dv_sum[...] = jnp.zeros_like(dv_sum)
    for step in range(rows // TILE):
        at = slice(step * TILE, (step + 1) * TILE)
        grad_all = g_ref[at, :]
        product = grad_all.astype(wide) * a_ref[at, :].astype(wide)
        dq = None
        for head in range(2):
            mine = (lane // HEAD_DIM) == head
            query = jnp.where(mine, q_ref[at, :] * HEAD_DIM ** (-0.5), 0).astype(low)
            grad = jnp.where(mine, grad_all, 0).astype(low)
            delta = jnp.sum(jnp.where(mine, product, 0.0), axis=-1, keepdims=True)
            log_total = log_ref[at, head * HEAD_DIM : head * HEAD_DIM + 1]
            for first, last, masked in key_pieces(step, TILE, key_len, whole):
                if last > first:
                    keys, values = k_ref[first:last, :], v_ref[first:last, :]
                    weights = jnp.exp(dot_low(query, keys, ROW_ROW) - log_total)
                    if masked:
                        origin = step * TILE + (0 if whole else start_ref[0])
                        weights = jnp.where(
                            allowed_at(origin, first, TILE, last - first), weights, 0.0
                        )
                    moved = (weights * (dot_low(grad, values, ROW_ROW) - delta)).astype(low)
                    dv_sum[first:last, :] += dot_low(weights, grad, COL_COL)
                    dk_sum[first:last, :] += dot_low(moved, query, COL_COL)
                    add = dot_low(moved, jnp.where(mine, keys, 0), ROW_COL)
                    dq = add if dq is None else dq + add
        dq_ref[at, :] = (dq * HEAD_DIM ** (-0.5)).astype(low)
    dk_ref[...] = dk_sum[...].astype(low)
    dv_ref[...] = dv_sum[...].astype(low)


def head_block(rows, first):
    return pl.BlockSpec((rows, 2 * HEAD_DIM), lambda pair: (0, first + pair))


def attend(start, queries, keys, values, firsts, whole):
    rows, key_len, pairs = queries.shape[0], keys.shape[0], HEADS // 2
    width = HEADS * HEAD_DIM
    cost = 4 * rows * key_len * width // (2 if whole else 1)
    return pl.pallas_call(
        functools.partial(attend_kernel, whole),
        grid=(pairs,),
        out_shape=(
            jax.ShapeDtypeStruct((rows, width), low),
            jax.ShapeDtypeStruct((rows, width), wide),
        ),
        in_specs=[
            pl.BlockSpec(memory_space=pltpu.SMEM),
            head_block(rows, firsts[0]),
            head_block(key_len, firsts[1]),
            head_block(key_len, firsts[2]),
        ],
        out_specs=(head_block(rows, 0), head_block(rows, 0)),
        cost_estimate=pl.CostEstimate(
            flops=cost, bytes_accessed=12 * rows * width, transcendentals=rows * key_len * HEADS
        ),
        name="attend",
    )(start, queries, keys, values)


def attend_back(start, queries, keys, values, firsts, grads, attended, logs, whole):
    rows, key_len, pairs = queries.shape[0], keys.shape[0], HEADS // 2
    width = HEADS * HEAD_DIM
    cost = 10 * rows * key_len * width // (2 if whole else 1)
    return pl.pallas_call(
        functools.partial(attend_back_kernel, whole),
        grid=(pairs,),
        out_shape=(
            jax.ShapeDtypeStruct((rows, width), low),
            jax.ShapeDtypeStruct((key_len, width), low),
            jax.ShapeDtypeStruct((key_len, width), low),
        ),
        in_specs=[
            pl.BlockSpec(memory_space=pltpu.SMEM),
            head_block(rows, firsts[0]),
            head_block(key_len, firsts[1]),
            head_block(key_len, firsts[2]),
            head_block(rows, 0),
            head_block(rows, 0),
            head_block(rows, 0),
        ],
        out_specs=(head_block(rows, 0), head_block(key_len, 0), head_block(key_len, 0)),
        scratch_shapes=[
            pltpu.VMEM((key_len, 2 * HEAD_DIM), wide),
            pltpu.VMEM((key_len, 2 * HEAD_DIM), wide),
        ],
        cost_estimate=pl.CostEstimate(
            flops=cost, bytes_accessed=20 * rows * width, transcendentals=rows * key_len * HEADS
        ),
        name="attend_back",
    )(start, queries, keys, values, grads, attended, logs)


def expert_kernel(x_ref, u_ref, w_ref, act_ref, grad_ref, input_ref, gate_grad_ref):
    x = x_ref[...]
    inputs, gate_grad = None, None
    hidden = w_ref.shape[3]
    for first in range(0, hidden, CHUNK):
        at = slice(first, first + CHUNK)
        w = w_ref[0, 0, :, at]
        v = dot_low(x, w, ROW_COL)
        u = u_ref[:, at].astype(wide)
        square = v * v
        t = jnp.tanh(ROOT * v * (1.0 + CUBIC * square))
        half = 0.5 * (1.0 + t)
        act = v * half
        slope = half + 0.5 * ROOT * v * (1.0 - t * t) * (1.0 + 3.0 * CUBIC * square)
        grad = (u * slope).astype(low)
        act_ref[:, at] = act.astype(low)
        grad_ref[:, at] = grad
        here = jnp.sum(act * u, axis=-1, keepdims=True)
        add = dot_low(grad, w, ROW_ROW)
        gate_grad = here if gate_grad is None else gate_grad + here
        inputs = add if inputs is None else inputs + add
    input_ref[...] = inputs.astype(low)
    gate_grad_ref[0] = gate_grad.T


def expert_stage(x, u, w):
    rows, width = x.shape
    hidden = w.shape[3]

    def row_block(columns):
        return pl.BlockSpec((TILE, columns), lambda i: (i, 0))

    return pl.pallas_call(
        expert_kernel,
        grid=(rows // TILE,),
        out_shape=(
            jax.ShapeDtypeStruct((rows, hidden), low),
            jax.ShapeDtypeStruct((rows, hidden), low),
            jax.ShapeDtypeStruct((rows, width), low),
            jax.ShapeDtypeStruct((rows // TILE, 1, TILE), wide),
        ),
        in_specs=[
            row_block(width),
            row_block(hidden),
            pl.BlockSpec((1, 1, width, hidden), lambda i: (0, 0, 0, 0)),
        ],
        out_specs=(
            row_block(hidden),
            row_block(hidden),
            row_block(width),
            pl.BlockSpec((1, 1, TILE), lambda i: (i, 0, 0)),
        ),
        cost_estimate=pl.CostEstimate(
            flops=4 * rows * width * hidden,
            bytes_accessed=6 * rows * hidden,
            transcendentals=rows * hidden,
        ),
        name="expert_stage",
    )(x, u, w)


def refresh_kernel(count, flag_ref, basis_ref, turned_ref, *refs):
    terms = [functools.reduce(jnp.add, [r[...].astype(wide) for r in refs[i : i + count]]) for i in (0, count)]
    master_ref, first_ref, second_ref, average_ref = refs[2 * count : 2 * count + 4]
    grad_out, master_out, first_out, second_out, average_out = refs[2 * count + 4 :]
    is_frozen = flag_ref[0] > 0
    grad = jnp.where(pl.program_id(0) == 0, terms[0], terms[1])
    grad_out[0, 0] = grad
    first_new, second_new, move = adam_move(
        dot_low(turned_ref[...], grad, ROW_COL), first_ref[0, 0], second_ref[0, 0]
    )
    master_new = master_ref[0, 0] - matrix_rate * dot_low(basis_ref[...], move, ROW_COL)
    master_new = jnp.where(is_frozen, master_ref[0, 0], master_new)
    master_out[0, 0] = master_new
    first_out[0, 0] = jnp.where(is_frozen, first_ref[0, 0], first_new)
    second_out[0, 0] = jnp.where(is_frozen, second_ref[0, 0], second_new)
    average_out[0, 0] = average_keep * average_ref[0, 0] + (1.0 - average_keep) * master_new


def refresh(flag, basis, terms, master, first, second, average):
    count = len(terms[0])
    _, mats, width, columns = master.shape
    step = 256 if columns % 256 == 0 else 128
    block = pl.BlockSpec((1, 1, width, step), lambda i, j: (0, i, 0, j))
    square = pl.BlockSpec((width, width), lambda i, j: (0, 0))
    return pl.pallas_call(
        functools.partial(refresh_kernel, count),
        grid=(mats, columns // step),
        out_shape=(jax.ShapeDtypeStruct(master.shape, wide),) * 5,
        in_specs=[
            pl.BlockSpec(memory_space=pltpu.SMEM),
            square,
            square,
        ]
        + [pl.BlockSpec((width, step), lambda i, j: (0, jnp.where(i == 0, j, columns // step - 1)))]
        * count
        + [pl.BlockSpec((width, step), lambda i, j: (0, jnp.where(i == 0, 0, j)))] * count
        + [block] * 4,
        out_specs=(block,) * 5,
        cost_estimate=pl.CostEstimate(
            flops=4 * mats * width * width * columns,
            bytes_accessed=38 * mats * width * columns,
            transcendentals=0,
        ),
        name="refresh",
    )(flag, basis, basis.T, *terms[0], *terms[1], master, first, second, average)


def deal_kernel(which_ref, block_ref, small_ref, out_ref):
    height = block_ref.shape[0]
    out_ref[0, :height] = block_ref[...]
    out_ref[0, height:] = small_ref[...]


def deal(which, rows, small, count):
    height, extra, block_width = rows.shape[0], small.shape[0], small.shape[1]
    if block_width % 128:
        return jnp.stack(
            [
                jnp.concatenate(
                    [
                        lax.dynamic_slice_in_dim(rows, which[s] * block_width, block_width, 1),
                        small,
                    ]
                )
                for s in range(count)
            ]
        )
    return pl.pallas_call(
        deal_kernel,
        grid_spec=pltpu.PrefetchScalarGridSpec(
            num_scalar_prefetch=1,
            grid=(count,),
            in_specs=[
                pl.BlockSpec((height, block_width), lambda s, which: (0, which[s])),
                pl.BlockSpec((extra, block_width), lambda s, which: (0, 0)),
            ],
            out_specs=pl.BlockSpec((1, height + extra, block_width), lambda s, which: (s, 0, 0)),
        ),
        out_shape=jax.ShapeDtypeStruct((count, height + extra, block_width), rows.dtype),
        name="deal",
    )(which, rows, small)


def trade_kernel(count, in_ref, out_ref, landed, send_sem, recv_sem):
    me = lax.axis_index("expert")
    barrier = pltpu.get_barrier_semaphore()
    for shift in range(1, count):
        peer = lax.rem(me + shift, count)
        pl.semaphore_signal(
            barrier, inc=1, device_id={"expert": peer}, device_id_type=pl.DeviceIdType.MESH
        )
    pl.semaphore_wait(barrier, count - 1)
    copies = []
    for shift in range(1, count):
        peer = lax.rem(me + shift, count)
        copy = pltpu.make_async_remote_copy(
            src_ref=in_ref.at[peer],
            dst_ref=landed.at[me],
            send_sem=send_sem.at[shift - 1],
            recv_sem=recv_sem.at[shift - 1],
            device_id={"expert": peer},
            device_id_type=pl.DeviceIdType.MESH,
        )
        copy.start()
        copies.append(copy)
    for shift, copy in zip(range(1, count), copies):
        copy.wait()
        source = lax.rem(me + count - shift, count)
        out_ref[pl.ds(source, 1)] = landed[pl.ds(source, 1)]
    out_ref[pl.ds(me, 1)] = in_ref[pl.ds(me, 1)]


def trade(value):
    count, size = value.shape
    lines = -(-size // 1024) * 8
    padded = jnp.pad(value, ((0, 0), (0, lines * 128 - size))).reshape(count, lines, 128)
    out = pl.pallas_call(
        functools.partial(trade_kernel, count),
        out_shape=jax.ShapeDtypeStruct(padded.shape, padded.dtype),
        in_specs=[pl.BlockSpec(memory_space=pltpu.VMEM)],
        out_specs=pl.BlockSpec(memory_space=pltpu.VMEM),
        scratch_shapes=[
            pltpu.VMEM(padded.shape, padded.dtype),
            pltpu.SemaphoreType.DMA((count - 1,)),
            pltpu.SemaphoreType.DMA((count - 1,)),
        ],
        compiler_params=pltpu.CompilerParams(collective_id=0, has_side_effects=True),
        name="trade",
    )(padded)
    return out.reshape(count, lines * 128)[:, :size]


def send_kernel(count, capacity, code_ref, row_ref, out_ref):
    place = lax.broadcasted_iota(jnp.int32, (count * capacity, row_ref.shape[0]), 0)
    hit = jnp.logical_or(place == code_ref[0, 0:1, :], place == code_ref[0, 1:2, :])
    rows = dot_low(hit.astype(wide), row_ref[...], ROW_COL)
    for e in range(count):
        out_ref[e, 0] = rows[e * capacity : (e + 1) * capacity].astype(low)


def send_rows(code, rows, count, capacity):
    blocks, _, row_len = code.shape
    width = rows.shape[1]
    return pl.pallas_call(
        functools.partial(send_kernel, count, capacity),
        grid=(blocks,),
        out_shape=jax.ShapeDtypeStruct((count, blocks, capacity, width), low),
        in_specs=[
            pl.BlockSpec((1, TOP, row_len), lambda j: (j, 0, 0)),
            pl.BlockSpec((row_len, width), lambda j: (j, 0)),
        ],
        out_specs=pl.BlockSpec((count, 1, capacity, width), lambda j: (0, j, 0, 0)),
        cost_estimate=pl.CostEstimate(
            flops=2 * blocks * count * capacity * row_len * width,
            bytes_accessed=2 * blocks * (count * capacity + row_len) * width,
            transcendentals=0,
        ),
        name="send_rows",
    )(code, rows)


def after(value, *others):
    return lax.optimization_barrier((value, *others))[0]


def on_device(
    tokens,
    cotangent,
    w_project,
    w_output,
    norm_gain,
    norm_bias,
    router,
    expert_weights,
    routes,
    keep_mask,
    frozen,
    owner_list,
    attend_master,
    attend_first,
    attend_second,
    attend_left,
    attend_right,
    expert_master,
    expert_first,
    expert_second,
    expert_average,
    expert_basis,
    router_first,
    router_second,
    norm_first,
    norm_second,
):
    seq_dev, row_len, model_width = tokens.shape
    expert_count = lax.axis_size("expert")
    dp_count = lax.axis_size("dp")
    my_index = lax.axis_index("expert")
    row_count = seq_dev * row_len
    capacity = max(2, 5 * row_len * TOP // (4 * expert_count))
    expert_total = router.shape[1]
    slots = expert_total * capacity
    parts = expert_count // seq_dev
    whole = parts == 1
    groups, across = None, None
    if not whole:
        groups = [[p * seq_dev + s for s in range(seq_dev)] for p in range(parts)]
        across = [[p * seq_dev + s for p in range(parts)] for s in range(seq_dev)]

    def swap(value):
        return lax.all_to_all(
            value, "expert", split_axis=0, concat_axis=0, tiled=True, axis_index_groups=groups
        )

    def ring(value):
        size = value.shape[0]
        me = my_index % size
        rows = [lax.dynamic_index_in_dim(value, me, 0, keepdims=False)]
        for shift in range(1, size):
            given = lax.dynamic_index_in_dim(value, (me + shift) % size, 0, keepdims=False)
            moves = [
                (d, d - d % size + (d % size + shift) % size) for d in range(expert_count)
            ]
            rows.append(lax.ppermute(given, "expert", moves))
        return rows

    def ring_place(rows):
        size = len(rows)
        rows = jnp.stack(rows[::-1])
        first = size - 1 - my_index % size
        return lax.dynamic_slice_in_dim(jnp.concatenate([rows, rows]), first, size, 0)

    lines = dp_count // 2
    line = lax.axis_index("dp") // 2
    core = lax.axis_index("dp") % 2

    def dp_move(value, shift):
        return lax.ppermute(value, "dp", [(d, (d + 2 * shift) % dp_count) for d in range(dp_count)])

    def other_core(value):
        return lax.ppermute(value, "dp", [(d, d ^ 1) for d in range(dp_count)])

    def cut_dp(value, axis, side):
        size = value.shape[axis] // dp_count
        return [
            lax.dynamic_slice_in_dim(
                value, ((line + shift) % lines * 2 + side) * size, size, axis
            )
            for shift in range(lines)
        ]

    def halve(value, axis, given):
        return [
            (mine.astype(wide) + other_core(theirs).astype(wide)).astype(low)
            for mine, theirs in zip(cut_dp(value, axis, core), given)
        ]

    def spread(half):
        return [half[0]] + [dp_move(half[shift], shift) for shift in range(1, lines)]

    def gather_dp(value):
        rows = [value] + [dp_move(value, shift) for shift in range(1, lines)]
        others = [other_core(row) for row in rows]
        pieces = []
        for place in range(dp_count):
            piece = None
            for mine, theirs, shift in zip(rows, others, range(lines)):
                here = jnp.where(core == place % 2, mine, theirs)
                here = jnp.where((line + lines - shift) % lines == place // 2, here, 0)
                piece = here if piece is None else piece + here
            pieces.append(piece)
        return pieces

    def exchange(value):
        return lax.all_to_all(value, "expert", split_axis=0, concat_axis=0, tiled=True)

    token_seq = swap(tokens)
    token_rows = token_seq.reshape(row_count, model_width).astype(wide)

    choice_ids = routes.reshape(seq_dev, row_len * TOP)
    onehot = choice_ids[..., None] == jnp.arange(expert_total, dtype=jnp.int32)
    before_me = jnp.tri(row_len * TOP, k=-1, dtype=low)
    earlier = jnp.einsum("pq,sqe->spe", before_me, onehot.astype(low), preferred_element_type=wide)
    slot_index = jnp.sum(jnp.where(onehot, earlier, 0.0), axis=-1).astype(jnp.int32)
    place = choice_ids * capacity + slot_index
    home_code = jnp.where(keep_mask.reshape(choice_ids.shape) > 0, place, -1 - choice_ids)
    home_code = jnp.swapaxes(home_code.reshape(seq_dev, row_len, TOP), 1, 2)
    code = ring_place(ring(home_code))

    def hits_of(codes):
        return [
            codes[:, k, :, None] == jnp.arange(slots, dtype=jnp.int32) for k in range(TOP)
        ]

    cot_slots = send_rows(
        home_code, cotangent.reshape(row_count, model_width), expert_total, capacity
    )
    cot_back = exchange(after(cot_slots, token_seq))
    normal_one, spread_one = norm_parts(token_rows)
    low_one = (normal_one * norm_gain[0] + norm_bias[0]).astype(low)
    projected = jnp.dot(low_one, w_project, preferred_element_type=wide).astype(low)
    start = ((my_index // seq_dev) * row_count).astype(jnp.int32).reshape(1)
    pairs = HEADS // 2
    if whole:
        key_value, firsts = projected, (0, pairs, 2 * pairs)
    else:
        key_value = lax.all_gather(
            projected[:, model_width:], "expert", axis=0, tiled=True, axis_index_groups=across
        )
        firsts = (0, 0, pairs)
    attended_low, logs = attend(start, projected, key_value, key_value, firsts, whole)
    middle = token_rows + jnp.dot(attended_low, w_output, preferred_element_type=wide)
    normal_two, spread_two = norm_parts(middle)
    low_two = (normal_two * norm_gain[1] + norm_bias[1]).astype(low)

    hits = hits_of(code)
    sending = send_rows(code, low_two, expert_total, capacity)
    received = exchange(after(sending, cot_back))
    cot_rows = jnp.swapaxes(
        cot_back.reshape(parts, seq_dev, seq_dev, capacity, model_width), 1, 2
    ).reshape(-1, model_width)
    w_second = expert_weights[0, 1]
    pulled = jnp.dot(cot_rows, w_second, preferred_element_type=wide).astype(low)
    received = received.reshape(-1, model_width)

    low_two_wide = low_two.astype(wide)
    logits = jnp.dot(low_two_wide, router, precision=precise).reshape(
        seq_dev, 1, row_len, expert_total
    )
    route = jnp.where(code >= 0, code // capacity, -1 - code)
    onehot_four = (route[..., None] == jnp.arange(expert_total, dtype=jnp.int32)).astype(wide)
    gates = jax.nn.softmax(jnp.sum(onehot_four * logits, axis=-1), axis=1)
    gate_slots = sum(
        jnp.sum(jnp.where(hits[k], gates[:, k, :, None], 0.0), axis=1) for k in range(TOP)
    )
    gate_slots = jnp.swapaxes(gate_slots.reshape(seq_dev, expert_total, capacity), 0, 1)
    gate_slots = gate_slots.reshape(expert_total, seq_dev * capacity)
    select = sum(jnp.where(hits[k], gates[:, k, :, None], 0.0) for k in range(TOP)).astype(low)
    select = select.reshape(seq_dev, row_len, expert_total, capacity)
    cot_seq = swap(after(cotangent, received, pulled, gate_slots))
    grad_final = cot_seq.reshape(row_count, model_width).astype(wide)

    activated_low, grad_before, grad_inputs, gate_grad = expert_stage(
        received, pulled, expert_weights
    )
    slot_shape = (expert_count, seq_dev, capacity)
    grad_inputs = grad_inputs.reshape(slot_shape + (model_width,))
    pair_slots = seq_dev * capacity
    traded = trade(
        jnp.concatenate([gate_slots, gate_grad.reshape(expert_count, pair_slots)], axis=1)
    )
    grad_inputs, activated_low, grad_before, traded, _ = lax.optimization_barrier(
        (grad_inputs, activated_low, grad_before, traded, cot_seq)
    )
    gate_rows = traded[:, :pair_slots].reshape(-1, 1)
    gate_grad_home = traded[:, pair_slots:]
    grad_home = exchange(grad_inputs)
    result = jnp.einsum(
        "rf,df->rd", activated_low, w_second, preferred_element_type=wide
    ).astype(low)
    grad_flat = (gate_rows * cot_rows.astype(wide)).astype(low)
    input_flat = (gate_rows * received.astype(wide)).astype(low)
    grad_first_w = jnp.einsum("rd,rf->df", input_flat, grad_before, preferred_element_type=wide)
    grad_second_w = jnp.einsum("rd,rf->df", grad_flat, activated_low, preferred_element_type=wide)
    flag_value = jnp.sum(
        frozen * (jnp.arange(frozen.shape[0], dtype=jnp.int32) == my_index).astype(jnp.int32)
    )
    trainable = (1 - flag_value).astype(wide)
    expert_grads = [(grad * trainable).astype(low) for grad in (grad_first_w, grad_second_w)]
    expert_given = [cut_dp(grad, 1, 1 - core) for grad in expert_grads]
    coming_back = exchange(after(result.reshape(slot_shape + (model_width,)), grad_home, expert_given))
    expert_half = [halve(grad, 1, given) for grad, given in zip(expert_grads, expert_given)]
    expert_terms = [spread(half) for half in expert_half]

    gate_grad_flat = jnp.swapaxes(
        gate_grad_home.reshape(expert_count, seq_dev, capacity), 0, 1
    ).reshape(seq_dev, 1, slots)
    grad_gate = jnp.stack(
        [jnp.sum(jnp.where(hits[k], gate_grad_flat, 0.0), axis=-1) for k in range(TOP)], axis=1
    )
    grad_chosen = gates * (grad_gate - jnp.sum(gates * grad_gate, axis=1, keepdims=True))
    grad_logits = jnp.sum(onehot_four * grad_chosen[..., None], axis=1).reshape(
        row_count, expert_total
    )
    router_local = jnp.dot(low_two_wide.T, grad_logits, precision=precise)
    grad_low_two = jnp.dot(grad_logits, router.T, precision=precise) + jnp.einsum(
        "jtec,ejcd->jtd", select, grad_home, preferred_element_type=wide
    ).reshape(row_count, model_width)
    moved_two, gain_two, bias_two = norm_back(grad_low_two, normal_two, spread_two, norm_gain[1])
    grad_middle = grad_final + moved_two
    grad_branch = grad_middle.astype(low)
    grad_w_output = jnp.einsum("rd,re->de", attended_low, grad_branch, preferred_element_type=wide)
    grad_attended = jnp.einsum("re,de->rd", grad_branch, w_output, preferred_element_type=wide).astype(
        low
    )

    grad_attended = after(grad_attended, expert_half)
    grad_query, grad_keys, grad_values = attend_back(
        start, projected, key_value, key_value, firsts, grad_attended, attended_low, logs, whole
    )
    mixture = jnp.einsum("jtec,ejcd->jtd", select, after(coming_back, grad_query), preferred_element_type=wide)
    output_seq = (
        (middle + mixture.reshape(row_count, model_width))
        .astype(low)
        .reshape(seq_dev, row_len, model_width)
    )
    if not whole:
        grad_keys, grad_values = (
            lax.psum_scatter(
                g, "expert", scatter_dimension=0, tiled=True, axis_index_groups=across
            )
            for g in (grad_keys, grad_values)
        )
    grad_projected = jnp.concatenate([grad_query, grad_keys, grad_values], axis=1)
    grad_low_one = jnp.einsum("re,de->rd", grad_projected, w_project, preferred_element_type=wide)
    moved_one, gain_one, bias_one = norm_back(grad_low_one, normal_one, spread_one, norm_gain[0])
    input_grad = (grad_middle + moved_one).astype(low).reshape(seq_dev, row_len, model_width)
    input_grad = swap(after(input_grad, coming_back, expert_terms))

    grad_w_project = jnp.einsum("rd,re->de", low_one, grad_projected, preferred_element_type=wide)
    grad_norms = jnp.stack([gain_one, gain_two, bias_one, bias_two])
    block_width = attend_master.shape[2]
    expert_grad, expert_master_new, expert_first_new, expert_second_new, expert_average_new = refresh(
        flag_value.astype(jnp.int32).reshape(1),
        expert_basis[0].astype(low),
        expert_terms,
        expert_master,
        expert_first,
        expert_second,
        expert_average,
    )

    slot_range = jnp.arange(expert_count, dtype=jnp.int32)
    which_block = jnp.sum(
        slot_range[None, :] * (owner_list[None, :] == slot_range[:, None]).astype(jnp.int32), axis=1
    )
    small_width = expert_total + 4
    small = jnp.concatenate([router_local, grad_norms.T], axis=1).astype(low)
    small = jnp.pad(small, ((0, 0), (0, 128 - small_width)))
    grad_full = jnp.concatenate(
        [grad_w_project.astype(low), grad_w_output.astype(low), small], axis=1
    )
    half_rows = halve(grad_full, 0, cut_dp(grad_full, 0, 1 - core))
    my_rows = sum(term.astype(wide) for term in spread(half_rows)).astype(low)
    height = my_rows.shape[0]
    small_rows = -(-small_width // 16) * 16
    small = jnp.pad(
        my_rows[:, block_width * expert_count :][:, :small_width].T,
        ((0, small_rows - small_width), (0, block_width - height)),
    )
    my_rows = deal(which_block, my_rows, small, expert_count)
    my_rows = after(exchange(after(my_rows, input_grad, output_seq)), expert_grad)
    my_rows_done = my_rows
    pieces = gather_dp(jnp.sum(my_rows.astype(wide), axis=0).astype(low))
    block_grad = jnp.concatenate([piece[:height] for piece in pieces]).astype(wide)
    small_sum = jnp.concatenate(
        [piece[height : height + small_width, :height] for piece in pieces], axis=1
    ).astype(wide)
    router_grad = small_sum[:expert_total].T
    norm_grad = small_sum[expert_total:]

    left_basis = attend_left[0].astype(low)
    right_basis = attend_right[0].astype(low)
    rotated = dot_low(dot_low(left_basis, block_grad, COL_COL), right_basis, ROW_COL)
    attend_first_new, attend_second_new, direction = adam_move(
        rotated, attend_first[0], attend_second[0]
    )
    stepped = dot_low(dot_low(left_basis, direction, ROW_COL), right_basis, ROW_ROW)
    attend_master_new = attend_master[0] - matrix_rate * stepped

    output = swap(after(output_seq, my_rows_done))

    output = after(output, attend_master_new)

    router_first_new, router_second_new, router_step = adam_move(
        router_grad, router_first, router_second
    )
    router_new = router - matrix_rate * router_step
    norm_params = jnp.concatenate([norm_gain, norm_bias], axis=0)
    norm_first_new, norm_second_new, norm_step = adam_move(norm_grad, norm_first, norm_second)
    norm_new = norm_params - small_rate * norm_step
    return (
        output,
        input_grad,
        norm_grad,
        norm_new,
        norm_first_new,
        norm_second_new,
        router_grad,
        router_new,
        router_first_new,
        router_second_new,
        block_grad[None],
        attend_master_new[None],
        attend_first_new[None],
        attend_second_new[None],
        expert_grad,
        expert_master_new,
        expert_first_new,
        expert_second_new,
        expert_average_new,
    )


def solution(mesh):
    return jax.shard_map(
        on_device,
        mesh=mesh,
        in_specs=(
            P("dp", "expert", None),
            P("dp", "expert", None),
            P(),
            P(),
            P(),
            P(),
            P(),
            P("expert", None, None, None),
            P("dp", "expert", None),
            P("dp", "expert", None),
            P(),
            P(),
            P("expert", None, None),
            P("expert", None, None),
            P("expert", None, None),
            P("expert", None, None),
            P("expert", None, None),
            P("expert", None, None, "dp"),
            P("expert", None, None, "dp"),
            P("expert", None, None, "dp"),
            P("expert", None, None, "dp"),
            P("expert", None, None),
            P(),
            P(),
            P(),
            P(),
        ),
        out_specs=(
            P("dp", "expert", None),
            P("dp", "expert", None),
            P(),
            P(),
            P(),
            P(),
            P(),
            P(),
            P(),
            P(),
            P("expert", None, None),
            P("expert", None, None),
            P("expert", None, None),
            P("expert", None, None),
            P("expert", None, None, "dp"),
            P("expert", None, None, "dp"),
            P("expert", None, None, "dp"),
            P("expert", None, None, "dp"),
            P("expert", None, None, "dp"),
        ),
        check_vma=False,
    )
```

```python
import functools

import jax
import jax.numpy as jnp
from jax import lax
from jax.experimental import pallas as pl
from jax.experimental.pallas import tpu as pltpu
from jax.sharding import PartitionSpec as P


HEADS = 12
HEAD_DIM = 64
TOP = 2
TILE = 256
CHUNK = 512
ROOT = 0.7978845608028654
CUBIC = 0.044715


norm_epsilon = 1e-05
beta_one = 0.9
beta_two = 0.95
adam_epsilon = 1e-08
adam_step = 10.0
matrix_rate = 0.1
small_rate = 0.5
average_keep = 0.9
precise = lax.Precision.HIGHEST
wide = jnp.float32
low = jnp.bfloat16


def norm_parts(values):
    center = values - jnp.mean(values, axis=-1, keepdims=True)
    spread = lax.rsqrt(jnp.mean(center * center, axis=-1, keepdims=True) + norm_epsilon)
    return center * spread, spread


def norm_back(grad, normal, spread, gain_row):
    g = grad * gain_row
    moved = spread * (
        g
        - jnp.mean(g, axis=-1, keepdims=True)
        - normal * jnp.mean(g * normal, axis=-1, keepdims=True)
    )
    return moved, jnp.sum(grad * normal, axis=0), jnp.sum(grad, axis=0)


def adam_move(gradient, first_moment, second_moment):
    first_new = beta_one * first_moment + (1.0 - beta_one) * gradient
    second_new = beta_two * second_moment + (1.0 - beta_two) * gradient * gradient
    direction = (
        first_new
        / (1.0 - beta_one**adam_step)
        / (jnp.sqrt(second_new / (1.0 - beta_two**adam_step)) + adam_epsilon)
    )
    return (first_new, second_new, direction)


def dot_low(a, b, dims):
    return lax.dot_general(a.astype(low), b.astype(low), (dims, ((), ())), preferred_element_type=wide)


ROW_COL = ((1,), (0,))
ROW_ROW = ((1,), (1,))
COL_COL = ((0,), (0,))


def key_pieces(step, tile, key_len, whole):
    if whole:
        return ((0, step * tile, False), (step * tile, (step + 1) * tile, True))
    return ((0, key_len, True),)


def allowed_at(first_query, first_key, tile, key_count):
    rows = lax.broadcasted_iota(jnp.int32, (tile, key_count), 0) + first_query
    columns = lax.broadcasted_iota(jnp.int32, (tile, key_count), 1) + first_key
    return columns <= rows


def attend_kernel(whole, start_ref, q_ref, k_ref, v_ref, out_ref, log_ref):
    rows, lanes = q_ref.shape
    key_len = k_ref.shape[0]
    lane = lax.broadcasted_iota(jnp.int32, (1, lanes), 1)
    for step in range(rows // TILE):
        at = slice(step * TILE, (step + 1) * TILE)
        total, logs = None, []
        for head in range(2):
            mine = (lane // HEAD_DIM) == head
            query = jnp.where(mine, q_ref[at, :] * HEAD_DIM ** (-0.5), 0).astype(low)
            parts = []
            for first, last, masked in key_pieces(step, TILE, key_len, whole):
                if last > first:
                    scores = dot_low(query, k_ref[first:last, :], ROW_ROW)
                    if masked:
                        origin = step * TILE + (0 if whole else start_ref[0])
                        scores = jnp.where(
                            allowed_at(origin, first, TILE, last - first), scores, -1e30
                        )
                    parts.append((first, last, scores))
            top = functools.reduce(
                jnp.maximum, [jnp.max(s, axis=-1, keepdims=True) for _, _, s in parts]
            )
            summed, acc = None, None
            for first, last, scores in parts:
                weights = jnp.exp(scores - top)
                here = jnp.sum(weights, axis=-1, keepdims=True)
                values = jnp.where(mine, v_ref[first:last, :], 0).astype(low)
                add = dot_low(weights, values, ROW_COL)
                summed = here if summed is None else summed + here
                acc = add if acc is None else acc + add
            acc = acc / summed
            total = acc if total is None else total + acc
            logs.append(top + jnp.log(summed))
        out_ref[at, :] = total.astype(out_ref.dtype)
        log_ref[at, :] = jnp.where(lane < HEAD_DIM, logs[0], logs[1])


def attend_back_kernel(
    whole, start_ref, q_ref, k_ref, v_ref, g_ref, a_ref, log_ref, dq_ref, dk_ref, dv_ref, dk_sum, dv_sum
):
    rows, lanes = q_ref.shape
    key_len = k_ref.shape[0]
    lane = lax.broadcasted_iota(jnp.int32, (1, lanes), 1)
    dk_sum[...] = jnp.zeros_like(dk_sum)
    dv_sum[...] = jnp.zeros_like(dv_sum)
    for step in range(rows // TILE):
        at = slice(step * TILE, (step + 1) * TILE)
        grad_all = g_ref[at, :]
        product = grad_all.astype(wide) * a_ref[at, :].astype(wide)
        dq = None
        for head in range(2):
            mine = (lane // HEAD_DIM) == head
            query = jnp.where(mine, q_ref[at, :] * HEAD_DIM ** (-0.5), 0).astype(low)
            grad = jnp.where(mine, grad_all, 0).astype(low)
            delta = jnp.sum(jnp.where(mine, product, 0.0), axis=-1, keepdims=True)
            log_total = log_ref[at, head * HEAD_DIM : head * HEAD_DIM + 1]
            for first, last, masked in key_pieces(step, TILE, key_len, whole):
                if last > first:
                    keys, values = k_ref[first:last, :], v_ref[first:last, :]
                    weights = jnp.exp(dot_low(query, keys, ROW_ROW) - log_total)
                    if masked:
                        origin = step * TILE + (0 if whole else start_ref[0])
                        weights = jnp.where(
                            allowed_at(origin, first, TILE, last - first), weights, 0.0
                        )
                    moved = (weights * (dot_low(grad, values, ROW_ROW) - delta)).astype(low)
                    dv_sum[first:last, :] += dot_low(weights, grad, COL_COL)
                    dk_sum[first:last, :] += dot_low(moved, query, COL_COL)
                    add = dot_low(moved, jnp.where(mine, keys, 0), ROW_COL)
                    dq = add if dq is None else dq + add
        dq_ref[at, :] = (dq * HEAD_DIM ** (-0.5)).astype(low)
    dk_ref[...] = dk_sum[...].astype(low)
    dv_ref[...] = dv_sum[...].astype(low)


def head_block(rows, first):
    return pl.BlockSpec((rows, 2 * HEAD_DIM), lambda pair: (0, first + pair))


def attend(start, queries, keys, values, firsts, whole):
    rows, key_len, pairs = queries.shape[0], keys.shape[0], HEADS // 2
    width = HEADS * HEAD_DIM
    cost = 4 * rows * key_len * width // (2 if whole else 1)
    return pl.pallas_call(
        functools.partial(attend_kernel, whole),
        grid=(pairs,),
        out_shape=(
            jax.ShapeDtypeStruct((rows, width), low),
            jax.ShapeDtypeStruct((rows, width), wide),
        ),
        in_specs=[
            pl.BlockSpec(memory_space=pltpu.SMEM),
            head_block(rows, firsts[0]),
            head_block(key_len, firsts[1]),
            head_block(key_len, firsts[2]),
        ],
        out_specs=(head_block(rows, 0), head_block(rows, 0)),
        cost_estimate=pl.CostEstimate(
            flops=cost, bytes_accessed=12 * rows * width, transcendentals=rows * key_len * HEADS
        ),
        name="attend",
    )(start, queries, keys, values)


def attend_back(start, queries, keys, values, firsts, grads, attended, logs, whole):
    rows, key_len, pairs = queries.shape[0], keys.shape[0], HEADS // 2
    width = HEADS * HEAD_DIM
    cost = 10 * rows * key_len * width // (2 if whole else 1)
    return pl.pallas_call(
        functools.partial(attend_back_kernel, whole),
        grid=(pairs,),
        out_shape=(
            jax.ShapeDtypeStruct((rows, width), low),
            jax.ShapeDtypeStruct((key_len, width), low),
            jax.ShapeDtypeStruct((key_len, width), low),
        ),
        in_specs=[
            pl.BlockSpec(memory_space=pltpu.SMEM),
            head_block(rows, firsts[0]),
            head_block(key_len, firsts[1]),
            head_block(key_len, firsts[2]),
            head_block(rows, 0),
            head_block(rows, 0),
            head_block(rows, 0),
        ],
        out_specs=(head_block(rows, 0), head_block(key_len, 0), head_block(key_len, 0)),
        scratch_shapes=[
            pltpu.VMEM((key_len, 2 * HEAD_DIM), wide),
            pltpu.VMEM((key_len, 2 * HEAD_DIM), wide),
        ],
        cost_estimate=pl.CostEstimate(
            flops=cost, bytes_accessed=20 * rows * width, transcendentals=rows * key_len * HEADS
        ),
        name="attend_back",
    )(start, queries, keys, values, grads, attended, logs)


def expert_kernel(x_ref, u_ref, w_ref, act_ref, grad_ref, input_ref, gate_grad_ref):
    x = x_ref[...]
    inputs, gate_grad = None, None
    hidden = w_ref.shape[3]
    for first in range(0, hidden, CHUNK):
        at = slice(first, first + CHUNK)
        w = w_ref[0, 0, :, at]
        v = dot_low(x, w, ROW_COL)
        u = u_ref[:, at].astype(wide)
        square = v * v
        t = jnp.tanh(ROOT * v * (1.0 + CUBIC * square))
        half = 0.5 * (1.0 + t)
        act = v * half
        slope = half + 0.5 * ROOT * v * (1.0 - t * t) * (1.0 + 3.0 * CUBIC * square)
        grad = (u * slope).astype(low)
        act_ref[:, at] = act.astype(low)
        grad_ref[:, at] = grad
        here = jnp.sum(act * u, axis=-1, keepdims=True)
        add = dot_low(grad, w, ROW_ROW)
        gate_grad = here if gate_grad is None else gate_grad + here
        inputs = add if inputs is None else inputs + add
    input_ref[...] = inputs.astype(low)
    gate_grad_ref[...] = gate_grad.T


def expert_stage(x, u, w):
    rows, width = x.shape
    hidden = w.shape[3]

    def row_block(columns):
        return pl.BlockSpec((TILE, columns), lambda i: (i, 0))

    return pl.pallas_call(
        expert_kernel,
        grid=(rows // TILE,),
        out_shape=(
            jax.ShapeDtypeStruct((rows, hidden), low),
            jax.ShapeDtypeStruct((rows, hidden), low),
            jax.ShapeDtypeStruct((rows, width), low),
            jax.ShapeDtypeStruct((1, rows), wide),
        ),
        in_specs=[
            row_block(width),
            row_block(hidden),
            pl.BlockSpec((1, 1, width, hidden), lambda i: (0, 0, 0, 0)),
        ],
        out_specs=(
            row_block(hidden),
            row_block(hidden),
            row_block(width),
            pl.BlockSpec((1, TILE), lambda i: (0, i)),
        ),
        cost_estimate=pl.CostEstimate(
            flops=4 * rows * width * hidden,
            bytes_accessed=6 * rows * hidden,
            transcendentals=rows * hidden,
        ),
        name="expert_stage",
    )(x, u, w)


def refresh_kernel(count, flag_ref, basis_ref, turned_ref, *refs):
    terms = [functools.reduce(jnp.add, [r[...].astype(wide) for r in refs[i : i + count]]) for i in (0, count)]
    master_ref, first_ref, second_ref, average_ref = refs[2 * count : 2 * count + 4]
    grad_out, master_out, first_out, second_out, average_out = refs[2 * count + 4 :]
    is_frozen = flag_ref[0] > 0
    grad = jnp.where(pl.program_id(0) == 0, terms[0], terms[1])
    grad_out[0, 0] = grad
    first_new, second_new, move = adam_move(
        dot_low(turned_ref[...], grad, ROW_COL), first_ref[0, 0], second_ref[0, 0]
    )
    master_new = master_ref[0, 0] - matrix_rate * dot_low(basis_ref[...], move, ROW_COL)
    master_new = jnp.where(is_frozen, master_ref[0, 0], master_new)
    master_out[0, 0] = master_new
    first_out[0, 0] = jnp.where(is_frozen, first_ref[0, 0], first_new)
    second_out[0, 0] = jnp.where(is_frozen, second_ref[0, 0], second_new)
    average_out[0, 0] = average_keep * average_ref[0, 0] + (1.0 - average_keep) * master_new


def refresh(flag, basis, terms, master, first, second, average):
    count = len(terms[0])
    _, mats, width, columns = master.shape
    step = 256 if columns % 256 == 0 else 128
    block = pl.BlockSpec((1, 1, width, step), lambda i, j: (0, i, 0, j))
    square = pl.BlockSpec((width, width), lambda i, j: (0, 0))
    return pl.pallas_call(
        functools.partial(refresh_kernel, count),
        grid=(mats, columns // step),
        out_shape=(jax.ShapeDtypeStruct(master.shape, wide),) * 5,
        in_specs=[
            pl.BlockSpec(memory_space=pltpu.SMEM),
            square,
            square,
        ]
        + [pl.BlockSpec((width, step), lambda i, j: (0, jnp.where(i == 0, j, columns // step - 1)))]
        * count
        + [pl.BlockSpec((width, step), lambda i, j: (0, jnp.where(i == 0, 0, j)))] * count
        + [block] * 4,
        out_specs=(block,) * 5,
        cost_estimate=pl.CostEstimate(
            flops=4 * mats * width * width * columns,
            bytes_accessed=38 * mats * width * columns,
            transcendentals=0,
        ),
        name="refresh",
    )(flag, basis, basis.T, *terms[0], *terms[1], master, first, second, average)


def turn_small(small, count):
    lane = lax.broadcasted_iota(jnp.int32, (count, small.shape[1]), 1)
    row = lax.broadcasted_iota(jnp.int32, (count, small.shape[1]), 0)
    return dot_low((lane == row).astype(wide), small, ROW_ROW).astype(low)


def deal_kernel(which_ref, block_ref, small_ref, out_ref):
    height = block_ref.shape[0]
    extra = out_ref.shape[1] - height
    out_ref[0, :height] = block_ref[...]
    out_ref[0, height:] = jnp.zeros((extra, out_ref.shape[2]), low)
    out_ref[0, height:, :height] = turn_small(small_ref[...], extra)


def deal(which, rows, extra, block_width, count):
    height, total = rows.shape
    if block_width % 128:
        small = turn_small(rows[:, block_width * count :], extra)
        small = jnp.pad(small, ((0, 0), (0, block_width - height)))
        return jnp.stack(
            [
                jnp.concatenate(
                    [
                        lax.dynamic_slice_in_dim(rows, which[s] * block_width, block_width, 1),
                        small,
                    ]
                )
                for s in range(count)
            ]
        )
    lanes = total - block_width * count
    return pl.pallas_call(
        deal_kernel,
        grid_spec=pltpu.PrefetchScalarGridSpec(
            num_scalar_prefetch=1,
            grid=(count,),
            in_specs=[
                pl.BlockSpec((height, block_width), lambda s, which: (0, which[s])),
                pl.BlockSpec((height, lanes), lambda s, which: (0, total // lanes - 1)),
            ],
            out_specs=pl.BlockSpec((1, height + extra, block_width), lambda s, which: (s, 0, 0)),
        ),
        out_shape=jax.ShapeDtypeStruct((count, height + extra, block_width), rows.dtype),
        name="deal",
    )(which, rows, rows)


def trade_kernel(count, in_ref, out_ref, landed, send_sem, recv_sem):
    me = lax.axis_index("expert")
    barrier = pltpu.get_barrier_semaphore()
    for shift in range(1, count):
        peer = lax.rem(me + shift, count)
        pl.semaphore_signal(
            barrier, inc=1, device_id={"expert": peer}, device_id_type=pl.DeviceIdType.MESH
        )
    pl.semaphore_wait(barrier, count - 1)
    copies = []
    for shift in range(1, count):
        peer = lax.rem(me + shift, count)
        copy = pltpu.make_async_remote_copy(
            src_ref=in_ref.at[peer],
            dst_ref=landed.at[me],
            send_sem=send_sem.at[shift - 1],
            recv_sem=recv_sem.at[shift - 1],
            device_id={"expert": peer},
            device_id_type=pl.DeviceIdType.MESH,
        )
        copy.start()
        copies.append(copy)
    for shift, copy in zip(range(1, count), copies):
        copy.wait()
        source = lax.rem(me + count - shift, count)
        out_ref[pl.ds(source, 1)] = landed[pl.ds(source, 1)]
    out_ref[pl.ds(me, 1)] = in_ref[pl.ds(me, 1)]


def trade(value):
    count, size = value.shape
    lines = -(-size // 1024) * 8
    padded = jnp.pad(value, ((0, 0), (0, lines * 128 - size))).reshape(count, lines, 128)
    out = pl.pallas_call(
        functools.partial(trade_kernel, count),
        out_shape=jax.ShapeDtypeStruct(padded.shape, padded.dtype),
        in_specs=[pl.BlockSpec(memory_space=pltpu.VMEM)],
        out_specs=pl.BlockSpec(memory_space=pltpu.VMEM),
        scratch_shapes=[
            pltpu.VMEM(padded.shape, padded.dtype),
            pltpu.SemaphoreType.DMA((count - 1,)),
            pltpu.SemaphoreType.DMA((count - 1,)),
        ],
        compiler_params=pltpu.CompilerParams(collective_id=0, has_side_effects=True),
        name="trade",
    )(padded)
    return out.reshape(count, lines * 128)[:, :size]


def send_kernel(count, capacity, code_ref, row_ref, out_ref):
    place = lax.broadcasted_iota(jnp.int32, (count * capacity, row_ref.shape[0]), 0)
    hit = jnp.logical_or(place == code_ref[0, 0:1, :], place == code_ref[0, 1:2, :])
    rows = dot_low(hit.astype(wide), row_ref[...], ROW_COL)
    for e in range(count):
        out_ref[e, 0] = rows[e * capacity : (e + 1) * capacity].astype(low)


def send_rows(code, rows, count, capacity):
    blocks, _, row_len = code.shape
    width = rows.shape[1]
    return pl.pallas_call(
        functools.partial(send_kernel, count, capacity),
        grid=(blocks,),
        out_shape=jax.ShapeDtypeStruct((count, blocks, capacity, width), low),
        in_specs=[
            pl.BlockSpec((1, TOP, row_len), lambda j: (j, 0, 0)),
            pl.BlockSpec((row_len, width), lambda j: (j, 0)),
        ],
        out_specs=pl.BlockSpec((count, 1, capacity, width), lambda j: (0, j, 0, 0)),
        cost_estimate=pl.CostEstimate(
            flops=2 * blocks * count * capacity * row_len * width,
            bytes_accessed=2 * blocks * (count * capacity + row_len) * width,
            transcendentals=0,
        ),
        name="send_rows",
    )(code, rows)


def after(value, *others):
    return lax.optimization_barrier((value, *others))[0]


def on_device(
    tokens,
    cotangent,
    w_project,
    w_output,
    norm_gain,
    norm_bias,
    router,
    expert_weights,
    routes,
    keep_mask,
    frozen,
    owner_list,
    attend_master,
    attend_first,
    attend_second,
    attend_left,
    attend_right,
    expert_master,
    expert_first,
    expert_second,
    expert_average,
    expert_basis,
    router_first,
    router_second,
    norm_first,
    norm_second,
):
    seq_dev, row_len, model_width = tokens.shape
    expert_count = lax.axis_size("expert")
    dp_count = lax.axis_size("dp")
    my_index = lax.axis_index("expert")
    row_count = seq_dev * row_len
    capacity = max(2, 5 * row_len * TOP // (4 * expert_count))
    expert_total = router.shape[1]
    slots = expert_total * capacity
    parts = expert_count // seq_dev
    whole = parts == 1
    groups, across = None, None
    if not whole:
        groups = [[p * seq_dev + s for s in range(seq_dev)] for p in range(parts)]
        across = [[p * seq_dev + s for p in range(parts)] for s in range(seq_dev)]

    def swap(value):
        return lax.all_to_all(
            value, "expert", split_axis=0, concat_axis=0, tiled=True, axis_index_groups=groups
        )

    def ring(value):
        size = value.shape[0]
        me = my_index % size
        rows = [lax.dynamic_index_in_dim(value, me, 0, keepdims=False)]
        for shift in range(1, size):
            given = lax.dynamic_index_in_dim(value, (me + shift) % size, 0, keepdims=False)
            moves = [
                (d, d - d % size + (d % size + shift) % size) for d in range(expert_count)
            ]
            rows.append(lax.ppermute(given, "expert", moves))
        return rows

    def ring_place(rows):
        size = len(rows)
        rows = jnp.stack(rows[::-1])
        first = size - 1 - my_index % size
        return lax.dynamic_slice_in_dim(jnp.concatenate([rows, rows]), first, size, 0)

    lines = dp_count // 2
    line = lax.axis_index("dp") // 2
    core = lax.axis_index("dp") % 2

    def dp_move(value, shift):
        return lax.ppermute(value, "dp", [(d, (d + 2 * shift) % dp_count) for d in range(dp_count)])

    def other_core(value):
        return lax.ppermute(value, "dp", [(d, d ^ 1) for d in range(dp_count)])

    def cut_dp(value, axis, side):
        size = value.shape[axis] // dp_count
        return [
            lax.dynamic_slice_in_dim(
                value, ((line + shift) % lines * 2 + side) * size, size, axis
            )
            for shift in range(lines)
        ]

    def halve(value, axis, given):
        return [
            (mine.astype(wide) + other_core(theirs).astype(wide)).astype(low)
            for mine, theirs in zip(cut_dp(value, axis, core), given)
        ]

    def spread(half):
        return [half[0]] + [dp_move(half[shift], shift) for shift in range(1, lines)]

    def gather_dp(value):
        rows = [value] + [dp_move(value, shift) for shift in range(1, lines)]
        others = [other_core(row) for row in rows]
        pieces = []
        for place in range(dp_count):
            piece = None
            for mine, theirs, shift in zip(rows, others, range(lines)):
                here = jnp.where(core == place % 2, mine, theirs)
                here = jnp.where((line + lines - shift) % lines == place // 2, here, 0)
                piece = here if piece is None else piece + here
            pieces.append(piece)
        return pieces

    def exchange(value):
        return lax.all_to_all(value, "expert", split_axis=0, concat_axis=0, tiled=True)

    token_seq = swap(tokens)
    token_rows = token_seq.reshape(row_count, model_width).astype(wide)

    choice_ids = routes.reshape(seq_dev, row_len * TOP)
    onehot = choice_ids[..., None] == jnp.arange(expert_total, dtype=jnp.int32)
    before_me = jnp.tri(row_len * TOP, k=-1, dtype=low)
    earlier = jnp.einsum("pq,sqe->spe", before_me, onehot.astype(low), preferred_element_type=wide)
    slot_index = jnp.sum(jnp.where(onehot, earlier, 0.0), axis=-1).astype(jnp.int32)
    place = choice_ids * capacity + slot_index
    home_code = jnp.where(keep_mask.reshape(choice_ids.shape) > 0, place, -1 - choice_ids)
    home_code = jnp.swapaxes(home_code.reshape(seq_dev, row_len, TOP), 1, 2)
    code = ring_place(ring(home_code))

    def hits_of(codes):
        return [
            codes[:, k, :, None] == jnp.arange(slots, dtype=jnp.int32) for k in range(TOP)
        ]

    cot_slots = send_rows(
        home_code, cotangent.reshape(row_count, model_width), expert_total, capacity
    )
    cot_back = exchange(after(cot_slots, token_seq))
    normal_one, spread_one = norm_parts(token_rows)
    low_one = (normal_one * norm_gain[0] + norm_bias[0]).astype(low)
    projected = jnp.dot(low_one, w_project, preferred_element_type=wide).astype(low)
    start = ((my_index // seq_dev) * row_count).astype(jnp.int32).reshape(1)
    pairs = HEADS // 2
    if whole:
        key_value, firsts = projected, (0, pairs, 2 * pairs)
    else:
        key_value = lax.all_gather(
            projected[:, model_width:], "expert", axis=0, tiled=True, axis_index_groups=across
        )
        firsts = (0, 0, pairs)
    attended_low, logs = attend(start, projected, key_value, key_value, firsts, whole)
    middle = token_rows + jnp.dot(attended_low, w_output, preferred_element_type=wide)
    normal_two, spread_two = norm_parts(middle)
    low_two = (normal_two * norm_gain[1] + norm_bias[1]).astype(low)

    hits = hits_of(code)
    sending = send_rows(code, low_two, expert_total, capacity)
    received = exchange(after(sending, cot_back))
    cot_rows = jnp.swapaxes(
        cot_back.reshape(parts, seq_dev, seq_dev, capacity, model_width), 1, 2
    ).reshape(-1, model_width)
    w_second = expert_weights[0, 1]
    pulled = jnp.dot(cot_rows, w_second, preferred_element_type=wide).astype(low)
    received = received.reshape(-1, model_width)

    low_two_wide = low_two.astype(wide)
    logits = jnp.dot(low_two_wide, router, precision=precise).reshape(
        seq_dev, 1, row_len, expert_total
    )
    route = jnp.where(code >= 0, code // capacity, -1 - code)
    onehot_four = (route[..., None] == jnp.arange(expert_total, dtype=jnp.int32)).astype(wide)
    gates = jax.nn.softmax(jnp.sum(onehot_four * logits, axis=-1), axis=1)
    gate_slots = sum(
        jnp.sum(jnp.where(hits[k], gates[:, k, :, None], 0.0), axis=1) for k in range(TOP)
    )
    gate_slots = jnp.swapaxes(gate_slots.reshape(seq_dev, expert_total, capacity), 0, 1)
    gate_slots = gate_slots.reshape(expert_total, seq_dev * capacity)
    select = sum(jnp.where(hits[k], gates[:, k, :, None], 0.0) for k in range(TOP)).astype(low)
    select = select.reshape(seq_dev, row_len, expert_total, capacity)
    cot_seq = swap(after(cotangent, received, pulled, gate_slots))
    grad_final = cot_seq.reshape(row_count, model_width).astype(wide)

    activated_low, grad_before, grad_inputs, gate_grad = expert_stage(
        received, pulled, expert_weights
    )
    slot_shape = (expert_count, seq_dev, capacity)
    grad_inputs = grad_inputs.reshape(slot_shape + (model_width,))
    pair_slots = seq_dev * capacity
    traded = trade(
        jnp.concatenate([gate_slots, gate_grad.reshape(expert_count, pair_slots)], axis=1)
    )
    grad_inputs, activated_low, grad_before, traded, _ = lax.optimization_barrier(
        (grad_inputs, activated_low, grad_before, traded, cot_seq)
    )
    gate_rows = traded[:, :pair_slots].reshape(-1, 1)
    gate_grad_home = traded[:, pair_slots:]
    grad_home = exchange(grad_inputs)
    result = jnp.einsum(
        "rf,df->rd", activated_low, w_second, preferred_element_type=wide
    ).astype(low)
    grad_flat = (gate_rows * cot_rows.astype(wide)).astype(low)
    input_flat = (gate_rows * received.astype(wide)).astype(low)
    grad_first_w = jnp.einsum("rd,rf->df", input_flat, grad_before, preferred_element_type=wide)
    grad_second_w = jnp.einsum("rd,rf->df", grad_flat, activated_low, preferred_element_type=wide)
    flag_value = jnp.sum(
        frozen * (jnp.arange(frozen.shape[0], dtype=jnp.int32) == my_index).astype(jnp.int32)
    )
    trainable = (1 - flag_value).astype(wide)
    expert_grads = [(grad * trainable).astype(low) for grad in (grad_first_w, grad_second_w)]
    expert_given = [cut_dp(grad, 1, 1 - core) for grad in expert_grads]
    coming_back = exchange(after(result.reshape(slot_shape + (model_width,)), grad_home, expert_given))
    expert_half = [halve(grad, 1, given) for grad, given in zip(expert_grads, expert_given)]
    expert_terms = [spread(half) for half in expert_half]

    gate_grad_flat = jnp.swapaxes(
        gate_grad_home.reshape(expert_count, seq_dev, capacity), 0, 1
    ).reshape(seq_dev, 1, slots)
    grad_gate = jnp.stack(
        [jnp.sum(jnp.where(hits[k], gate_grad_flat, 0.0), axis=-1) for k in range(TOP)], axis=1
    )
    grad_chosen = gates * (grad_gate - jnp.sum(gates * grad_gate, axis=1, keepdims=True))
    grad_logits = jnp.sum(onehot_four * grad_chosen[..., None], axis=1).reshape(
        row_count, expert_total
    )
    router_local = jnp.dot(low_two_wide.T, grad_logits, precision=precise)
    grad_low_two = jnp.dot(grad_logits, router.T, precision=precise) + jnp.einsum(
        "jtec,ejcd->jtd", select, grad_home, preferred_element_type=wide
    ).reshape(row_count, model_width)
    moved_two, gain_two, bias_two = norm_back(grad_low_two, normal_two, spread_two, norm_gain[1])
    grad_middle = grad_final + moved_two
    grad_branch = grad_middle.astype(low)
    grad_w_output = jnp.einsum("rd,re->de", attended_low, grad_branch, preferred_element_type=wide)
    grad_attended = jnp.einsum("re,de->rd", grad_branch, w_output, preferred_element_type=wide).astype(
        low
    )

    grad_attended = after(grad_attended, expert_half)
    grad_query, grad_keys, grad_values = attend_back(
        start, projected, key_value, key_value, firsts, grad_attended, attended_low, logs, whole
    )
    mixture = jnp.einsum("jtec,ejcd->jtd", select, after(coming_back, grad_query), preferred_element_type=wide)
    output_seq = (
        (middle + mixture.reshape(row_count, model_width))
        .astype(low)
        .reshape(seq_dev, row_len, model_width)
    )
    if not whole:
        grad_keys, grad_values = (
            lax.psum_scatter(
                g, "expert", scatter_dimension=0, tiled=True, axis_index_groups=across
            )
            for g in (grad_keys, grad_values)
        )
    grad_projected = jnp.concatenate([grad_query, grad_keys, grad_values], axis=1)
    grad_low_one = jnp.einsum("re,de->rd", grad_projected, w_project, preferred_element_type=wide)
    moved_one, gain_one, bias_one = norm_back(grad_low_one, normal_one, spread_one, norm_gain[0])
    input_grad = (grad_middle + moved_one).astype(low).reshape(seq_dev, row_len, model_width)
    input_grad = swap(after(input_grad, coming_back, expert_terms))

    grad_w_project = jnp.einsum("rd,re->de", low_one, grad_projected, preferred_element_type=wide)
    grad_norms = jnp.stack([gain_one, gain_two, bias_one, bias_two])
    block_width = attend_master.shape[2]
    expert_grad, expert_master_new, expert_first_new, expert_second_new, expert_average_new = refresh(
        flag_value.astype(jnp.int32).reshape(1),
        expert_basis[0].astype(low),
        expert_terms,
        expert_master,
        expert_first,
        expert_second,
        expert_average,
    )

    slot_range = jnp.arange(expert_count, dtype=jnp.int32)
    which_block = jnp.sum(
        slot_range[None, :] * (owner_list[None, :] == slot_range[:, None]).astype(jnp.int32), axis=1
    )
    small_width = expert_total + 4
    small = jnp.concatenate([router_local, grad_norms.T], axis=1).astype(low)
    small = jnp.pad(small, ((0, 0), (0, 128 - small_width)))
    grad_full = jnp.concatenate(
        [grad_w_project.astype(low), grad_w_output.astype(low), small], axis=1
    )
    half_rows = halve(grad_full, 0, cut_dp(grad_full, 0, 1 - core))
    dp_terms, output_seq = lax.optimization_barrier((spread(half_rows), output_seq))
    my_rows = sum(term.astype(wide) for term in dp_terms).astype(low)
    height = my_rows.shape[0]
    small_rows = -(-small_width // 16) * 16
    my_rows = deal(which_block, my_rows, small_rows, block_width, expert_count)
    my_rows = after(exchange(after(my_rows, input_grad)), expert_grad)
    my_rows_done = my_rows
    pieces = gather_dp(jnp.sum(my_rows.astype(wide), axis=0).astype(low))
    block_grad = jnp.concatenate([piece[:height] for piece in pieces]).astype(wide)
    small_sum = jnp.concatenate(
        [piece[height : height + small_width, :height] for piece in pieces], axis=1
    ).astype(wide)
    router_grad = small_sum[:expert_total].T
    norm_grad = small_sum[expert_total:]

    left_basis = attend_left[0].astype(low)
    right_basis = attend_right[0].astype(low)
    rotated = dot_low(dot_low(left_basis, block_grad, COL_COL), right_basis, ROW_COL)
    attend_first_new, attend_second_new, direction = adam_move(
        rotated, attend_first[0], attend_second[0]
    )
    stepped = dot_low(dot_low(left_basis, direction, ROW_COL), right_basis, ROW_ROW)
    attend_master_new = attend_master[0] - matrix_rate * stepped

    output = swap(after(output_seq, my_rows_done))

    output = after(output, attend_master_new)

    router_first_new, router_second_new, router_step = adam_move(
        router_grad, router_first, router_second
    )
    router_new = router - matrix_rate * router_step
    norm_params = jnp.concatenate([norm_gain, norm_bias], axis=0)
    norm_first_new, norm_second_new, norm_step = adam_move(norm_grad, norm_first, norm_second)
    norm_new = norm_params - small_rate * norm_step
    return (
        output,
        input_grad,
        norm_grad,
        norm_new,
        norm_first_new,
        norm_second_new,
        router_grad,
        router_new,
        router_first_new,
        router_second_new,
        block_grad[None],
        attend_master_new[None],
        attend_first_new[None],
        attend_second_new[None],
        expert_grad,
        expert_master_new,
        expert_first_new,
        expert_second_new,
        expert_average_new,
    )


def solution(mesh):
    return jax.shard_map(
        on_device,
        mesh=mesh,
        in_specs=(
            P("dp", "expert", None),
            P("dp", "expert", None),
            P(),
            P(),
            P(),
            P(),
            P(),
            P("expert", None, None, None),
            P("dp", "expert", None),
            P("dp", "expert", None),
            P(),
            P(),
            P("expert", None, None),
            P("expert", None, None),
            P("expert", None, None),
            P("expert", None, None),
            P("expert", None, None),
            P("expert", None, None, "dp"),
            P("expert", None, None, "dp"),
            P("expert", None, None, "dp"),
            P("expert", None, None, "dp"),
            P("expert", None, None),
            P(),
            P(),
            P(),
            P(),
        ),
        out_specs=(
            P("dp", "expert", None),
            P("dp", "expert", None),
            P(),
            P(),
            P(),
            P(),
            P(),
            P(),
            P(),
            P(),
            P("expert", None, None),
            P("expert", None, None),
            P("expert", None, None),
            P("expert", None, None),
            P("expert", None, None, "dp"),
            P("expert", None, None, "dp"),
            P("expert", None, None, "dp"),
            P("expert", None, None, "dp"),
            P("expert", None, None, "dp"),
        ),
        check_vma=False,
    )
```
